16 devices in a mesh: data: 16 (over z, y, x, core).
Axes of the slice: x: 2, y: 2, z: 2, core: 2. Of those that a mesh axis runs over, the one named last changes fastest.
Arguments:
- grad_attn: bfloat16 [16, 4, 1638400], P('data')
- grad_mlp: bfloat16 [16, 2, 6553600], P('data')
- grad_wide: bfloat16 [16, 1, 5120], P('data')
- grad_vec: bfloat16 [16, 11, 1280], P('data')
- weight_attn: float32 [4, 1638400], P(None, 'data')
- weight_mlp: float32 [2, 6553600], P(None, 'data')
- weight_wide: float32 [1, 5120], P(None, 'data')
- weight_vec: float32 [11, 1280], P(None, 'data')
- mom1_attn: float32 [4, 1638400], P(None, 'data')
- mom1_mlp: float32 [2, 6553600], P(None, 'data')
- mom1_wide: float32 [1, 5120], P(None, 'data')
- mom1_vec: float32 [11, 1280], P(None, 'data')
- mom2_attn: float32 [4, 1638400], P(None, 'data')
- mom2_mlp: float32 [2, 6553600], P(None, 'data')
- mom2_wide: float32 [1, 5120], P(None, 'data')
- mom2_vec: float32 [11, 1280], P(None, 'data')
Outputs:
- output 1: bfloat16 [4, 1638400], replicated
- output 2: bfloat16 [2, 6553600], replicated
- output 3: bfloat16 [1, 5120], replicated
- output 4: bfloat16 [11, 1280], replicated
- output 5: float32 [4, 1638400], P(None, 'data')
- output 6: float32 [2, 6553600], P(None, 'data')
- output 7: float32 [1, 5120], P(None, 'data')
- output 8: float32 [11, 1280], P(None, 'data')
- output 9: float32 [4, 1638400], P(None, 'data')
- output 10: float32 [2, 6553600], P(None, 'data')
- output 11: float32 [1, 5120], P(None, 'data')
- output 12: float32 [11, 1280], P(None, 'data')
- output 13: float32 [4, 1638400], P(None, 'data')
- output 14: float32 [2, 6553600], P(None, 'data')
- output 15: float32 [1, 5120], P(None, 'data')
- output 16: float32 [11, 1280], P(None, 'data')
All inputs are finite; a program needn't handle non-finite values.
Results may differ from the reference program's by a relative error of at most 0.001.
Values are sent between devices in bfloat16 or wider.
A program may use at most 1 GiB of HBM per device.

```python
import jax
import jax.numpy as jnp

GROUP_SIZE = 16
LAYERS = 1
D = 1280
FF = 5120
STEP_NUMBER = 10

LEARN_RATE = 0.04
BETA_FIRST = 0.9
BETA_SECOND = 0.999
EPSILON = 1e-6
WEIGHT_DECAY = 0.01
MAX_NORM = 1.0
TARGET_NORM = 3.0


def bank_layout():
    gain_rows = jnp.array([1.0, 0.0, 0.0, 0.0, 0.0, 0.0, 1.0, 0.0, 0.0] * LAYERS + [1.0, 0.0])
    counts = (4 * LAYERS, 2 * LAYERS, LAYERS, 9 * LAYERS + 2)
    lengths = (D * D, D * FF, FF, D)
    base_scales = (
        jnp.full((4 * LAYERS,), D ** -0.5),
        jnp.array([D ** -0.5, FF ** -0.5] * LAYERS),
        jnp.full((LAYERS,), 0.05),
        0.05 + 0.15 * gain_rows,
    )
    offsets = (jnp.zeros((4 * LAYERS,)), jnp.zeros((2 * LAYERS,)), jnp.zeros((LAYERS,)), gain_rows)
    return counts, lengths, base_scales, offsets


def setup_inputs(seed: int = 0) -> dict:
    root_key = jax.random.key(seed)
    counts, lengths, base_scales, offsets = bank_layout()
    bank_keys = [jax.random.split(jax.random.fold_in(root_key, bank_index), 6) for bank_index in range(4)]
    grad_mults = [jnp.exp(jax.random.uniform(bank_keys[bank_index][0], (counts[bank_index],), minval=-1.0, maxval=1.0)) for bank_index in range(4)]
    weighted = sum(lengths[bank_index] * jnp.sum(grad_mults[bank_index] ** 2) for bank_index in range(4))
    grad_unit = TARGET_NORM * jnp.sqrt(GROUP_SIZE / weighted)
    clip_guess = MAX_NORM / TARGET_NORM
    grad_banks, weights, firsts, seconds = [], [], [], []
    for bank_index in range(4):
        bank_keyset = bank_keys[bank_index]
        row_count = counts[bank_index]
        row_length = lengths[bank_index]
        grad_scale = grad_unit * grad_mults[bank_index]
        device_grads = jax.random.normal(bank_keyset[1], (GROUP_SIZE, row_count, row_length)) * grad_scale[None, :, None]
        grad_banks.append(device_grads.astype(jnp.bfloat16))
        weight_spread = jnp.exp(jax.random.uniform(bank_keyset[2], (row_count,), minval=-1.2, maxval=1.2))
        row_scale = base_scales[bank_index] * weight_spread
        weights.append(offsets[bank_index][:, None] + row_scale[:, None] * jax.random.normal(bank_keyset[3], (row_count, row_length)))
        moment_unit = clip_guess * grad_scale / GROUP_SIZE ** 0.5
        firsts.append(0.1 * moment_unit[:, None] * jax.random.normal(bank_keyset[4], (row_count, row_length)))
        seconds.append(0.001 * (moment_unit * moment_unit)[:, None] * jnp.exp(0.5 * jax.random.normal(bank_keyset[5], (row_count, row_length))))
    bank_names = ("attn", "mlp", "wide", "vec")
    inputs = {}
    for prefix, arrays in (("grad_", grad_banks), ("weight_", weights), ("mom1_", firsts), ("mom2_", seconds)):
        for bank_index in range(4):
            inputs[prefix + bank_names[bank_index]] = arrays[bank_index]
    return inputs


def lamb_bank(mean_grad, weight, first_moment, second_moment, clip_coef):
    clipped = clip_coef * mean_grad
    new_first = BETA_FIRST * first_moment + (1.0 - BETA_FIRST) * clipped
    new_second = BETA_SECOND * second_moment + (1.0 - BETA_SECOND) * (clipped * clipped)
    update = (new_first / (1.0 - BETA_FIRST ** STEP_NUMBER)) / (jnp.sqrt(new_second / (1.0 - BETA_SECOND ** STEP_NUMBER)) + EPSILON) + WEIGHT_DECAY * weight
    weight_norm = jnp.sqrt(jnp.sum(weight * weight, axis=1, keepdims=True))
    update_norm = jnp.sqrt(jnp.sum(update * update, axis=1, keepdims=True))
    new_weight = weight - LEARN_RATE * (weight_norm / update_norm) * update
    return new_weight.astype(jnp.bfloat16), new_weight, new_first, new_second


def reference(grad_attn, grad_mlp, grad_wide, grad_vec, weight_attn, weight_mlp, weight_wide, weight_vec, mom1_attn, mom1_mlp, mom1_wide, mom1_vec, mom2_attn, mom2_mlp, mom2_wide, mom2_vec):
    mean_attn = jnp.sum(grad_attn, axis=0, dtype=jnp.float32) / GROUP_SIZE
    mean_mlp = jnp.sum(grad_mlp, axis=0, dtype=jnp.float32) / GROUP_SIZE
    mean_wide = jnp.sum(grad_wide, axis=0, dtype=jnp.float32) / GROUP_SIZE
    mean_vec = jnp.sum(grad_vec, axis=0, dtype=jnp.float32) / GROUP_SIZE
    total_square = jnp.sum(mean_attn * mean_attn) + jnp.sum(mean_mlp * mean_mlp) + jnp.sum(mean_wide * mean_wide) + jnp.sum(mean_vec * mean_vec)
    clip_coef = jnp.minimum(1.0, MAX_NORM / jnp.sqrt(total_square))
    attn_out = lamb_bank(mean_attn, weight_attn, mom1_attn, mom2_attn, clip_coef)
    mlp_out = lamb_bank(mean_mlp, weight_mlp, mom1_mlp, mom2_mlp, clip_coef)
    wide_out = lamb_bank(mean_wide, weight_wide, mom1_wide, mom2_wide, clip_coef)
    vec_out = lamb_bank(mean_vec, weight_vec, mom1_vec, mom2_vec, clip_coef)
    return (attn_out[0], mlp_out[0], wide_out[0], vec_out[0], attn_out[1], mlp_out[1], wide_out[1], vec_out[1], attn_out[2], mlp_out[2], wide_out[2], vec_out[2], attn_out[3], mlp_out[3], wide_out[3], vec_out[3])
```

```python
import functools

import jax
import jax.numpy as jnp
from jax import lax
from jax.experimental import pallas as pl
from jax.experimental.pallas import tpu as pltpu
from jax.sharding import PartitionSpec as P

STEP_NUMBER = 10
LEARN_RATE = 0.04
BETA_FIRST = 0.9
BETA_SECOND = 0.999
EPSILON = 1e-6
WEIGHT_DECAY = 0.01
MAX_NORM = 1.0

MESH = pl.DeviceIdType.MESH
GROUP = 16
LANES = 128
ATTN_ROWS = 3200
MLP_ROWS = 6400
THIRD = 3200
PIECE = 320
PIECES = THIRD // PIECE
LOAD_SLOTS = 3
SEND_SLOTS = 4
SMALL_ROWS = 16
CORE = 1
ORDERS = ((2, 4, 8), (4, 8, 2), (8, 2, 4))
UNITS = (
    (0, (0, 1, 2), ()),
    (0, (0, 1), ()),
    (0, (0, 2), ()),
    (1, (1, 2), (0,)),
    (0, (0,), ()),
    (1, (1,), (1,)),
    (2, (2,), (2, 3)),
    (None, (), (4, 5, 6)),
)


def flip(index, width):
    return index + width * (1 - 2 * ((index // width) % 2))


def flip_all(index, widths):
    for width in widths:
        index = flip(index, width)
    return index


def meet_everyone(me):
    barrier = pltpu.get_barrier_semaphore()

    def signal(step, carry):
        pl.semaphore_signal(barrier, inc=1, device_id=((me + step) % GROUP,), device_id_type=MESH)
        return carry

    lax.fori_loop(1, GROUP, signal, 0)
    pl.semaphore_wait(barrier, GROUP - 1)


def tile_to_everyone(me, source_of, slots, send_sems, recv_sems, begin):
    def copy(step):
        return pltpu.make_async_remote_copy(
            source_of((me + step) % GROUP), slots.at[me], send_sems.at[step], recv_sems.at[step],
            device_id=((me + step) % GROUP,), device_id_type=MESH)

    def arrival(step):
        return pltpu.make_async_remote_copy(
            source_of((me + step) % GROUP), slots.at[(me - step + GROUP) % GROUP], send_sems.at[step], recv_sems.at[step],
            device_id=((me + step) % GROUP,), device_id_type=MESH)

    def start(step, carry):
        copy(step).start()
        return carry

    def finish(step, carry):
        arrival(step).wait()
        return carry

    lax.fori_loop(1, GROUP, start if begin else finish, 0)


def scatter_kernel(grad_attn, grad_mlp, grad_small, sums, small_sums, total, pair_raw, landed,
                   raw_own, raw_pair, partial, outgoing, square_sum, small_slots, square_slots,
                   load_sems, send_sems, pair_send_first, pair_recv_first, pair_send, pair_recv, land_sems,
                   small_send, small_recv, square_send, square_recv, local_sem):
    me = lax.axis_index("data")
    twin = flip(me, CORE)
    meet_everyone(me)

    def grad_of(third, owner, row, count):
        if third == 0:
            return grad_attn.at[owner, pl.ds(row, count)]
        return grad_mlp.at[owner, pl.ds(row + (third - 1) * THIRD, count)]

    def owner_of(unit, third):
        return flip_all(me, [ORDERS[third][place] for place in UNITS[unit][1]])

    def pair_first(third, piece):
        rows = piece * PIECE
        return pltpu.make_async_remote_copy(
            grad_of(third, flip(owner_of(0, third), CORE), rows, PIECE), pair_raw.at[0, third, pl.ds(rows, PIECE)],
            pair_send_first.at[third, piece], pair_recv_first.at[third, piece], device_id=(twin,), device_id_type=MESH)

    def pair_copy(unit, third):
        return pltpu.make_async_remote_copy(
            grad_of(third, flip(owner_of(unit, third), CORE), 0, THIRD), pair_raw.at[unit, third],
            pair_send.at[unit, third], pair_recv.at[unit, third], device_id=(twin,), device_id_type=MESH)

    def start_first(piece, carry):
        for third in range(3):
            pair_first(third, piece).start()
        return carry

    lax.fori_loop(0, PIECES, start_first, 0)
    for unit in range(1, 8):
        for third in range(3):
            pair_copy(unit, third).start()
    own_small = pltpu.make_async_copy(grad_small.at[me], small_slots.at[me], local_sem)
    own_small.start()
    tile_to_everyone(me, lambda owner: grad_small.at[owner], small_slots, small_send, small_recv, True)
    square_sum[...] = jnp.zeros_like(square_sum)

    def loads(unit, third, piece):
        rows = piece * PIECE
        slot = (unit * PIECES + piece) % LOAD_SLOTS
        copies = [
            pltpu.make_async_copy(grad_of(third, owner_of(unit, third), rows, PIECE), raw_own.at[slot, third], load_sems.at[slot, third, 0]),
            pltpu.make_async_copy(pair_raw.at[unit, third, pl.ds(rows, PIECE)], raw_pair.at[slot, third], load_sems.at[slot, third, 1]),
        ]
        for place, source in enumerate(UNITS[unit][2]):
            copies.append(pltpu.make_async_copy(
                landed.at[source, third, pl.ds(rows, PIECE)], partial.at[slot, third, place], load_sems.at[slot, third, 2 + place]))
        return copies

    def send(unit, third, piece):
        rows = piece * PIECE
        slot = (unit * PIECES + piece) % SEND_SLOTS
        to = flip(me, ORDERS[third][UNITS[unit][0]])
        return pltpu.make_async_remote_copy(
            outgoing.at[slot, third], landed.at[unit, third, pl.ds(rows, PIECE)],
            send_sems.at[slot, third], land_sems.at[unit, third, piece], device_id=(to,), device_id_type=MESH)

    def begin(unit, piece):
        for third in range(3):
            if unit == 0:
                pair_first(third, piece).wait_recv()
            else:
                @pl.when(piece == 0)
                def _():
                    pair_copy(unit, third).wait_recv()
            for source in UNITS[unit][2]:
                send(source, third, piece).wait_recv()
            for copy in loads(unit, third, piece):
                copy.start()

    ahead = LOAD_SLOTS - 1
    for piece in range(ahead):
        begin(0, piece)

    for unit in range(8):
        def work(piece, carry, unit=unit):
            @pl.when(piece + ahead < PIECES)
            def _():
                begin(unit, piece + ahead)
            if unit < 7:
                @pl.when(piece + ahead >= PIECES)
                def _():
                    begin(unit + 1, piece + ahead - PIECES)
            slot = (unit * PIECES + piece) % LOAD_SLOTS
            out_slot = (unit * PIECES + piece) % SEND_SLOTS
            for third in range(3):
                for copy in loads(unit, third, piece):
                    copy.wait()
                value = raw_own[slot, third].astype(jnp.float32) + raw_pair[slot, third].astype(jnp.float32)
                for place in range(len(UNITS[unit][2])):
                    value = value + partial[slot, third, place]
                if unit < 7:
                    if unit == 0:
                        @pl.when(piece >= SEND_SLOTS)
                        def _():
                            send(unit, third, piece).wait_send()
                    else:
                        send(unit, third, piece).wait_send()
                    outgoing[out_slot, third] = value
                    send(unit, third, piece).start()
                else:
                    value = value * (1.0 / GROUP)
                    sums[pl.ds(pl.multiple_of(third * THIRD + piece * PIECE, PIECE), PIECE)] = value
                    square_sum[...] += jnp.sum((value * value).reshape(PIECE // 8, 8, LANES), axis=0)
            return carry

        lax.fori_loop(0, PIECES, work, 0)

    own_small.wait()
    tile_to_everyone(me, lambda owner: grad_small.at[owner], small_slots, small_send, small_recv, False)
    small = jnp.sum(small_slots[...].astype(jnp.float32), axis=0) * (1.0 / GROUP)
    small_sums[...] = small
    squares = square_sum[...] + (small * small)[0:8] + (small * small)[8:16]
    square_sum[...] = squares
    square_slots[me] = squares
    tile_to_everyone(me, lambda owner: square_sum, square_slots, square_send, square_recv, True)
    for slot in range(SEND_SLOTS):
        for third in range(3):
            send(6, third, slot).wait_send()

    def drain(piece, carry):
        for third in range(3):
            pair_first(third, piece).wait_send()
        return carry

    lax.fori_loop(0, PIECES, drain, 0)
    for unit in range(1, 8):
        for third in range(3):
            pair_copy(unit, third).wait_send()
    tile_to_everyone(me, lambda owner: square_sum, square_slots, square_send, square_recv, False)
    total[...] = jnp.full((8, LANES), jnp.sum(square_slots[...]), jnp.float32)


def reduce_scatter(grad_attn, grad_mlp, grad_small):
    rows = ATTN_ROWS + MLP_ROWS
    anywhere = pl.BlockSpec(memory_space=pl.ANY)
    inside = pl.BlockSpec(memory_space=pltpu.VMEM)
    dma = pltpu.SemaphoreType.DMA
    return pl.pallas_call(
        scatter_kernel,
        name="scatter",
        out_shape=(
            jax.ShapeDtypeStruct((rows, LANES), jnp.float32),
            jax.ShapeDtypeStruct((SMALL_ROWS, LANES), jnp.float32),
            jax.ShapeDtypeStruct((8, LANES), jnp.float32),
            jax.ShapeDtypeStruct((8, 3, THIRD, LANES), jnp.bfloat16),
            jax.ShapeDtypeStruct((7, 3, THIRD, LANES), jnp.float32),
        ),
        in_specs=[anywhere] * 3,
        out_specs=(inside, inside, inside, anywhere, anywhere),
        scratch_shapes=[
            pltpu.VMEM((LOAD_SLOTS, 3, PIECE, LANES), jnp.bfloat16),
            pltpu.VMEM((LOAD_SLOTS, 3, PIECE, LANES), jnp.bfloat16),
            pltpu.VMEM((LOAD_SLOTS, 3, 3, PIECE, LANES), jnp.float32),
            pltpu.VMEM((SEND_SLOTS, 3, PIECE, LANES), jnp.float32),
            pltpu.VMEM((8, LANES), jnp.float32),
            pltpu.VMEM((GROUP, SMALL_ROWS, LANES), jnp.bfloat16),
            pltpu.VMEM((GROUP, 8, LANES), jnp.float32),
            dma((LOAD_SLOTS, 3, 5)),
            dma((SEND_SLOTS, 3)),
            dma((3, PIECES)),
            dma((3, PIECES)),
            dma((8, 3)),
            dma((8, 3)),
            dma((7, 3, PIECES)),
            dma((GROUP,)),
            dma((GROUP,)),
            dma((GROUP,)),
            dma((GROUP,)),
            dma(()),
        ],
        compiler_params=pltpu.CompilerParams(collective_id=0, has_side_effects=True),
    )(grad_attn, grad_mlp, grad_small)[:3]


def gather_kernel(part_sums, weight, update, small_weight, small_update,
                  all_attn, all_mlp, all_small, ratios,
                  fresh, fresh_small, slots,
                  tile_send, tile_recv, small_send, small_recv, own_send, link_send, link_recv, twin_send, twin_recv):
    me = lax.axis_index("data")
    twin = flip(me, CORE)
    meet_everyone(me)
    slots[me] = part_sums[...]
    tile_to_everyone(me, lambda owner: part_sums, slots, tile_send, tile_recv, True)
    tile_to_everyone(me, lambda owner: part_sums, slots, tile_send, tile_recv, False)
    sums = jnp.sum(slots[...], axis=0)
    lane = lax.broadcasted_iota(jnp.int32, (8, LANES), 1)

    def column(place):
        return jnp.sum(jnp.where(lane == place, sums, 0.0), axis=1, keepdims=True)

    def same_tensor(value, rows):
        total = value
        for shift in range(rows, 8, rows):
            total = total + pltpu.roll(value, shift, 0)
        return total

    def wide_rows(value):
        row = lax.broadcasted_iota(jnp.int32, (8, 1), 0)
        mine = jnp.logical_and(row >= 3, row < 6)
        return jnp.where(mine, jnp.sum(jnp.where(mine, value, 0.0), axis=0, keepdims=True), value)

    def spread(value):
        return jnp.broadcast_to(value, (8, LANES))

    def ratio(weights, updates):
        safe = jnp.where(updates > 0.0, updates, 1.0)
        return jnp.sqrt(weights) / jnp.sqrt(safe)

    ratio_attn = ratio(same_tensor(spread(column(0)), 4), same_tensor(spread(column(1)), 4))
    ratio_mlp = ratio(same_tensor(spread(column(2)), 2), same_tensor(spread(column(3)), 2))
    ratio_low = ratio(spread(column(4)), spread(column(5)))
    ratio_high = ratio(spread(wide_rows(column(6))), spread(wide_rows(column(7))))
    ratios[0] = ratio_attn
    ratios[1] = ratio_mlp
    ratios[2] = ratio_low
    ratios[3] = ratio_high

    def place_of(third, owner):
        if third == 0:
            return all_attn.at[owner]
        return all_mlp.at[owner, pl.ds((third - 1) * THIRD, THIRD)]

    def link(third, stage, hops, source=None):
        number = {0: 0, 1: 1, 2: 3}[stage] + {(): 0, (0,): 1, (1,): 2, (0, 1): 3}[hops]
        to = flip(me, ORDERS[third][stage])
        owner = flip_all(me, [ORDERS[third][hop] for hop in hops])
        place = place_of(third, owner)
        return pltpu.make_async_remote_copy(
            place if source is None else source, place, link_send.at[third, number], link_recv.at[third, number],
            device_id=(to,), device_id_type=MESH)

    def landed(third, stage, hops):
        number = {0: 0, 1: 1, 2: 3}[stage] + {(): 0, (0,): 1, (1,): 2, (0, 1): 3}[hops]
        owner = flip_all(flip(me, ORDERS[third][stage]), [ORDERS[third][hop] for hop in hops])
        place = place_of(third, owner)
        return pltpu.make_async_remote_copy(
            place, place, link_send.at[third, number], link_recv.at[third, number],
            device_id=(flip(me, ORDERS[third][stage]),), device_id_type=MESH)

    def to_twin(third, number, hops, source=None):
        owner = flip_all(me, [ORDERS[third][hop] for hop in hops])
        place = place_of(third, owner)
        return pltpu.make_async_remote_copy(
            place if source is None else source, place, twin_send.at[third, number], twin_recv.at[third, number],
            device_id=(twin,), device_id_type=MESH)

    def from_twin(third, number, hops):
        owner = flip_all(twin, [ORDERS[third][hop] for hop in hops])
        place = place_of(third, owner)
        return pltpu.make_async_remote_copy(
            place, place, twin_send.at[third, number], twin_recv.at[third, number],
            device_id=(twin,), device_id_type=MESH)

    own = []
    for third in range(3):
        scale = LEARN_RATE * (ratio_attn if third == 0 else ratio_mlp)

        def refresh(piece, carry, third=third, scale=scale):
            rows = pl.ds(pl.multiple_of(third * THIRD + piece * PIECE, PIECE), PIECE)
            old = weight[rows].reshape(PIECE // 8, 8, LANES)
            step = update[rows].reshape(PIECE // 8, 8, LANES)
            fresh[rows] = (old - scale[None] * step).reshape(PIECE, LANES).astype(jnp.bfloat16)
            return carry

        lax.fori_loop(0, PIECES, refresh, 0)
        source = fresh.at[pl.ds(third * THIRD, THIRD)]
        link(third, 0, (), source).start()
    for stage in (1, 2):
        for third in range(3):
            link(third, stage, (), fresh.at[pl.ds(third * THIRD, THIRD)]).start()
    for third in range(3):
        source = fresh.at[pl.ds(third * THIRD, THIRD)]
        to_twin(third, 0, (), source).start()
        copy = pltpu.make_async_copy(source, place_of(third, me), own_send.at[third])
        copy.start()
        own.append(copy)
    low = small_weight[0:8] - LEARN_RATE * ratio_low * small_update[0:8]
    high = small_weight[8:16] - LEARN_RATE * ratio_high * small_update[8:16]
    fresh_small[...] = jnp.concatenate([low, high], axis=0).astype(jnp.bfloat16)
    own_small = pltpu.make_async_copy(fresh_small, all_small.at[me], own_send.at[3])
    own_small.start()
    tile_to_everyone(me, lambda owner: fresh_small, all_small, small_send, small_recv, True)

    arrivals = (
        (0, (), ((1, (0,)), (2, (0,)))),
        (1, (), ((2, (1,)),)),
        (2, (), ()),
        (1, (0,), ((2, (0, 1)),)),
        (2, (0,), ()),
        (2, (1,), ()),
        (2, (0, 1), ()),
    )
    number = 1
    sent = []
    for stage, hops, forwards in arrivals:
        for third in range(3):
            landed(third, stage, hops).wait_recv()
            for forward in forwards:
                copy = link(third, *forward)
                copy.start()
                sent.append(copy)
            to_twin(third, number, (stage,) + hops).start()
        number += 1
    number = 0
    for hops in ((),) + tuple((stage,) + hops for stage, hops, _ in arrivals):
        for third in range(3):
            copy = from_twin(third, number, hops)
            copy.wait_recv()
            to_twin(third, number, hops).wait_send()
        number += 1
    for third in range(3):
        for stage in range(3):
            link(third, stage, ()).wait_send()
    for copy in sent:
        copy.wait_send()
    for copy in own:
        copy.wait()
    own_small.wait()
    tile_to_everyone(me, lambda owner: fresh_small, all_small, small_send, small_recv, False)


def all_gather(part_sums, weight, update, small_weight, small_update):
    anywhere = pl.BlockSpec(memory_space=pl.ANY)
    inside = pl.BlockSpec(memory_space=pltpu.VMEM)
    dma = pltpu.SemaphoreType.DMA
    rows = ATTN_ROWS + MLP_ROWS
    return pl.pallas_call(
        gather_kernel,
        name="gather",
        out_shape=(
            jax.ShapeDtypeStruct((GROUP, ATTN_ROWS, LANES), jnp.bfloat16),
            jax.ShapeDtypeStruct((GROUP, MLP_ROWS, LANES), jnp.bfloat16),
            jax.ShapeDtypeStruct((GROUP, SMALL_ROWS, LANES), jnp.bfloat16),
            jax.ShapeDtypeStruct((4, 8, LANES), jnp.float32),
        ),
        in_specs=[inside] * 5,
        out_specs=(anywhere, anywhere, anywhere, inside),
        scratch_shapes=[
            pltpu.VMEM((rows, LANES), jnp.bfloat16),
            pltpu.VMEM((SMALL_ROWS, LANES), jnp.bfloat16),
            pltpu.VMEM((GROUP, 8, LANES), jnp.float32),
            dma((GROUP,)), dma((GROUP,)), dma((GROUP,)), dma((GROUP,)),
            dma((4,)), dma((3, 7)), dma((3, 7)), dma((3, 8)), dma((3, 8)),
        ],
        compiler_params=pltpu.CompilerParams(collective_id=1, has_side_effects=True),
    )(part_sums, weight, update, small_weight, small_update)


def linear(bank):
    rows, length = bank.shape
    return bank.reshape(rows, length // LANES, LANES).transpose(1, 0, 2).reshape(rows * length // LANES, LANES)


def banked(flat, rows):
    blocks = flat.size // (rows * LANES)
    return flat.reshape(blocks, rows, LANES).transpose(1, 0, 2).reshape(rows, blocks * LANES)


def pack_small(wide, vec):
    lead = [(0, 0)] * (wide.ndim - 1)
    vec_rows = jnp.pad(vec, lead + [(0, 0), (0, LANES - 80)])
    wide_rows = jnp.pad(wide, lead + [(0, 64)]).reshape(wide.shape[:-1] + (3, LANES))
    return jnp.concatenate([vec_rows, jnp.pad(wide_rows, lead + [(0, 2), (0, 0)])], axis=-2)


def unpack_small(packed):
    lead = packed.shape[:-2]
    return packed[..., 11:14, :].reshape(lead + (3 * LANES,))[..., :320], packed[..., :11, :80]


def solution(mesh):
    grad_spec = P("data", None, None)
    shard_spec = P(None, "data")
    full_spec = P(None, None)

    def direction(mean_grad, weight, first, second, clip_coef):
        clipped = clip_coef * mean_grad
        new_first = BETA_FIRST * first + (1.0 - BETA_FIRST) * clipped
        new_second = BETA_SECOND * second + (1.0 - BETA_SECOND) * (clipped * clipped)
        update = (new_first / (1.0 - BETA_FIRST ** STEP_NUMBER)) / (jnp.sqrt(new_second / (1.0 - BETA_SECOND ** STEP_NUMBER)) + EPSILON) + WEIGHT_DECAY * weight
        return update, new_first, new_second

    def local_step(*banks):
        grads = banks[0:4]
        attn_grad = linear(grads[0][0]).reshape(GROUP, ATTN_ROWS, LANES)
        mlp_grad = linear(grads[1][0]).reshape(GROUP, MLP_ROWS, LANES)
        small_grad = pack_small(grads[2][0].reshape(GROUP, 320), grads[3][0].reshape(11, GROUP, 80).transpose(1, 0, 2))
        sums, small_sums, total = reduce_scatter(attn_grad, mlp_grad, small_grad)
        clip_coef = jnp.minimum(1.0, MAX_NORM / jnp.sqrt(total[0, 0]))
        states = []
        for first in (4, 8, 12):
            attn, mlp, wide, vec = banks[first:first + 4]
            states.append((jnp.concatenate([linear(attn), linear(mlp)], axis=0), pack_small(wide[0], vec)))
        (weight, small_weight), (first, small_first), (second, small_second) = states
        update, new_first, new_second = direction(sums, weight, first, second, clip_coef)
        small_update, small_new_first, small_new_second = direction(small_sums, small_weight, small_first, small_second, clip_coef)

        def tile_sum(value):
            return jnp.sum((value * value).reshape(-1, 8, LANES), axis=(0, 2))

        columns = [
            tile_sum(weight[:ATTN_ROWS]), tile_sum(update[:ATTN_ROWS]), tile_sum(weight[ATTN_ROWS:]), tile_sum(update[ATTN_ROWS:]),
            tile_sum(small_weight[:8]), tile_sum(small_update[:8]), tile_sum(small_weight[8:]), tile_sum(small_update[8:]),
        ]
        part_sums = jnp.pad(jnp.stack(columns, axis=1), ((0, 0), (0, LANES - 8)))
        all_attn, all_mlp, all_small, ratios = all_gather(part_sums, weight, update, small_weight, small_update)

        def stepped(weight, update, ratio):
            return (weight.reshape(-1, 8, LANES) - LEARN_RATE * ratio[None] * update.reshape(-1, 8, LANES)).reshape(weight.shape)

        new_attn = stepped(weight[:ATTN_ROWS], update[:ATTN_ROWS], ratios[0])
        new_mlp = stepped(weight[ATTN_ROWS:], update[ATTN_ROWS:], ratios[1])
        new_small = small_weight - LEARN_RATE * ratios[2:4].reshape(SMALL_ROWS, LANES) * small_update
        replica_wide, replica_vec = unpack_small(all_small)
        replicas = [
            banked(all_attn, 4), banked(all_mlp, 2), replica_wide.reshape(1, 5120),
            replica_vec.transpose(1, 0, 2).reshape(11, 1280),
        ]
        outs = list(replicas)
        for attn, mlp, small in (
            (new_attn, new_mlp, new_small),
            (new_first[:ATTN_ROWS], new_first[ATTN_ROWS:], small_new_first),
            (new_second[:ATTN_ROWS], new_second[ATTN_ROWS:], small_new_second),
        ):
            wide, vec = unpack_small(small)
            outs += [banked(attn, 4), banked(mlp, 2), wide[None], vec]
        return tuple(outs)

    return jax.shard_map(local_step, mesh=mesh, in_specs=(grad_spec,) * 4 + (shard_spec,) * 12, out_specs=(full_spec,) * 4 + (shard_spec,) * 12, check_vma=False)
```

```python
import functools

import jax
import jax.numpy as jnp
from jax import lax
from jax.experimental import pallas as pl
from jax.experimental.pallas import tpu as pltpu
from jax.sharding import PartitionSpec as P

STEP_NUMBER = 10
LEARN_RATE = 0.04
BETA_FIRST = 0.9
BETA_SECOND = 0.999
EPSILON = 1e-6
WEIGHT_DECAY = 0.01
MAX_NORM = 1.0

MESH = pl.DeviceIdType.MESH
GROUP = 16
LANES = 128
ATTN_ROWS = 3200
MLP_ROWS = 6400
ROWS = ATTN_ROWS + MLP_ROWS
THIRD = 3200
PIECE = 320
PIECES = THIRD // PIECE
LOAD_SLOTS = 3
SEND_SLOTS = 4
SMALL_ROWS = 16
BLOCK = 64
CHUNK = 640
CHUNKS = THIRD // CHUNK
OUT_SLOTS = 4
SCATTER_VMEM = 20 * 2 ** 20
UPDATE_VMEM = 8 * 2 ** 20
GATHER_VMEM = 2 * 2 ** 20
FINISH_VMEM = 3 * 2 ** 20
CORE = 1
ORDERS = ((2, 4, 8), (4, 8, 2), (8, 2, 4))
UNITS = (
    (0, (0, 1, 2), ()),
    (0, (0, 1), ()),
    (0, (0, 2), ()),
    (1, (1, 2), (0,)),
    (0, (0,), ()),
    (1, (1,), (1,)),
    (2, (2,), (2, 3)),
    (None, (), (4, 5, 6)),
)


def flip(index, width):
    return index + width * (1 - 2 * ((index // width) % 2))


def flip_all(index, widths):
    for width in widths:
        index = flip(index, width)
    return index


def meet_everyone(me):
    barrier = pltpu.get_barrier_semaphore()

    def signal(step, carry):
        pl.semaphore_signal(barrier, inc=1, device_id=((me + step) % GROUP,), device_id_type=MESH)
        return carry

    lax.fori_loop(1, GROUP, signal, 0)
    pl.semaphore_wait(barrier, GROUP - 1)


def tile_to_everyone(me, source_of, slots, send_sems, recv_sems, begin):
    def copy(step):
        return pltpu.make_async_remote_copy(
            source_of((me + step) % GROUP), slots.at[me], send_sems.at[step], recv_sems.at[step],
            device_id=((me + step) % GROUP,), device_id_type=MESH)

    def arrival(step):
        return pltpu.make_async_remote_copy(
            source_of((me + step) % GROUP), slots.at[(me - step + GROUP) % GROUP], send_sems.at[step], recv_sems.at[step],
            device_id=((me + step) % GROUP,), device_id_type=MESH)

    def start(step, carry):
        copy(step).start()
        return carry

    def finish(step, carry):
        arrival(step).wait()
        return carry

    lax.fori_loop(1, GROUP, start if begin else finish, 0)


def scatter_kernel(grad_attn, grad_mlp, grad_small, sums, small_sums, total, pair_raw, landed,
                   raw_own, raw_pair, partial, outgoing, square_sum, small_slots, square_slots,
                   load_sems, send_sems, pair_send_first, pair_recv_first, pair_send, pair_recv, land_sems,
                   small_send, small_recv, square_send, square_recv, local_sem):
    me = lax.axis_index("data")
    twin = flip(me, CORE)
    meet_everyone(me)

    def grad_of(third, owner, row, count):
        if third == 0:
            return grad_attn.at[owner, pl.ds(row, count)]
        return grad_mlp.at[owner, pl.ds(row + (third - 1) * THIRD, count)]

    def owner_of(unit, third):
        return flip_all(me, [ORDERS[third][place] for place in UNITS[unit][1]])

    def pair_first(third, piece):
        rows = piece * PIECE
        return pltpu.make_async_remote_copy(
            grad_of(third, flip(owner_of(0, third), CORE), rows, PIECE), pair_raw.at[0, third, pl.ds(rows, PIECE)],
            pair_send_first.at[third, piece], pair_recv_first.at[third, piece], device_id=(twin,), device_id_type=MESH)

    def pair_copy(unit, third):
        return pltpu.make_async_remote_copy(
            grad_of(third, flip(owner_of(unit, third), CORE), 0, THIRD), pair_raw.at[unit, third],
            pair_send.at[unit, third], pair_recv.at[unit, third], device_id=(twin,), device_id_type=MESH)

    def start_first(piece, carry):
        for third in range(3):
            pair_first(third, piece).start()
        return carry

    lax.fori_loop(0, PIECES, start_first, 0)
    for unit in range(1, 8):
        for third in range(3):
            pair_copy(unit, third).start()
    own_small = pltpu.make_async_copy(grad_small.at[me], small_slots.at[me], local_sem)
    own_small.start()
    tile_to_everyone(me, lambda owner: grad_small.at[owner], small_slots, small_send, small_recv, True)
    square_sum[...] = jnp.zeros_like(square_sum)

    def loads(unit, third, piece):
        rows = piece * PIECE
        slot = (unit * PIECES + piece) % LOAD_SLOTS
        copies = [
            pltpu.make_async_copy(grad_of(third, owner_of(unit, third), rows, PIECE), raw_own.at[slot, third], load_sems.at[slot, third, 0]),
            pltpu.make_async_copy(pair_raw.at[unit, third, pl.ds(rows, PIECE)], raw_pair.at[slot, third], load_sems.at[slot, third, 1]),
        ]
        for place, source in enumerate(UNITS[unit][2]):
            copies.append(pltpu.make_async_copy(
                landed.at[source, third, pl.ds(rows, PIECE)], partial.at[slot, third, place], load_sems.at[slot, third, 2 + place]))
        return copies

    def send(unit, third, piece):
        rows = piece * PIECE
        slot = (unit * PIECES + piece) % SEND_SLOTS
        to = flip(me, ORDERS[third][UNITS[unit][0]])
        return pltpu.make_async_remote_copy(
            outgoing.at[slot, third], landed.at[unit, third, pl.ds(rows, PIECE)],
            send_sems.at[slot, third], land_sems.at[unit, third, piece], device_id=(to,), device_id_type=MESH)

    def begin(unit, piece):
        for third in range(3):
            if unit == 0:
                pair_first(third, piece).wait_recv()
            else:
                @pl.when(piece == 0)
                def _():
                    pair_copy(unit, third).wait_recv()
            for source in UNITS[unit][2]:
                send(source, third, piece).wait_recv()
            for copy in loads(unit, third, piece):
                copy.start()

    ahead = LOAD_SLOTS - 1
    for piece in range(ahead):
        begin(0, piece)

    for unit in range(8):
        def work(piece, carry, unit=unit):
            @pl.when(piece + ahead < PIECES)
            def _():
                begin(unit, piece + ahead)
            if unit < 7:
                @pl.when(piece + ahead >= PIECES)
                def _():
                    begin(unit + 1, piece + ahead - PIECES)
            slot = (unit * PIECES + piece) % LOAD_SLOTS
            out_slot = (unit * PIECES + piece) % SEND_SLOTS
            for third in range(3):
                for copy in loads(unit, third, piece):
                    copy.wait()
                value = raw_own[slot, third].astype(jnp.float32) + raw_pair[slot, third].astype(jnp.float32)
                for place in range(len(UNITS[unit][2])):
                    value = value + partial[slot, third, place]
                if unit < 7:
                    if unit == 0:
                        @pl.when(piece >= SEND_SLOTS)
                        def _():
                            send(unit, third, piece).wait_send()
                    else:
                        send(unit, third, piece).wait_send()
                    outgoing[out_slot, third] = value
                    send(unit, third, piece).start()
                else:
                    value = value * (1.0 / GROUP)
                    sums[pl.ds(pl.multiple_of(third * THIRD + piece * PIECE, PIECE), PIECE)] = value
                    square_sum[...] += jnp.sum((value * value).reshape(PIECE // 8, 8, LANES), axis=0)
            return carry

        lax.fori_loop(0, PIECES, work, 0)

    own_small.wait()
    tile_to_everyone(me, lambda owner: grad_small.at[owner], small_slots, small_send, small_recv, False)
    small = jnp.sum(small_slots[...].astype(jnp.float32), axis=0) * (1.0 / GROUP)
    small_sums[...] = small
    squares = square_sum[...] + (small * small)[0:8] + (small * small)[8:16]
    square_sum[...] = squares
    square_slots[me] = squares
    tile_to_everyone(me, lambda owner: square_sum, square_slots, square_send, square_recv, True)
    for slot in range(SEND_SLOTS):
        for third in range(3):
            send(6, third, slot).wait_send()

    def drain(piece, carry):
        for third in range(3):
            pair_first(third, piece).wait_send()
        return carry

    lax.fori_loop(0, PIECES, drain, 0)
    for unit in range(1, 8):
        for third in range(3):
            pair_copy(unit, third).wait_send()
    tile_to_everyone(me, lambda owner: square_sum, square_slots, square_send, square_recv, False)
    total[...] = jnp.full((8, LANES), jnp.sum(square_slots[...]), jnp.float32)


def reduce_scatter(grad_attn, grad_mlp, grad_small):
    anywhere = pl.BlockSpec(memory_space=pl.ANY)
    inside = pl.BlockSpec(memory_space=pltpu.VMEM)
    dma = pltpu.SemaphoreType.DMA
    return pl.pallas_call(
        scatter_kernel,
        name="scatter",
        out_shape=(
            pltpu.VMEM((ROWS, LANES), jnp.float32),
            pltpu.VMEM((SMALL_ROWS, LANES), jnp.float32),
            pltpu.VMEM((8, LANES), jnp.float32),
            pltpu.HBM((8, 3, THIRD, LANES), jnp.bfloat16),
            pltpu.HBM((7, 3, THIRD, LANES), jnp.float32),
        ),
        in_specs=[anywhere] * 3,
        out_specs=(inside, inside, inside, anywhere, anywhere),
        scratch_shapes=[
            pltpu.VMEM((LOAD_SLOTS, 3, PIECE, LANES), jnp.bfloat16),
            pltpu.VMEM((LOAD_SLOTS, 3, PIECE, LANES), jnp.bfloat16),
            pltpu.VMEM((LOAD_SLOTS, 3, 3, PIECE, LANES), jnp.float32),
            pltpu.VMEM((SEND_SLOTS, 3, PIECE, LANES), jnp.float32),
            pltpu.VMEM((8, LANES), jnp.float32),
            pltpu.VMEM((GROUP, SMALL_ROWS, LANES), jnp.bfloat16),
            pltpu.VMEM((GROUP, 8, LANES), jnp.float32),
            dma((LOAD_SLOTS, 3, 5)),
            dma((SEND_SLOTS, 3)),
            dma((3, PIECES)),
            dma((3, PIECES)),
            dma((8, 3)),
            dma((8, 3)),
            dma((7, 3, PIECES)),
            dma((GROUP,)),
            dma((GROUP,)),
            dma((GROUP,)),
            dma((GROUP,)),
            dma(()),
        ],
        compiler_params=pltpu.CompilerParams(collective_id=0, has_side_effects=True, vmem_limit_bytes=SCATTER_VMEM),
    )(*[pltpu.with_memory_space_constraint(grad, pltpu.HBM) for grad in (grad_attn, grad_mlp)], grad_small)[:3]


def bank_part(third, attn, mlp):
    return (attn, 0) if third == 0 else (mlp, (third - 1) * THIRD)


def update_kernel(sums, small_sums, total, weight_attn, weight_mlp, first_attn, first_mlp, second_attn, second_mlp,
                  small_weight, small_first, small_second,
                  update, small_update, part_sums, new_first_attn, new_first_mlp, new_second_attn, new_second_mlp,
                  small_new_first, small_new_second,
                  first_out, second_out, out_sems):
    clip_coef = jnp.minimum(1.0, MAX_NORM / jnp.sqrt(total[0:1, :]))

    def direction(mean_grad, weight, first, second):
        clipped = clip_coef * mean_grad
        new_first = BETA_FIRST * first + (1.0 - BETA_FIRST) * clipped
        new_second = BETA_SECOND * second + (1.0 - BETA_SECOND) * (clipped * clipped)
        root = jnp.sqrt(new_second * (1.0 / (1.0 - BETA_SECOND ** STEP_NUMBER))) + EPSILON
        return (new_first * (1.0 / (1.0 - BETA_FIRST ** STEP_NUMBER))) / root + WEIGHT_DECAY * weight, new_first, new_second

    def tile_sum(value):
        return jnp.sum((value * value).reshape(-1, 8, LANES), axis=0)

    def copies(third, chunk):
        slot = (third * CHUNKS + chunk) % OUT_SLOTS
        first_to, base = bank_part(third, new_first_attn, new_first_mlp)
        second_to, _ = bank_part(third, new_second_attn, new_second_mlp)
        rows = pl.ds(base + chunk * CHUNK, CHUNK)
        return (
            pltpu.make_async_copy(first_out.at[slot], first_to.at[rows], out_sems.at[slot, 0]),
            pltpu.make_async_copy(second_out.at[slot], second_to.at[rows], out_sems.at[slot, 1]),
        )

    totals = []
    for third in range(3):
        weight, base = bank_part(third, weight_attn, weight_mlp)
        first, _ = bank_part(third, first_attn, first_mlp)
        second, _ = bank_part(third, second_attn, second_mlp)

        def work(chunk, carry, third=third, weight=weight, first=first, second=second, base=base):
            slot = (third * CHUNKS + chunk) % OUT_SLOTS
            place = third * CHUNKS + chunk

            @pl.when(place >= OUT_SLOTS)
            def _():
                for copy in copies(third, chunk):
                    copy.wait()

            def block(step, carry):
                squares_weight, squares_update = carry
                inner = pl.multiple_of(step * BLOCK, BLOCK)
                rows = pl.ds(pl.multiple_of(base + chunk * CHUNK + inner, BLOCK), BLOCK)
                old = weight[rows]
                new_update, new_first, new_second = direction(
                    sums[pl.ds(pl.multiple_of(third * THIRD + chunk * CHUNK + inner, BLOCK), BLOCK)], old, first[rows], second[rows])
                first_out[slot, pl.ds(inner, BLOCK)] = new_first
                second_out[slot, pl.ds(inner, BLOCK)] = new_second
                update[pl.ds(pl.multiple_of(third * THIRD + chunk * CHUNK + inner, BLOCK), BLOCK)] = new_update
                return squares_weight + tile_sum(old), squares_update + tile_sum(new_update)

            carry = lax.fori_loop(0, CHUNK // BLOCK, block, carry)
            for copy in copies(third, chunk):
                copy.start()
            return carry

        zero = jnp.zeros((8, LANES), jnp.float32)
        totals.append(lax.fori_loop(0, CHUNKS, work, (zero, zero)))
    small, small_m, small_v = direction(small_sums[...], small_weight[...], small_first[...], small_second[...])
    small_update[...] = small
    small_new_first[...] = small_m
    small_new_second[...] = small_v
    old = small_weight[...]
    columns = [
        totals[0][0], totals[0][1], totals[1][0] + totals[2][0], totals[1][1] + totals[2][1],
        (old * old)[0:8], (small * small)[0:8], (old * old)[8:16], (small * small)[8:16],
    ]
    lane = lax.broadcasted_iota(jnp.int32, (8, LANES), 1)
    tile = jnp.zeros((8, LANES), jnp.float32)
    for place, column in enumerate(columns):
        tile = jnp.where(lane == place, jnp.sum(column, axis=1, keepdims=True), tile)
    part_sums[...] = tile
    for place in range(3 * CHUNKS - OUT_SLOTS, 3 * CHUNKS):
        for copy in copies(place // CHUNKS, place % CHUNKS):
            copy.wait()


def resident(value):
    return pltpu.with_memory_space_constraint(value, pltpu.VMEM)


def update_step(sums, small_sums, total, weights, firsts, seconds, smalls):
    anywhere = pl.BlockSpec(memory_space=pl.ANY)
    inside = pl.BlockSpec(memory_space=pltpu.VMEM)
    attn = pltpu.HBM((ATTN_ROWS, LANES), jnp.float32)
    mlp = pltpu.HBM((MLP_ROWS, LANES), jnp.float32)
    small = jax.ShapeDtypeStruct((SMALL_ROWS, LANES), jnp.float32)
    operands = [sums, small_sums, total, *weights, *firsts, *seconds]
    return pl.pallas_call(
        update_kernel,
        name="update",
        out_shape=(
            pltpu.VMEM((ROWS, LANES), jnp.float32),
            pltpu.VMEM((SMALL_ROWS, LANES), jnp.float32),
            pltpu.VMEM((8, LANES), jnp.float32),
            attn, mlp, attn, mlp, small, small,
        ),
        in_specs=[inside] * 12,
        out_specs=(inside, inside, inside, anywhere, anywhere, anywhere, anywhere, inside, inside),
        scratch_shapes=[
            pltpu.VMEM((OUT_SLOTS, CHUNK, LANES), jnp.float32),
            pltpu.VMEM((OUT_SLOTS, CHUNK, LANES), jnp.float32),
            pltpu.SemaphoreType.DMA((OUT_SLOTS, 2)),
        ],
        compiler_params=pltpu.CompilerParams(vmem_limit_bytes=UPDATE_VMEM),
    )(*[resident(value) for value in operands], *smalls)


def gather_kernel(part_sums, weight_attn, weight_mlp, update, small_weight, small_update,
                  everything, all_small, ratios,
                  fresh_small, slots,
                  tile_send, tile_recv, small_send, small_recv, own_send, link_send, link_recv, twin_send, twin_recv):
    me = lax.axis_index("data")
    twin = flip(me, CORE)
    meet_everyone(me)
    slots[me] = part_sums[...]
    tile_to_everyone(me, lambda owner: part_sums, slots, tile_send, tile_recv, True)
    tile_to_everyone(me, lambda owner: part_sums, slots, tile_send, tile_recv, False)
    sums = jnp.sum(slots[...], axis=0)
    lane = lax.broadcasted_iota(jnp.int32, (8, LANES), 1)

    def column(place):
        return jnp.sum(jnp.where(lane == place, sums, 0.0), axis=1, keepdims=True)

    def same_tensor(value, rows):
        total = value
        for shift in range(rows, 8, rows):
            total = total + pltpu.roll(value, shift, 0)
        return total

    def wide_rows(value):
        row = lax.broadcasted_iota(jnp.int32, (8, 1), 0)
        mine = jnp.logical_and(row >= 3, row < 6)
        return jnp.where(mine, jnp.sum(jnp.where(mine, value, 0.0), axis=0, keepdims=True), value)

    def spread(value):
        return jnp.broadcast_to(value, (8, LANES))

    def ratio(weights, updates):
        safe = jnp.where(updates > 0.0, updates, 1.0)
        return jnp.sqrt(weights) / jnp.sqrt(safe)

    ratio_attn = ratio(same_tensor(spread(column(0)), 4), same_tensor(spread(column(1)), 4))
    ratio_mlp = ratio(same_tensor(spread(column(2)), 2), same_tensor(spread(column(3)), 2))
    ratio_low = ratio(spread(column(4)), spread(column(5)))
    ratio_high = ratio(spread(wide_rows(column(6))), spread(wide_rows(column(7))))
    ratios[0] = ratio_attn
    ratios[1] = ratio_mlp
    ratios[2] = ratio_low
    ratios[3] = ratio_high

    def place_of(third, owner):
        return everything.at[owner, pl.ds(third * THIRD, THIRD)]

    def link(third, stage, hops):
        number = {0: 0, 1: 1, 2: 3}[stage] + {(): 0, (0,): 1, (1,): 2, (0, 1): 3}[hops]
        to = flip(me, ORDERS[third][stage])
        owner = flip_all(me, [ORDERS[third][hop] for hop in hops])
        place = place_of(third, owner)
        return pltpu.make_async_remote_copy(
            place, place, link_send.at[third, number], link_recv.at[third, number],
            device_id=(to,), device_id_type=MESH)

    def landed(third, stage, hops):
        number = {0: 0, 1: 1, 2: 3}[stage] + {(): 0, (0,): 1, (1,): 2, (0, 1): 3}[hops]
        owner = flip_all(flip(me, ORDERS[third][stage]), [ORDERS[third][hop] for hop in hops])
        place = place_of(third, owner)
        return pltpu.make_async_remote_copy(
            place, place, link_send.at[third, number], link_recv.at[third, number],
            device_id=(flip(me, ORDERS[third][stage]),), device_id_type=MESH)

    def to_twin(third, number, hops):
        owner = flip_all(me, [ORDERS[third][hop] for hop in hops])
        place = place_of(third, owner)
        return pltpu.make_async_remote_copy(
            place, place, twin_send.at[third, number], twin_recv.at[third, number],
            device_id=(twin,), device_id_type=MESH)

    def from_twin(third, number, hops):
        owner = flip_all(twin, [ORDERS[third][hop] for hop in hops])
        place = place_of(third, owner)
        return pltpu.make_async_remote_copy(
            place, place, twin_send.at[third, number], twin_recv.at[third, number],
            device_id=(twin,), device_id_type=MESH)

    for third in range(3):
        scale = LEARN_RATE * (ratio_attn if third == 0 else ratio_mlp)
        weight, base = bank_part(third, weight_attn, weight_mlp)

        def refresh(piece, carry, third=third, scale=scale, weight=weight, base=base):
            rows = pl.ds(pl.multiple_of(third * THIRD + piece * PIECE, PIECE), PIECE)
            old = weight[pl.ds(pl.multiple_of(base + piece * PIECE, PIECE), PIECE)].reshape(PIECE // 8, 8, LANES)
            step = update[rows].reshape(PIECE // 8, 8, LANES)
            everything[me, rows] = (old - scale[None] * step).reshape(PIECE, LANES).astype(jnp.bfloat16)
            return carry

        lax.fori_loop(0, PIECES, refresh, 0)
        link(third, 0, ()).start()
    for stage in (1, 2):
        for third in range(3):
            link(third, stage, ()).start()
    for third in range(3):
        to_twin(third, 0, ()).start()
    low = small_weight[0:8] - LEARN_RATE * ratio_low * small_update[0:8]
    high = small_weight[8:16] - LEARN_RATE * ratio_high * small_update[8:16]
    fresh_small[...] = jnp.concatenate([low, high], axis=0).astype(jnp.bfloat16)
    own_small = pltpu.make_async_copy(fresh_small, all_small.at[me], own_send)
    own_small.start()
    tile_to_everyone(me, lambda owner: fresh_small, all_small, small_send, small_recv, True)

    arrivals = (
        (0, (), ((1, (0,)), (2, (0,)))),
        (1, (), ((2, (1,)),)),
        (2, (), ()),
        (1, (0,), ((2, (0, 1)),)),
        (2, (0,), ()),
        (2, (1,), ()),
        (2, (0, 1), ()),
    )
    number = 1
    sent = []
    for stage, hops, forwards in arrivals:
        for third in range(3):
            landed(third, stage, hops).wait_recv()
            for forward in forwards:
                copy = link(third, *forward)
                copy.start()
                sent.append(copy)
            to_twin(third, number, (stage,) + hops).start()
        number += 1
    number = 0
    for hops in ((),) + tuple((stage,) + hops for stage, hops, _ in arrivals):
        for third in range(3):
            copy = from_twin(third, number, hops)
            copy.wait_recv()
            to_twin(third, number, hops).wait_send()
        number += 1
    for third in range(3):
        for stage in range(3):
            link(third, stage, ()).wait_send()
    for copy in sent:
        copy.wait_send()
    own_small.wait()
    tile_to_everyone(me, lambda owner: fresh_small, all_small, small_send, small_recv, False)


def all_gather(part_sums, weights, update, small_weight, small_update):
    inside = pl.BlockSpec(memory_space=pltpu.VMEM)
    dma = pltpu.SemaphoreType.DMA
    return pl.pallas_call(
        gather_kernel,
        name="gather",
        out_shape=(
            pltpu.VMEM((GROUP, ROWS, LANES), jnp.bfloat16),
            pltpu.VMEM((GROUP, SMALL_ROWS, LANES), jnp.bfloat16),
            pltpu.VMEM((4, 8, LANES), jnp.float32),
        ),
        in_specs=[inside] * 6,
        out_specs=(inside,) * 3,
        scratch_shapes=[
            pltpu.VMEM((SMALL_ROWS, LANES), jnp.bfloat16),
            pltpu.VMEM((GROUP, 8, LANES), jnp.float32),
            dma((GROUP,)), dma((GROUP,)), dma((GROUP,)), dma((GROUP,)),
            dma(()), dma((3, 7)), dma((3, 7)), dma((3, 8)), dma((3, 8)),
        ],
        compiler_params=pltpu.CompilerParams(collective_id=1, has_side_effects=True, vmem_limit_bytes=GATHER_VMEM),
    )(*[resident(value) for value in (part_sums, *weights, update)], small_weight, small_update)


def write_kernel(everything, replica_attn, replica_mlp, attn_sems, mlp_sems):
    writes = []
    for owner in range(GROUP):
        writes.append(pltpu.make_async_copy(
            everything.at[owner, pl.ds(0, ATTN_ROWS)], replica_attn.at[pl.ds(owner * ATTN_ROWS, ATTN_ROWS)], attn_sems.at[owner]))
        writes.append(pltpu.make_async_copy(
            everything.at[owner, pl.ds(ATTN_ROWS, MLP_ROWS)], replica_mlp.at[pl.ds(owner * MLP_ROWS, MLP_ROWS)], mlp_sems.at[owner]))
    for copy in writes:
        copy.start()
    for copy in writes:
        copy.wait()


def write_replica(everything):
    anywhere = pl.BlockSpec(memory_space=pl.ANY)
    dma = pltpu.SemaphoreType.DMA
    return pl.pallas_call(
        write_kernel,
        name="write",
        out_shape=(
            pltpu.HBM((GROUP * ATTN_ROWS, LANES), jnp.bfloat16),
            pltpu.HBM((GROUP * MLP_ROWS, LANES), jnp.bfloat16),
        ),
        in_specs=[pl.BlockSpec(memory_space=pltpu.VMEM)],
        out_specs=(anywhere,) * 2,
        scratch_shapes=[dma((GROUP,)), dma((GROUP,))],
        compiler_params=pltpu.CompilerParams(vmem_limit_bytes=FINISH_VMEM),
    )(resident(everything))


def finish_kernel(weight_attn, weight_mlp, update, ratios, all_small, small_weight, small_update,
                  new_attn, new_mlp, replica_small, new_small,
                  fresh, fresh_small, weight_sems, small_sems):
    writes = []
    for tile in range(2):
        rows = pl.ds(8 * tile, 8)
        fresh_small[rows] = small_weight[rows] - LEARN_RATE * ratios[2 + tile] * small_update[rows]
    for place, (source, to) in enumerate(((all_small, replica_small), (fresh_small, new_small))):
        copy = pltpu.make_async_copy(source, to, small_sems.at[place])
        copy.start()
        writes.append(copy)
    def write(third, chunk):
        slot = (third * CHUNKS + chunk) % OUT_SLOTS
        to, base = bank_part(third, new_attn, new_mlp)
        return pltpu.make_async_copy(fresh.at[slot], to.at[pl.ds(base + chunk * CHUNK, CHUNK)], weight_sems.at[slot])

    for third in range(3):
        scale = LEARN_RATE * ratios[0 if third == 0 else 1]
        weight, base = bank_part(third, weight_attn, weight_mlp)

        def work(chunk, carry, third=third, scale=scale, weight=weight, base=base):
            slot = (third * CHUNKS + chunk) % OUT_SLOTS

            @pl.when(third * CHUNKS + chunk >= OUT_SLOTS)
            def _():
                write(third, chunk).wait()

            def refresh(block, inner):
                start = chunk * CHUNK + block * BLOCK
                old = weight[pl.ds(pl.multiple_of(base + start, BLOCK), BLOCK)].reshape(BLOCK // 8, 8, LANES)
                step = update[pl.ds(pl.multiple_of(third * THIRD + start, BLOCK), BLOCK)].reshape(BLOCK // 8, 8, LANES)
                fresh[slot, pl.ds(pl.multiple_of(block * BLOCK, BLOCK), BLOCK)] = (old - scale[None] * step).reshape(BLOCK, LANES)
                return inner

            lax.fori_loop(0, CHUNK // BLOCK, refresh, 0)
            write(third, chunk).start()
            return carry

        lax.fori_loop(0, CHUNKS, work, 0)
    for place in range(3 * CHUNKS - OUT_SLOTS, 3 * CHUNKS):
        write(place // CHUNKS, place % CHUNKS).wait()
    for copy in writes:
        copy.wait()


def finish(all_small, weights, update, small_weight, small_update, ratios):
    anywhere = pl.BlockSpec(memory_space=pl.ANY)
    inside = pl.BlockSpec(memory_space=pltpu.VMEM)
    dma = pltpu.SemaphoreType.DMA
    return pl.pallas_call(
        finish_kernel,
        name="finish",
        out_shape=(
            pltpu.HBM((ATTN_ROWS, LANES), jnp.float32),
            pltpu.HBM((MLP_ROWS, LANES), jnp.float32),
            pltpu.HBM((GROUP, SMALL_ROWS, LANES), jnp.bfloat16),
            pltpu.HBM((SMALL_ROWS, LANES), jnp.float32),
        ),
        in_specs=[inside] * 7,
        out_specs=(anywhere,) * 4,
        scratch_shapes=[
            pltpu.VMEM((OUT_SLOTS, CHUNK, LANES), jnp.float32), pltpu.VMEM((SMALL_ROWS, LANES), jnp.float32),
            dma((OUT_SLOTS,)), dma((2,)),
        ],
        compiler_params=pltpu.CompilerParams(vmem_limit_bytes=FINISH_VMEM),
    )(*[resident(value) for value in (*weights, update, ratios, all_small)], small_weight, small_update)


def linear(bank):
    rows, length = bank.shape
    return bank.reshape(rows, length // LANES, LANES).transpose(1, 0, 2).reshape(rows * length // LANES, LANES)


def banked(flat, rows):
    blocks = flat.size // (rows * LANES)
    return flat.reshape(blocks, rows, LANES).transpose(1, 0, 2).reshape(rows, blocks * LANES)


def pack_small(wide, vec):
    lead = [(0, 0)] * (wide.ndim - 1)
    vec_rows = jnp.pad(vec, lead + [(0, 0), (0, LANES - 80)])
    wide_rows = jnp.pad(wide, lead + [(0, 64)]).reshape(wide.shape[:-1] + (3, LANES))
    return jnp.concatenate([vec_rows, jnp.pad(wide_rows, lead + [(0, 2), (0, 0)])], axis=-2)


def unpack_small(packed):
    lead = packed.shape[:-2]
    return packed[..., 11:14, :].reshape(lead + (3 * LANES,))[..., :320], packed[..., :11, :80]


def solution(mesh):
    grad_spec = P("data", None, None)
    shard_spec = P(None, "data")
    full_spec = P(None, None)

    def local_step(*banks):
        grads = banks[0:4]
        attn_grad = linear(grads[0][0]).reshape(GROUP, ATTN_ROWS, LANES)
        mlp_grad = linear(grads[1][0]).reshape(GROUP, MLP_ROWS, LANES)
        small_grad = pack_small(grads[2][0].reshape(GROUP, 320), grads[3][0].reshape(11, GROUP, 80).transpose(1, 0, 2))
        states, smalls = [], []
        for first in (4, 8, 12):
            attn, mlp, wide, vec = banks[first:first + 4]
            states.append((linear(attn), linear(mlp)))
            smalls.append(pack_small(wide[0], vec))
        small_grad, *smalls = lax.optimization_barrier((small_grad, *smalls))
        sums, small_sums, total = reduce_scatter(attn_grad, mlp_grad, small_grad)
        update, small_update, part_sums, *moments = update_step(sums, small_sums, total, *states, smalls)
        everything, all_small, ratios = all_gather(part_sums, states[0], update, smalls[0], small_update)
        replica_attn, replica_mlp = write_replica(everything)
        replica_attn, all_small = lax.optimization_barrier((replica_attn, all_small))
        new_attn, new_mlp, all_small, new_small = finish(
            all_small, states[0], update, smalls[0], small_update, ratios)
        replica_wide, replica_vec = unpack_small(all_small)
        outs = [
            banked(replica_attn, 4), banked(replica_mlp, 2), replica_wide.reshape(1, 5120),
            replica_vec.transpose(1, 0, 2).reshape(11, 1280),
        ]
        for attn, mlp, small in (
            (new_attn, new_mlp, new_small),
            (moments[0], moments[1], moments[4]),
            (moments[2], moments[3], moments[5]),
        ):
            wide, vec = unpack_small(small)
            outs += [banked(attn, 4), banked(mlp, 2), wide[None], vec]
        return tuple(outs)

    return jax.shard_map(local_step, mesh=mesh, in_specs=(grad_spec,) * 4 + (shard_spec,) * 12, out_specs=(full_spec,) * 4 + (shard_spec,) * 12, check_vma=False)
```

```python
import functools

import jax
import jax.numpy as jnp
from jax import lax
from jax.experimental import pallas as pl
from jax.experimental.pallas import tpu as pltpu
from jax.sharding import PartitionSpec as P

STEP_NUMBER = 10
LEARN_RATE = 0.04
BETA_FIRST = 0.9
BETA_SECOND = 0.999
EPSILON = 1e-6
WEIGHT_DECAY = 0.01
MAX_NORM = 1.0

MESH = pl.DeviceIdType.MESH
GROUP = 16
LANES = 128
TILE = (8, LANES)
THIRDS = range(3)
VECS = 11
VEC_SHARE = 80
VEC = 1280
WIDE = 5120
WIDE_PARTS = ((0, LANES), (1, LANES), (2, 64))
WIDE_SHARE = 320
MIB = 2 ** 20
ATTN_ROWS = 3200
MLP_ROWS = 6400
ROWS = ATTN_ROWS + MLP_ROWS
THIRD = 3200
PIECE = 320
PIECES = THIRD // PIECE
LOAD_SLOTS = 3
SEND_SLOTS = 4
SMALL_ROWS = 16
BLOCK = 64
PARTS = 4
LAST = THIRD // PARTS
CHUNK = 640
CHUNKS = THIRD // CHUNK
OUT_SLOTS = 4
SCATTER_VMEM = 30 * MIB
UPDATE_VMEM = 8 * MIB
GATHER_VMEM = 2 * MIB
FINISH_VMEM = 3 * MIB
CORE = 1
ORDERS = ((2, 4, 8), (4, 8, 2), (8, 2, 4))
UNITS = (
    (0, (0, 1, 2), ()),
    (0, (0, 1), ()),
    (0, (0, 2), ()),
    (1, (1, 2), (0,)),
    (0, (0,), ()),
    (1, (1,), (1,)),
    (2, (2,), (2, 3)),
    (None, (), (4, 5, 6)),
)


ARRIVALS = [(0, ()), (1, ()), (2, ()), (1, (0,)), (2, (0,)), (2, (1,))]


def flip(index, width):
    return index + width * (1 - 2 * ((index // width) % 2))


def flip_all(index, widths):
    for width in widths:
        index = flip(index, width)
    return index


def meet_everyone(me):
    barrier = pltpu.get_barrier_semaphore()

    def signal(step, carry):
        pl.semaphore_signal(barrier, inc=1, device_id=((me + step) % GROUP,), device_id_type=MESH)
        return carry

    lax.fori_loop(1, GROUP, signal, 0)
    pl.semaphore_wait(barrier, GROUP - 1)


def tile_to_everyone(me, source_of, slots, send_sems, recv_sems, begin):
    def copy(step):
        return pltpu.make_async_remote_copy(
            source_of((me + step) % GROUP), slots.at[me], send_sems.at[step], recv_sems.at[step],
            device_id=((me + step) % GROUP,), device_id_type=MESH)

    def arrival(step):
        return pltpu.make_async_remote_copy(
            source_of((me + step) % GROUP), slots.at[(me - step + GROUP) % GROUP], send_sems.at[step], recv_sems.at[step],
            device_id=((me + step) % GROUP,), device_id_type=MESH)

    def start(step, carry):
        copy(step).start()
        return carry

    def finish(step, carry):
        arrival(step).wait()
        return carry

    lax.fori_loop(1, GROUP, start if begin else finish, 0)


def small_places(packed, wide, vec):
    places = [(packed.at[pl.ds(0, VECS), pl.ds(0, VEC_SHARE)], vec)]
    for part, width in WIDE_PARTS:
        places.append((packed.at[pl.ds(VECS + part, 1), pl.ds(0, width)], wide.at[:, pl.ds(LANES * part, width)]))
    return places


def pack_rows(wide, vec, packed):
    packed[...] = jnp.zeros_like(packed)
    for inner, outer in small_places(packed, wide, vec):
        inner[...] = outer[...]


def unpack_rows(packed, wide, vec):
    for inner, outer in small_places(packed, wide, vec):
        outer[...] = inner[...]


def shares_from(wide, vec, wide_rows, vec_rows, packed):
    wide_rows[...] = jnp.zeros_like(wide_rows)
    wide_rows[:1] = wide[...].astype(jnp.float32)
    vec_rows[...] = jnp.zeros_like(vec_rows)
    vec_rows[:VECS] = vec[...].astype(jnp.float32)
    packed[...] = jnp.zeros_like(packed)

    def window(rows, start):
        block, shift = start // LANES * LANES, start % LANES
        value = rows[:, block:block + LANES]
        if shift == 0:
            return value
        lane = lax.broadcasted_iota(jnp.int32, value.shape, 1)
        value = pltpu.roll(value, LANES - shift, 1)
        if block + LANES == rows.shape[1]:
            return value
        after = pltpu.roll(rows[:, block + LANES:block + 2 * LANES], LANES - shift, 1)
        return jnp.where(lane < LANES - shift, value, after)

    lane = lax.broadcasted_iota(jnp.int32, (SMALL_ROWS, LANES), 1)
    for owner in range(GROUP):
        packed[owner] = jnp.where(lane < VEC_SHARE, window(vec_rows, VEC_SHARE * owner), 0.0)
        for part, width in WIDE_PARTS:
            value = window(wide_rows, WIDE_SHARE * owner + LANES * part)
            packed[owner, pl.ds(VECS + part, 1)] = jnp.where(lane[:1] < width, value[:1], 0.0)


def shares_to(shares, wide, vec, wide_rows, pair):
    lane = lax.broadcasted_iota(jnp.int32, (SMALL_ROWS, LANES), 1)
    low = lax.broadcasted_iota(jnp.int32, (1, LANES), 1) < 64
    for block in range(VEC // LANES):
        value = jnp.zeros((SMALL_ROWS, LANES), jnp.float32)
        for owner in range(GROUP):
            begin, end = max(VEC_SHARE * owner, LANES * block), min(VEC_SHARE * (owner + 1), LANES * (block + 1))
            if begin < end:
                shift = (VEC_SHARE * owner - LANES * block) % LANES
                moved = shares[owner].astype(jnp.float32)
                if shift:
                    moved = pltpu.roll(moved, shift, 1)
                inside = jnp.logical_and(lane >= begin - LANES * block, lane < end - LANES * block)
                value = jnp.where(inside, moved, value)
        vec[:, LANES * block:LANES * (block + 1)] = value[:VECS].astype(jnp.bfloat16)
    for place in range(GROUP // 2):
        pair[0] = shares[2 * place].astype(jnp.float32)
        pair[1] = pltpu.roll(shares[2 * place + 1].astype(jnp.float32), 64, 1)
        even, odd = [[pair[half, pl.ds(VECS + part, 1)] for part, _ in WIDE_PARTS] for half in range(2)]
        blocks = [
            even[0], even[1], jnp.where(low, even[2], odd[0]), jnp.where(low, odd[0], odd[1]), jnp.where(low, odd[1], odd[2]),
        ]
        for number, value in enumerate(blocks):
            wide_rows[:1, pl.ds(LANES * (len(blocks) * place + number), LANES)] = value
    wide[...] = wide_rows[:1].astype(jnp.bfloat16)


def scatter_kernel(grad_attn, grad_mlp, grad_wide, grad_vec, sums, small_sums, total, pair_raw, landed,
                   raw_own, raw_pair, partial, outgoing, square_sum, small_slots, square_slots,
                   pair_near, landed_near, wide_raw, vec_raw, wide_rows, vec_rows, packed, small_shares,
                   load_sems, send_sems, pair_send_first, pair_recv_first, pair_send, pair_recv, land_sems,
                   small_send, small_recv, square_send, square_recv, local_sems):
    me = lax.axis_index("data")
    twin = flip(me, CORE)
    meet_everyone(me)

    def grad_of(third, owner, row, count):
        if third == 0:
            return grad_attn.at[owner, pl.ds(row, count)]
        return grad_mlp.at[owner, pl.ds(row + (third - 1) * THIRD, count)]

    def owner_of(unit, third):
        return flip_all(me, [ORDERS[third][place] for place in UNITS[unit][1]])

    def pair_first(third, piece):
        rows = piece * PIECE
        return pltpu.make_async_remote_copy(
            grad_of(third, flip(owner_of(0, third), CORE), rows, PIECE), pair_near.at[third, pl.ds(rows, PIECE)],
            pair_send_first.at[third, piece], pair_recv_first.at[third, piece], device_id=(twin,), device_id_type=MESH)

    def pair_copy(unit, third):
        return pltpu.make_async_remote_copy(
            grad_of(third, flip(owner_of(unit, third), CORE), 0, THIRD), pair_raw.at[unit - 1, third],
            pair_send.at[unit, third], pair_recv.at[unit, third], device_id=(twin,), device_id_type=MESH)

    def start_first(piece, carry):
        for third in THIRDS:
            pair_first(third, piece).start()
        return carry

    lax.fori_loop(0, PIECES, start_first, 0)
    own_small = (
        pltpu.make_async_copy(grad_wide, wide_raw, local_sems.at[0]), pltpu.make_async_copy(grad_vec, vec_raw, local_sems.at[1]))
    for copy in own_small:
        copy.start()
    square_sum[...] = jnp.zeros_like(square_sum)

    def loads(unit, third, piece):
        rows = piece * PIECE
        slot = (unit * PIECES + piece) % LOAD_SLOTS
        copies = [
            pltpu.make_async_copy(grad_of(third, owner_of(unit, third), rows, PIECE), raw_own.at[slot, third], load_sems.at[slot, third, 0])]
        if unit > 0:
            copies.append(pltpu.make_async_copy(
                pair_raw.at[unit - 1, third, pl.ds(rows, PIECE)], raw_pair.at[slot, third], load_sems.at[slot, third, 1]))
        for place, source in enumerate(UNITS[unit][2]):
            if source < 6:
                copies.append(pltpu.make_async_copy(
                    landed.at[source, third, pl.ds(rows, PIECE)], partial.at[slot, third, place], load_sems.at[slot, third, 2 + place]))
        return copies

    def send(unit, third, piece):
        rows = piece * PIECE
        slot = (unit * PIECES + piece) % SEND_SLOTS
        to = flip(me, ORDERS[third][UNITS[unit][0]])
        return pltpu.make_async_remote_copy(
            outgoing.at[slot, third], (landed.at[unit, third] if unit < 6 else landed_near.at[third]).at[pl.ds(rows, PIECE)],
            send_sems.at[slot, third], land_sems.at[unit, third, piece], device_id=(to,), device_id_type=MESH)

    def begin(unit, piece):
        for third in THIRDS:
            if unit > 0:
                @pl.when(piece == 0)
                def _():
                    pair_copy(unit, third).wait_recv()
            for source in UNITS[unit][2]:
                if source < 6:
                    send(source, third, piece).wait_recv()
            for copy in loads(unit, third, piece):
                copy.start()

    ahead = LOAD_SLOTS - 1
    for piece in range(ahead):
        begin(0, piece)

    for unit in range(8):
        def work(piece, carry, unit=unit):
            @pl.when(piece + ahead < PIECES)
            def _():
                begin(unit, piece + ahead)
            if unit < 7:
                @pl.when(piece + ahead >= PIECES)
                def _():
                    begin(unit + 1, piece + ahead - PIECES)
            slot = (unit * PIECES + piece) % LOAD_SLOTS
            out_slot = (unit * PIECES + piece) % SEND_SLOTS
            for third in THIRDS:
                for copy in loads(unit, third, piece):
                    copy.wait()
                rows = pl.ds(pl.multiple_of(piece * PIECE, PIECE), PIECE)
                if unit == 0:
                    pair_first(third, piece).wait_recv()
                    value = raw_own[slot, third].astype(jnp.float32) + pair_near[third, rows].astype(jnp.float32)
                else:
                    value = raw_own[slot, third].astype(jnp.float32) + raw_pair[slot, third].astype(jnp.float32)
                for place, source in enumerate(UNITS[unit][2]):
                    if source < 6:
                        value = value + partial[slot, third, place]
                    else:
                        send(source, third, piece).wait_recv()
                        value = value + landed_near[third, rows]
                if unit < 7:
                    if unit == 0:
                        @pl.when(piece >= SEND_SLOTS)
                        def _():
                            send(unit, third, piece).wait_send()
                    else:
                        send(unit, third, piece).wait_send()
                    outgoing[out_slot, third] = value
                    send(unit, third, piece).start()
                else:
                    value = value * (1.0 / GROUP)
                    sums[pl.ds(pl.multiple_of(third * THIRD + piece * PIECE, PIECE), PIECE)] = value
                    square_sum[...] += jnp.sum((value * value).reshape(PIECE // 8, 8, LANES), axis=0)
            if unit == 0:
                @pl.when(piece == 0)
                def _():
                    for later in range(1, 8):
                        for third in THIRDS:
                            pair_copy(later, third).start()
            return carry

        lax.fori_loop(0, PIECES, work, 0)
        if unit == 0:
            for copy in own_small:
                copy.wait()
            shares_from(wide_raw, vec_raw, wide_rows, vec_rows, packed)
            small_shares[...] = packed[...].astype(jnp.bfloat16)
            small_slots[me] = small_shares[me]
        if unit == 1:
            tile_to_everyone(me, lambda owner: small_shares.at[owner], small_slots, small_send, small_recv, True)

    tile_to_everyone(me, lambda owner: small_shares.at[owner], small_slots, small_send, small_recv, False)
    small = jnp.sum(small_slots[...].astype(jnp.float32), axis=0) * (1.0 / GROUP)
    small_sums[...] = small
    squares = square_sum[...] + (small * small)[0:8] + (small * small)[8:16]
    square_sum[...] = squares
    square_slots[me] = squares
    tile_to_everyone(me, lambda owner: square_sum, square_slots, square_send, square_recv, True)
    for slot in range(SEND_SLOTS):
        for third in THIRDS:
            send(6, third, slot).wait_send()

    def drain(piece, carry):
        for third in THIRDS:
            pair_first(third, piece).wait_send()
        return carry

    lax.fori_loop(0, PIECES, drain, 0)
    for unit in range(1, 8):
        for third in THIRDS:
            pair_copy(unit, third).wait_send()
    tile_to_everyone(me, lambda owner: square_sum, square_slots, square_send, square_recv, False)
    total[...] = jnp.full(TILE, jnp.sum(square_slots[...]), jnp.float32)


def reduce_scatter(grad_attn, grad_mlp, grad_wide, grad_vec):
    anywhere = pl.BlockSpec(memory_space=pl.ANY)
    inside = pl.BlockSpec(memory_space=pltpu.VMEM)
    dma = pltpu.SemaphoreType.DMA
    return pl.pallas_call(
        scatter_kernel,
        name="scatter",
        out_shape=(
            pltpu.VMEM((ROWS, LANES), jnp.float32),
            pltpu.VMEM((SMALL_ROWS, LANES), jnp.float32),
            pltpu.VMEM(TILE, jnp.float32),
            pltpu.HBM((7, 3, THIRD, LANES), jnp.bfloat16),
            pltpu.HBM((6, 3, THIRD, LANES), jnp.float32),
        ),
        in_specs=[anywhere] * 4,
        out_specs=(inside, inside, inside, anywhere, anywhere),
        scratch_shapes=[
            pltpu.VMEM((LOAD_SLOTS, 3, PIECE, LANES), jnp.bfloat16),
            pltpu.VMEM((LOAD_SLOTS, 3, PIECE, LANES), jnp.bfloat16),
            pltpu.VMEM((LOAD_SLOTS, 3, 3, PIECE, LANES), jnp.float32),
            pltpu.VMEM((SEND_SLOTS, 3, PIECE, LANES), jnp.float32),
            pltpu.VMEM(TILE, jnp.float32),
            pltpu.VMEM((GROUP, SMALL_ROWS, LANES), jnp.bfloat16),
            pltpu.VMEM((GROUP, 8, LANES), jnp.float32),
            pltpu.VMEM((3, THIRD, LANES), jnp.bfloat16),
            pltpu.VMEM((3, THIRD, LANES), jnp.float32),
            pltpu.VMEM((1, 5120), jnp.bfloat16),
            pltpu.VMEM((11, 1280), jnp.bfloat16),
            pltpu.VMEM((8, 5120), jnp.float32),
            pltpu.VMEM((SMALL_ROWS, 1280), jnp.float32),
            pltpu.VMEM((GROUP, SMALL_ROWS, LANES), jnp.float32),
            pltpu.VMEM((GROUP, SMALL_ROWS, LANES), jnp.bfloat16),
            dma((LOAD_SLOTS, 3, 5)),
            dma((SEND_SLOTS, 3)),
            dma((3, PIECES)),
            dma((3, PIECES)),
            dma((8, 3)),
            dma((8, 3)),
            dma((7, 3, PIECES)),
            dma((GROUP,)),
            dma((GROUP,)),
            dma((GROUP,)),
            dma((GROUP,)),
            dma((2,)),
        ],
        compiler_params=pltpu.CompilerParams(collective_id=0, has_side_effects=True, vmem_limit_bytes=SCATTER_VMEM),
    )(*[pltpu.with_memory_space_constraint(grad, pltpu.HBM) for grad in (grad_attn, grad_mlp, grad_wide, grad_vec)])[:3]


def bank_part(third, attn, mlp):
    return (attn, 0) if third == 0 else (mlp, (third - 1) * THIRD)


def update_kernel(sums, small_sums, total, weight_attn, weight_mlp, first_attn, first_mlp, second_attn, second_mlp,
                  weight_wide, weight_vec, first_wide, first_vec, second_wide, second_vec,
                  update, small_update, small_weight, part_sums, new_first_attn, new_first_mlp, new_second_attn, new_second_mlp,
                  new_first_wide, new_first_vec, new_second_wide, new_second_vec,
                  first_out, second_out, small_first, small_second, out_sems):
    clip_coef = jnp.minimum(1.0, MAX_NORM / jnp.sqrt(total[0:1, :]))

    def direction(mean_grad, weight, first, second):
        clipped = clip_coef * mean_grad
        new_first = BETA_FIRST * first + (1.0 - BETA_FIRST) * clipped
        new_second = BETA_SECOND * second + (1.0 - BETA_SECOND) * (clipped * clipped)
        root = jnp.sqrt(new_second * (1.0 / (1.0 - BETA_SECOND ** STEP_NUMBER))) + EPSILON
        return (new_first * (1.0 / (1.0 - BETA_FIRST ** STEP_NUMBER))) / root + WEIGHT_DECAY * weight, new_first, new_second

    def tile_sum(value):
        return jnp.sum((value * value).reshape(-1, 8, LANES), axis=0)

    def copies(third, chunk):
        slot = (third * CHUNKS + chunk) % OUT_SLOTS
        first_to, base = bank_part(third, new_first_attn, new_first_mlp)
        second_to, _ = bank_part(third, new_second_attn, new_second_mlp)
        rows = pl.ds(base + chunk * CHUNK, CHUNK)
        return (
            pltpu.make_async_copy(first_out.at[slot], first_to.at[rows], out_sems.at[slot, 0]),
            pltpu.make_async_copy(second_out.at[slot], second_to.at[rows], out_sems.at[slot, 1]),
        )

    totals = []
    for third in THIRDS:
        weight, base = bank_part(third, weight_attn, weight_mlp)
        first, _ = bank_part(third, first_attn, first_mlp)
        second, _ = bank_part(third, second_attn, second_mlp)

        def work(chunk, carry, third=third, weight=weight, first=first, second=second, base=base):
            slot = (third * CHUNKS + chunk) % OUT_SLOTS
            place = third * CHUNKS + chunk

            @pl.when(place >= OUT_SLOTS)
            def _():
                for copy in copies(third, chunk):
                    copy.wait()

            def block(step, carry):
                squares_weight, squares_update = carry
                inner = pl.multiple_of(step * BLOCK, BLOCK)
                rows = pl.ds(pl.multiple_of(base + chunk * CHUNK + inner, BLOCK), BLOCK)
                old = weight[rows]
                new_update, new_first, new_second = direction(
                    sums[pl.ds(pl.multiple_of(third * THIRD + chunk * CHUNK + inner, BLOCK), BLOCK)], old, first[rows], second[rows])
                first_out[slot, pl.ds(inner, BLOCK)] = new_first
                second_out[slot, pl.ds(inner, BLOCK)] = new_second
                update[pl.ds(pl.multiple_of(third * THIRD + chunk * CHUNK + inner, BLOCK), BLOCK)] = new_update
                return squares_weight + tile_sum(old), squares_update + tile_sum(new_update)

            carry = lax.fori_loop(0, CHUNK // BLOCK, block, carry)
            for copy in copies(third, chunk):
                copy.start()
            return carry

        zero = jnp.zeros(TILE, jnp.float32)
        totals.append(lax.fori_loop(0, CHUNKS, work, (zero, zero)))
    pack_rows(weight_wide, weight_vec, small_weight)
    pack_rows(first_wide, first_vec, small_first)
    pack_rows(second_wide, second_vec, small_second)
    small, small_m, small_v = direction(small_sums[...], small_weight[...], small_first[...], small_second[...])
    small_update[...] = small
    small_first[...] = small_m
    small_second[...] = small_v
    unpack_rows(small_first, new_first_wide, new_first_vec)
    unpack_rows(small_second, new_second_wide, new_second_vec)
    old = small_weight[...]
    columns = [
        totals[0][0], totals[0][1], totals[1][0] + totals[2][0], totals[1][1] + totals[2][1],
        (old * old)[0:8], (small * small)[0:8], (old * old)[8:16], (small * small)[8:16],
    ]
    lane = lax.broadcasted_iota(jnp.int32, TILE, 1)
    tile = jnp.zeros(TILE, jnp.float32)
    for place, column in enumerate(columns):
        tile = jnp.where(lane == place, jnp.sum(column, axis=1, keepdims=True), tile)
    part_sums[...] = tile
    for place in range(3 * CHUNKS - OUT_SLOTS, 3 * CHUNKS):
        for copy in copies(place // CHUNKS, place % CHUNKS):
            copy.wait()


def resident(value):
    return pltpu.with_memory_space_constraint(value, pltpu.VMEM)


def update_step(sums, small_sums, total, weights, firsts, seconds, smalls):
    anywhere = pl.BlockSpec(memory_space=pl.ANY)
    inside = pl.BlockSpec(memory_space=pltpu.VMEM)
    attn = pltpu.HBM((ATTN_ROWS, LANES), jnp.float32)
    mlp = pltpu.HBM((MLP_ROWS, LANES), jnp.float32)
    wide = jax.ShapeDtypeStruct((1, 320), jnp.float32)
    vec = jax.ShapeDtypeStruct((11, 80), jnp.float32)
    operands = [sums, small_sums, total, *weights, *firsts, *seconds]
    return pl.pallas_call(
        update_kernel,
        name="update",
        out_shape=(
            pltpu.VMEM((ROWS, LANES), jnp.float32),
            pltpu.VMEM((SMALL_ROWS, LANES), jnp.float32),
            pltpu.VMEM((SMALL_ROWS, LANES), jnp.float32),
            pltpu.VMEM(TILE, jnp.float32),
            attn, mlp, attn, mlp, wide, vec, wide, vec,
        ),
        in_specs=[inside] * 15,
        out_specs=(inside,) * 4 + (anywhere,) * 4 + (inside,) * 4,
        scratch_shapes=[
            pltpu.VMEM((OUT_SLOTS, CHUNK, LANES), jnp.float32),
            pltpu.VMEM((OUT_SLOTS, CHUNK, LANES), jnp.float32),
            pltpu.VMEM((SMALL_ROWS, LANES), jnp.float32),
            pltpu.VMEM((SMALL_ROWS, LANES), jnp.float32),
            pltpu.SemaphoreType.DMA((OUT_SLOTS, 2)),
        ],
        compiler_params=pltpu.CompilerParams(vmem_limit_bytes=UPDATE_VMEM),
    )(*[resident(value) for value in operands], *smalls)


def gather_kernel(part_sums, weight_attn, weight_mlp, update, small_weight, small_update,
                  everything, all_wide, all_vec, ratios,
                  all_small, fresh_small, slots, wide_flat, pair,
                  tile_send, tile_recv, small_send, small_recv, link_send, link_recv, twin_send, twin_recv,
                  last_send, last_recv, last_twin_send, last_twin_recv):
    me = lax.axis_index("data")
    twin = flip(me, CORE)
    meet_everyone(me)
    slots[me] = part_sums[...]
    tile_to_everyone(me, lambda owner: part_sums, slots, tile_send, tile_recv, True)
    tile_to_everyone(me, lambda owner: part_sums, slots, tile_send, tile_recv, False)
    sums = jnp.sum(slots[...], axis=0)
    lane = lax.broadcasted_iota(jnp.int32, TILE, 1)

    def column(place):
        return jnp.sum(jnp.where(lane == place, sums, 0.0), axis=1, keepdims=True)

    def same_tensor(value, rows):
        total = value
        for shift in range(rows, 8, rows):
            total = total + pltpu.roll(value, shift, 0)
        return total

    def wide_rows(value):
        row = lax.broadcasted_iota(jnp.int32, (8, 1), 0)
        mine = jnp.logical_and(row >= 3, row < 6)
        return jnp.where(mine, jnp.sum(jnp.where(mine, value, 0.0), axis=0, keepdims=True), value)

    def spread(value):
        return jnp.broadcast_to(value, TILE)

    def ratio(weights, updates):
        safe = jnp.where(updates > 0.0, updates, 1.0)
        return jnp.sqrt(weights) / jnp.sqrt(safe)

    ratio_attn = ratio(same_tensor(spread(column(0)), 4), same_tensor(spread(column(1)), 4))
    ratio_mlp = ratio(same_tensor(spread(column(2)), 2), same_tensor(spread(column(3)), 2))
    ratio_low = ratio(spread(column(4)), spread(column(5)))
    ratio_high = ratio(spread(wide_rows(column(6))), spread(wide_rows(column(7))))
    ratios[0] = ratio_attn
    ratios[1] = ratio_mlp
    ratios[2] = ratio_low
    ratios[3] = ratio_high

    def place_of(third, owner):
        return everything.at[owner, pl.ds(third * THIRD, THIRD)]

    def link(third, stage, hops):
        number = ARRIVALS.index((stage, hops))
        to = flip(me, ORDERS[third][stage])
        owner = flip_all(me, [ORDERS[third][hop] for hop in hops])
        place = place_of(third, owner)
        return pltpu.make_async_remote_copy(
            place, place, link_send.at[third, number], link_recv.at[third, number],
            device_id=(to,), device_id_type=MESH)

    def landed(third, stage, hops):
        number = ARRIVALS.index((stage, hops))
        owner = flip_all(flip(me, ORDERS[third][stage]), [ORDERS[third][hop] for hop in hops])
        place = place_of(third, owner)
        return pltpu.make_async_remote_copy(
            place, place, link_send.at[third, number], link_recv.at[third, number],
            device_id=(flip(me, ORDERS[third][stage]),), device_id_type=MESH)

    def to_twin(third, number, hops):
        owner = flip_all(me, [ORDERS[third][hop] for hop in hops])
        place = place_of(third, owner)
        return pltpu.make_async_remote_copy(
            place, place, twin_send.at[third, number], twin_recv.at[third, number],
            device_id=(twin,), device_id_type=MESH)

    def from_twin(third, number, hops):
        owner = flip_all(twin, [ORDERS[third][hop] for hop in hops])
        place = place_of(third, owner)
        return pltpu.make_async_remote_copy(
            place, place, twin_send.at[third, number], twin_recv.at[third, number],
            device_id=(twin,), device_id_type=MESH)

    for third in THIRDS:
        scale = LEARN_RATE * (ratio_attn if third == 0 else ratio_mlp)
        weight, base = bank_part(third, weight_attn, weight_mlp)

        def refresh(piece, carry, third=third, scale=scale, weight=weight, base=base):
            rows = pl.ds(pl.multiple_of(third * THIRD + piece * PIECE, PIECE), PIECE)
            old = weight[pl.ds(pl.multiple_of(base + piece * PIECE, PIECE), PIECE)].reshape(PIECE // 8, 8, LANES)
            step = update[rows].reshape(PIECE // 8, 8, LANES)
            everything[me, rows] = (old - scale[None] * step).reshape(PIECE, LANES).astype(jnp.bfloat16)
            return carry

        lax.fori_loop(0, PIECES, refresh, 0)
        link(third, 0, ()).start()
    for stage in (1, 2):
        for third in THIRDS:
            link(third, stage, ()).start()
    for third in THIRDS:
        to_twin(third, 0, ()).start()
    low = small_weight[0:8] - LEARN_RATE * ratio_low * small_update[0:8]
    high = small_weight[8:16] - LEARN_RATE * ratio_high * small_update[8:16]
    fresh_small[...] = jnp.concatenate([low, high], axis=0).astype(jnp.bfloat16)
    all_small[me] = fresh_small[...]
    tile_to_everyone(me, lambda owner: fresh_small, all_small, small_send, small_recv, True)

    def last_part(third, part, owner, to, send_sem, recv_sem):
        place = everything.at[owner, pl.ds(third * THIRD + part * LAST, LAST)]
        return pltpu.make_async_remote_copy(
            place, place, send_sem.at[third, part], recv_sem.at[third, part], device_id=(to,), device_id_type=MESH)

    def last_link(third, part):
        owner = flip_all(me, ORDERS[third][:2])
        return last_part(third, part, owner, flip(me, ORDERS[third][2]), last_send, last_recv)

    def last_landed(third, part):
        return last_part(third, part, flip_all(me, ORDERS[third]), flip(me, ORDERS[third][2]), last_send, last_recv)

    def last_to_twin(third, part):
        return last_part(third, part, flip_all(me, ORDERS[third]), twin, last_twin_send, last_twin_recv)

    def last_from_twin(third, part):
        return last_part(third, part, flip_all(twin, ORDERS[third]), twin, last_twin_send, last_twin_recv)

    sent = []
    for number, (stage, hops) in enumerate(ARRIVALS):
        for third in THIRDS:
            landed(third, stage, hops).wait_recv()
            for later in () if hops else range(stage + 1, len(THIRDS)):
                copy = link(third, later, (stage,))
                copy.start()
                sent.append(copy)
            if hops and stage == 1:
                for part in range(PARTS):
                    last_link(third, part).start()
            to_twin(third, number + 1, (stage,) + hops).start()
        if number == 2:
            tile_to_everyone(me, lambda owner: fresh_small, all_small, small_send, small_recv, False)
            shares_to(all_small, all_wide, all_vec, wide_flat, pair)
    for number, hops in enumerate(((),) + tuple((stage,) + hops for stage, hops in ARRIVALS)):
        for third in THIRDS:
            from_twin(third, number, hops).wait_recv()
            to_twin(third, number, hops).wait_send()
    for third in THIRDS:
        for stage in range(3):
            link(third, stage, ()).wait_send()
    for copy in sent:
        copy.wait_send()
    for part in range(PARTS):
        for third in THIRDS:
            last_landed(third, part).wait_recv()
            last_to_twin(third, part).start()
    for part in range(PARTS):
        for third in THIRDS:
            last_link(third, part).wait_send()
            last_to_twin(third, part).wait_send()
            last_from_twin(third, part).wait_recv()


def all_gather(part_sums, weights, update, small_weight, small_update):
    inside = pl.BlockSpec(memory_space=pltpu.VMEM)
    dma = pltpu.SemaphoreType.DMA
    return pl.pallas_call(
        gather_kernel,
        name="gather",
        out_shape=(
            pltpu.VMEM((GROUP, ROWS, LANES), jnp.bfloat16),
            pltpu.VMEM((1, 5120), jnp.bfloat16),
            pltpu.VMEM((11, 1280), jnp.bfloat16),
            pltpu.VMEM((4, 8, LANES), jnp.float32),
        ),
        in_specs=[inside] * 6,
        out_specs=(inside,) * 4,
        scratch_shapes=[
            pltpu.VMEM((GROUP, SMALL_ROWS, LANES), jnp.bfloat16),
            pltpu.VMEM((SMALL_ROWS, LANES), jnp.bfloat16),
            pltpu.VMEM((GROUP, 8, LANES), jnp.float32),
            pltpu.VMEM((8, 5120), jnp.float32),
            pltpu.VMEM((2, SMALL_ROWS, LANES), jnp.float32),
            *[dma((GROUP,))] * 4,
            *[dma((len(THIRDS), len(ARRIVALS)))] * 2, *[dma((len(THIRDS), len(ARRIVALS) + 1))] * 2, *[dma((len(THIRDS), PARTS))] * 4,
        ],
        compiler_params=pltpu.CompilerParams(collective_id=1, has_side_effects=True, vmem_limit_bytes=GATHER_VMEM),
    )(*[resident(value) for value in (part_sums, *weights, update, small_weight, small_update)])


def write_kernel(everything, replica_attn, replica_mlp, attn_sems, mlp_sems):
    writes = []
    for owner in range(GROUP):
        writes.append(pltpu.make_async_copy(
            everything.at[owner, pl.ds(0, ATTN_ROWS)], replica_attn.at[pl.ds(owner * ATTN_ROWS, ATTN_ROWS)], attn_sems.at[owner]))
        writes.append(pltpu.make_async_copy(
            everything.at[owner, pl.ds(ATTN_ROWS, MLP_ROWS)], replica_mlp.at[pl.ds(owner * MLP_ROWS, MLP_ROWS)], mlp_sems.at[owner]))
    for copy in writes:
        copy.start()
    for copy in writes:
        copy.wait()


def write_replica(everything):
    anywhere = pl.BlockSpec(memory_space=pl.ANY)
    dma = pltpu.SemaphoreType.DMA
    return pl.pallas_call(
        write_kernel,
        name="write",
        out_shape=(
            pltpu.HBM((GROUP * ATTN_ROWS, LANES), jnp.bfloat16),
            pltpu.HBM((GROUP * MLP_ROWS, LANES), jnp.bfloat16),
        ),
        in_specs=[pl.BlockSpec(memory_space=pltpu.VMEM)],
        out_specs=(anywhere,) * 2,
        scratch_shapes=[dma((GROUP,)), dma((GROUP,))],
        compiler_params=pltpu.CompilerParams(vmem_limit_bytes=FINISH_VMEM),
    )(resident(everything))


def finish_kernel(weight_attn, weight_mlp, update, ratios, all_wide, all_vec, small_weight, small_update,
                  new_attn, new_mlp, replica_wide, replica_vec, new_wide, new_vec,
                  fresh, fresh_small, weight_sems):
    for tile in range(2):
        rows = pl.ds(8 * tile, 8)
        fresh_small[rows] = small_weight[rows] - LEARN_RATE * ratios[2 + tile] * small_update[rows]
    unpack_rows(fresh_small, new_wide, new_vec)
    replica_wide[...] = all_wide[...]
    replica_vec[...] = all_vec[...]
    def write(third, chunk):
        slot = (third * CHUNKS + chunk) % OUT_SLOTS
        to, base = bank_part(third, new_attn, new_mlp)
        return pltpu.make_async_copy(fresh.at[slot], to.at[pl.ds(base + chunk * CHUNK, CHUNK)], weight_sems.at[slot])

    for third in THIRDS:
        scale = LEARN_RATE * ratios[0 if third == 0 else 1]
        weight, base = bank_part(third, weight_attn, weight_mlp)

        def work(chunk, carry, third=third, scale=scale, weight=weight, base=base):
            slot = (third * CHUNKS + chunk) % OUT_SLOTS

            @pl.when(third * CHUNKS + chunk >= OUT_SLOTS)
            def _():
                write(third, chunk).wait()

            def refresh(block, inner):
                start = chunk * CHUNK + block * BLOCK
                old = weight[pl.ds(pl.multiple_of(base + start, BLOCK), BLOCK)].reshape(BLOCK // 8, 8, LANES)
                step = update[pl.ds(pl.multiple_of(third * THIRD + start, BLOCK), BLOCK)].reshape(BLOCK // 8, 8, LANES)
                fresh[slot, pl.ds(pl.multiple_of(block * BLOCK, BLOCK), BLOCK)] = (old - scale[None] * step).reshape(BLOCK, LANES)
                return inner

            lax.fori_loop(0, CHUNK // BLOCK, refresh, 0)
            write(third, chunk).start()
            return carry

        lax.fori_loop(0, CHUNKS, work, 0)
    for place in range(3 * CHUNKS - OUT_SLOTS, 3 * CHUNKS):
        write(place // CHUNKS, place % CHUNKS).wait()


def finish(all_wide, all_vec, weights, update, small_weight, small_update, ratios):
    anywhere = pl.BlockSpec(memory_space=pl.ANY)
    inside = pl.BlockSpec(memory_space=pltpu.VMEM)
    dma = pltpu.SemaphoreType.DMA
    return pl.pallas_call(
        finish_kernel,
        name="finish",
        out_shape=(
            pltpu.HBM((ATTN_ROWS, LANES), jnp.float32),
            pltpu.HBM((MLP_ROWS, LANES), jnp.float32),
            jax.ShapeDtypeStruct((1, 5120), jnp.bfloat16),
            jax.ShapeDtypeStruct((11, 1280), jnp.bfloat16),
            jax.ShapeDtypeStruct((1, 320), jnp.float32),
            jax.ShapeDtypeStruct((11, 80), jnp.float32),
        ),
        in_specs=[inside] * 8,
        out_specs=(anywhere,) * 2 + (inside,) * 4,
        scratch_shapes=[
            pltpu.VMEM((OUT_SLOTS, CHUNK, LANES), jnp.float32), pltpu.VMEM((SMALL_ROWS, LANES), jnp.float32),
            dma((OUT_SLOTS,)),
        ],
        compiler_params=pltpu.CompilerParams(vmem_limit_bytes=FINISH_VMEM),
    )(*[resident(value) for value in (*weights, update, ratios, all_wide, all_vec, small_weight, small_update)])


def linear(bank):
    rows, length = bank.shape
    return bank.reshape(rows, length // LANES, LANES).transpose(1, 0, 2).reshape(rows * length // LANES, LANES)


def banked(flat, rows):
    blocks = flat.size // (rows * LANES)
    return flat.reshape(blocks, rows, LANES).transpose(1, 0, 2).reshape(rows, blocks * LANES)


def solution(mesh):
    grad_spec = P("data", None, None)
    shard_spec = P(None, "data")
    full_spec = P(None, None)

    def local_step(*banks):
        grads = banks[0:4]
        attn_grad = linear(grads[0][0]).reshape(GROUP, ATTN_ROWS, LANES)
        mlp_grad = linear(grads[1][0]).reshape(GROUP, MLP_ROWS, LANES)
        states = [(linear(banks[first]), linear(banks[first + 1])) for first in (4, 8, 12)]
        smalls = [bank for first in (4, 8, 12) for bank in banks[first + 2:first + 4]]
        sums, small_sums, total = reduce_scatter(attn_grad, mlp_grad, grads[2][0], grads[3][0])
        update, small_update, small_weight, part_sums, *moments = update_step(sums, small_sums, total, *states, smalls)
        everything, all_wide, all_vec, ratios = all_gather(part_sums, states[0], update, small_weight, small_update)
        replica_attn, replica_mlp = write_replica(everything)
        replica_attn, all_wide = lax.optimization_barrier((replica_attn, all_wide))
        new_attn, new_mlp, replica_wide, replica_vec, new_wide, new_vec = finish(
            all_wide, all_vec, states[0], update, small_weight, small_update, ratios)
        return (
            banked(replica_attn, 4), banked(replica_mlp, 2), replica_wide, replica_vec,
            banked(new_attn, 4), banked(new_mlp, 2), new_wide, new_vec,
            banked(moments[0], 4), banked(moments[1], 2), moments[4], moments[5],
            banked(moments[2], 4), banked(moments[3], 2), moments[6], moments[7],
        )

    return jax.shard_map(local_step, mesh=mesh, in_specs=(grad_spec,) * 4 + (shard_spec,) * 12, out_specs=(full_spec,) * 4 + (shard_spec,) * 12, check_vma=False)
```

```python
import functools

import jax
import jax.numpy as jnp
from jax import lax
from jax.experimental import pallas as pl
from jax.experimental.pallas import tpu as pltpu
from jax.sharding import PartitionSpec as P

STEP_NUMBER = 10
LEARN_RATE = 0.04
BETA_FIRST = 0.9
BETA_SECOND = 0.999
EPSILON = 1e-6
WEIGHT_DECAY = 0.01
MAX_NORM = 1.0
ROOT_FLOOR = 1e-36

MESH = pl.DeviceIdType.MESH
GROUP = 16
LANES = 128
TILE = (8, LANES)
THIRDS = range(3)
VECS = 11
VEC_SHARE = 80
VEC = 1280
WIDE = 5120
WIDE_PARTS = ((0, LANES), (1, LANES), (2, 64))
WIDE_SHARE = 320
MIB = 2 ** 20
ATTN_ROWS = 3200
MLP_ROWS = 6400
ROWS = ATTN_ROWS + MLP_ROWS
THIRD = 3200
PIECE = 320
PIECES = THIRD // PIECE
LOAD_SLOTS = 3
SEND_SLOTS = 4
SMALL_ROWS = 16
BLOCK = 320
PARTS = 4
LAST = THIRD // PARTS
OWN_PARTS = ((0, 640), (640, 2560))
CHUNK = 640
CHUNKS = THIRD // CHUNK
OUT_SLOTS = 4
SCATTER_VMEM = 30 * MIB
UPDATE_VMEM = 8 * MIB
GATHER_VMEM = 2 * MIB
FINISH_VMEM = 3 * MIB
CORE = 1
ORDERS = ((2, 4, 8), (4, 8, 2), (8, 2, 4))
UNITS = (
    (0, (0, 1, 2), ()),
    (0, (0, 1), ()),
    (0, (0, 2), ()),
    (1, (1, 2), (0,)),
    (0, (0,), ()),
    (1, (1,), (1,)),
    (2, (2,), (2, 3)),
    (None, (), (4, 5, 6)),
)


ARRIVALS = [(0, ()), (1, ()), (2, ()), (1, (0,)), (2, (0,)), (2, (1,))]


def flip(index, width):
    return index + width * (1 - 2 * ((index // width) % 2))


def flip_all(index, widths):
    for width in widths:
        index = flip(index, width)
    return index


def greet_everyone(me):
    barrier = pltpu.get_barrier_semaphore()

    def signal(step, carry):
        pl.semaphore_signal(barrier, inc=1, device_id=((me + step) % GROUP,), device_id_type=MESH)
        return carry

    lax.fori_loop(1, GROUP, signal, 0)


def meet_everyone():
    pl.semaphore_wait(pltpu.get_barrier_semaphore(), GROUP - 1)


def tile_to_everyone(me, source_of, slots, send_sems, recv_sems, begin):
    def copy(step):
        return pltpu.make_async_remote_copy(
            source_of((me + step) % GROUP), slots.at[me], send_sems.at[step], recv_sems.at[step],
            device_id=((me + step) % GROUP,), device_id_type=MESH)

    def arrival(step):
        return pltpu.make_async_remote_copy(
            source_of((me + step) % GROUP), slots.at[(me - step + GROUP) % GROUP], send_sems.at[step], recv_sems.at[step],
            device_id=((me + step) % GROUP,), device_id_type=MESH)

    def start(step, carry):
        copy(step).start()
        return carry

    def finish(step, carry):
        arrival(step).wait()
        return carry

    lax.fori_loop(1, GROUP, start if begin else finish, 0)


def small_places(packed, wide, vec):
    places = [(packed.at[pl.ds(0, VECS), pl.ds(0, VEC_SHARE)], vec)]
    for part, width in WIDE_PARTS:
        places.append((packed.at[pl.ds(VECS + part, 1), pl.ds(0, width)], wide.at[:, pl.ds(LANES * part, width)]))
    return places


def pack_rows(wide, vec, packed):
    packed[...] = jnp.zeros_like(packed)
    for inner, outer in small_places(packed, wide, vec):
        inner[...] = outer[...]


def unpack_rows(packed, wide, vec):
    for inner, outer in small_places(packed, wide, vec):
        outer[...] = inner[...]


def shares_from(wide, vec, wide_rows, vec_rows, packed):
    wide_rows[...] = jnp.zeros_like(wide_rows)
    wide_rows[:1] = wide[...].astype(jnp.float32)
    vec_rows[...] = jnp.zeros_like(vec_rows)
    vec_rows[:VECS] = vec[...].astype(jnp.float32)
    packed[...] = jnp.zeros_like(packed)

    def window(rows, start):
        block, shift = start // LANES * LANES, start % LANES
        value = rows[:, block:block + LANES]
        if shift == 0:
            return value
        lane = lax.broadcasted_iota(jnp.int32, value.shape, 1)
        value = pltpu.roll(value, LANES - shift, 1)
        if block + LANES == rows.shape[1]:
            return value
        after = pltpu.roll(rows[:, block + LANES:block + 2 * LANES], LANES - shift, 1)
        return jnp.where(lane < LANES - shift, value, after)

    lane = lax.broadcasted_iota(jnp.int32, (SMALL_ROWS, LANES), 1)
    for owner in range(GROUP):
        packed[owner] = jnp.where(lane < VEC_SHARE, window(vec_rows, VEC_SHARE * owner), 0.0)
        for part, width in WIDE_PARTS:
            value = window(wide_rows, WIDE_SHARE * owner + LANES * part)
            packed[owner, pl.ds(VECS + part, 1)] = jnp.where(lane[:1] < width, value[:1], 0.0)


def shares_to(shares, wide, vec, wide_rows, pair):
    lane = lax.broadcasted_iota(jnp.int32, (SMALL_ROWS, LANES), 1)
    low = lax.broadcasted_iota(jnp.int32, (1, LANES), 1) < 64
    for block in range(VEC // LANES):
        value = jnp.zeros((SMALL_ROWS, LANES), jnp.float32)
        for owner in range(GROUP):
            begin, end = max(VEC_SHARE * owner, LANES * block), min(VEC_SHARE * (owner + 1), LANES * (block + 1))
            if begin < end:
                shift = (VEC_SHARE * owner - LANES * block) % LANES
                moved = shares[owner].astype(jnp.float32)
                if shift:
                    moved = pltpu.roll(moved, shift, 1)
                inside = jnp.logical_and(lane >= begin - LANES * block, lane < end - LANES * block)
                value = jnp.where(inside, moved, value)
        vec[:, LANES * block:LANES * (block + 1)] = value[:VECS].astype(jnp.bfloat16)
    for place in range(GROUP // 2):
        pair[0] = shares[2 * place].astype(jnp.float32)
        pair[1] = pltpu.roll(shares[2 * place + 1].astype(jnp.float32), 64, 1)
        even, odd = [[pair[half, pl.ds(VECS + part, 1)] for part, _ in WIDE_PARTS] for half in range(2)]
        blocks = [
            even[0], even[1], jnp.where(low, even[2], odd[0]), jnp.where(low, odd[0], odd[1]), jnp.where(low, odd[1], odd[2]),
        ]
        for number, value in enumerate(blocks):
            wide_rows[:1, pl.ds(LANES * (len(blocks) * place + number), LANES)] = value
    wide[...] = wide_rows[:1].astype(jnp.bfloat16)


def scatter_kernel(grad_attn, grad_mlp, grad_wide, grad_vec, sums, small_sums, total, pair_raw, landed,
                   raw_own, raw_pair, partial, outgoing, square_sum, small_slots, square_slots,
                   pair_near, landed_near, wide_raw, vec_raw, wide_rows, vec_rows, packed, small_shares,
                   load_sems, send_sems, pair_send_first, pair_recv_first, pair_send, pair_recv, land_sems,
                   small_send, small_recv, square_send, square_recv, local_sems):
    me = lax.axis_index("data")
    twin = flip(me, CORE)
    greet_everyone(me)

    def grad_of(third, owner, row, count):
        if third == 0:
            return grad_attn.at[owner, pl.ds(row, count)]
        return grad_mlp.at[owner, pl.ds(row + (third - 1) * THIRD, count)]

    def owner_of(unit, third):
        return flip_all(me, [ORDERS[third][place] for place in UNITS[unit][1]])

    def pair_first(third, piece):
        rows = piece * PIECE
        return pltpu.make_async_remote_copy(
            grad_of(third, flip(owner_of(0, third), CORE), rows, PIECE), pair_near.at[third, pl.ds(rows, PIECE)],
            pair_send_first.at[third, piece], pair_recv_first.at[third, piece], device_id=(twin,), device_id_type=MESH)

    def pair_copy(unit, third):
        return pltpu.make_async_remote_copy(
            grad_of(third, flip(owner_of(unit, third), CORE), 0, THIRD), pair_raw.at[unit - 1, third],
            pair_send.at[unit, third], pair_recv.at[unit, third], device_id=(twin,), device_id_type=MESH)

    def start_first(piece, carry):
        for third in THIRDS:
            pair_first(third, piece).start()
        return carry

    own_small = (
        pltpu.make_async_copy(grad_wide, wide_raw, local_sems.at[0]), pltpu.make_async_copy(grad_vec, vec_raw, local_sems.at[1]))
    for copy in own_small:
        copy.start()

    def loads(unit, third, piece):
        rows = piece * PIECE
        slot = (unit * PIECES + piece) % LOAD_SLOTS
        copies = [
            pltpu.make_async_copy(grad_of(third, owner_of(unit, third), rows, PIECE), raw_own.at[slot, third], load_sems.at[slot, third, 0])]
        if unit > 0:
            copies.append(pltpu.make_async_copy(
                pair_raw.at[unit - 1, third, pl.ds(rows, PIECE)], raw_pair.at[slot, third], load_sems.at[slot, third, 1]))
        for place, source in enumerate(UNITS[unit][2]):
            if source < 6:
                copies.append(pltpu.make_async_copy(
                    landed.at[source, third, pl.ds(rows, PIECE)], partial.at[slot, third, place], load_sems.at[slot, third, 2 + place]))
        return copies

    def send(unit, third, piece):
        rows = piece * PIECE
        slot = (unit * PIECES + piece) % SEND_SLOTS
        to = flip(me, ORDERS[third][UNITS[unit][0]])
        return pltpu.make_async_remote_copy(
            outgoing.at[slot, third], (landed.at[unit, third] if unit < 6 else landed_near.at[third]).at[pl.ds(rows, PIECE)],
            send_sems.at[slot, third], land_sems.at[unit, third, piece], device_id=(to,), device_id_type=MESH)

    def begin(unit, piece):
        for third in THIRDS:
            if unit > 0:
                @pl.when(piece == 0)
                def _():
                    pair_copy(unit, third).wait_recv()
            for source in UNITS[unit][2]:
                if source < 6:
                    send(source, third, piece).wait_recv()
            for copy in loads(unit, third, piece):
                copy.start()

    ahead = LOAD_SLOTS - 1
    for piece in range(ahead):
        begin(0, piece)
    meet_everyone()
    lax.fori_loop(0, PIECES, start_first, 0)

    for unit in range(8):
        def work(piece, carry, unit=unit):
            @pl.when(piece + ahead < PIECES)
            def _():
                begin(unit, piece + ahead)
            if unit < 7:
                @pl.when(piece + ahead >= PIECES)
                def _():
                    begin(unit + 1, piece + ahead - PIECES)
            slot = (unit * PIECES + piece) % LOAD_SLOTS
            out_slot = (unit * PIECES + piece) % SEND_SLOTS
            for third in THIRDS:
                for copy in loads(unit, third, piece):
                    copy.wait()
                rows = pl.ds(pl.multiple_of(piece * PIECE, PIECE), PIECE)
                if unit == 0:
                    pair_first(third, piece).wait_recv()
                    value = raw_own[slot, third].astype(jnp.float32) + pair_near[third, rows].astype(jnp.float32)
                else:
                    value = raw_own[slot, third].astype(jnp.float32) + raw_pair[slot, third].astype(jnp.float32)
                for place, source in enumerate(UNITS[unit][2]):
                    if source < 6:
                        value = value + partial[slot, third, place]
                    else:
                        send(source, third, piece).wait_recv()
                        value = value + landed_near[third, rows]
                if unit < 7:
                    if unit == 0:
                        @pl.when(piece >= SEND_SLOTS)
                        def _():
                            send(unit, third, piece).wait_send()
                    else:
                        send(unit, third, piece).wait_send()
                    outgoing[out_slot, third] = value
                    send(unit, third, piece).start()
                else:
                    value = value * (1.0 / GROUP)
                    sums[pl.ds(pl.multiple_of(third * THIRD + piece * PIECE, PIECE), PIECE)] = value
                    square_sum[...] += jnp.sum((value * value).reshape(PIECE // 8, 8, LANES), axis=0)
            if unit == 0:
                @pl.when(piece == 0)
                def _():
                    for later in range(1, 8):
                        for third in THIRDS:
                            pair_copy(later, third).start()
            return carry

        lax.fori_loop(0, PIECES, work, 0)
        if unit == 0:
            for copy in own_small:
                copy.wait()
            shares_from(wide_raw, vec_raw, wide_rows, vec_rows, packed)
            small_shares[...] = packed[...].astype(jnp.bfloat16)
            small_slots[me] = small_shares[me]
        if unit == 1:
            tile_to_everyone(me, lambda owner: small_shares.at[owner], small_slots, small_send, small_recv, True)
        if unit == 5:
            tile_to_everyone(me, lambda owner: small_shares.at[owner], small_slots, small_send, small_recv, False)
            small = jnp.sum(small_slots[...].astype(jnp.float32), axis=0) * (1.0 / GROUP)
            small_sums[...] = small
            square_sum[...] = (small * small)[0:8] + (small * small)[8:16]

    square_slots[me] = square_sum[...]
    tile_to_everyone(me, lambda owner: square_sum, square_slots, square_send, square_recv, True)
    for slot in range(SEND_SLOTS):
        for third in THIRDS:
            send(6, third, slot).wait_send()

    def drain(piece, carry):
        for third in THIRDS:
            pair_first(third, piece).wait_send()
        return carry

    lax.fori_loop(0, PIECES, drain, 0)
    for unit in range(1, 8):
        for third in THIRDS:
            pair_copy(unit, third).wait_send()
    tile_to_everyone(me, lambda owner: square_sum, square_slots, square_send, square_recv, False)
    total[...] = jnp.full(TILE, jnp.sum(square_slots[...]), jnp.float32)


def reduce_scatter(grad_attn, grad_mlp, grad_wide, grad_vec):
    anywhere = pl.BlockSpec(memory_space=pl.ANY)
    inside = pl.BlockSpec(memory_space=pltpu.VMEM)
    dma = pltpu.SemaphoreType.DMA
    return pl.pallas_call(
        scatter_kernel,
        name="scatter",
        out_shape=(
            pltpu.VMEM((ROWS, LANES), jnp.float32),
            pltpu.VMEM((SMALL_ROWS, LANES), jnp.float32),
            pltpu.VMEM(TILE, jnp.float32),
            pltpu.HBM((7, 3, THIRD, LANES), jnp.bfloat16),
            pltpu.HBM((6, 3, THIRD, LANES), jnp.float32),
        ),
        in_specs=[anywhere] * 4,
        out_specs=(inside, inside, inside, anywhere, anywhere),
        scratch_shapes=[
            pltpu.VMEM((LOAD_SLOTS, 3, PIECE, LANES), jnp.bfloat16),
            pltpu.VMEM((LOAD_SLOTS, 3, PIECE, LANES), jnp.bfloat16),
            pltpu.VMEM((LOAD_SLOTS, 3, 3, PIECE, LANES), jnp.float32),
            pltpu.VMEM((SEND_SLOTS, 3, PIECE, LANES), jnp.float32),
            pltpu.VMEM(TILE, jnp.float32),
            pltpu.VMEM((GROUP, SMALL_ROWS, LANES), jnp.bfloat16),
            pltpu.VMEM((GROUP, 8, LANES), jnp.float32),
            pltpu.VMEM((3, THIRD, LANES), jnp.bfloat16),
            pltpu.VMEM((3, THIRD, LANES), jnp.float32),
            pltpu.VMEM((1, 5120), jnp.bfloat16),
            pltpu.VMEM((11, 1280), jnp.bfloat16),
            pltpu.VMEM((8, 5120), jnp.float32),
            pltpu.VMEM((SMALL_ROWS, 1280), jnp.float32),
            pltpu.VMEM((GROUP, SMALL_ROWS, LANES), jnp.float32),
            pltpu.VMEM((GROUP, SMALL_ROWS, LANES), jnp.bfloat16),
            dma((LOAD_SLOTS, 3, 5)),
            dma((SEND_SLOTS, 3)),
            dma((3, PIECES)),
            dma((3, PIECES)),
            dma((8, 3)),
            dma((8, 3)),
            dma((7, 3, PIECES)),
            dma((GROUP,)),
            dma((GROUP,)),
            dma((GROUP,)),
            dma((GROUP,)),
            dma((2,)),
        ],
        compiler_params=pltpu.CompilerParams(collective_id=0, has_side_effects=True, vmem_limit_bytes=SCATTER_VMEM),
    )(*[pltpu.with_memory_space_constraint(grad, pltpu.HBM) for grad in (grad_attn, grad_mlp, grad_wide, grad_vec)])[:3]


def bank_part(third, attn, mlp):
    return (attn, 0) if third == 0 else (mlp, (third - 1) * THIRD)


def update_kernel(sums, small_sums, total, weight_attn, weight_mlp, first_attn, first_mlp, second_attn, second_mlp,
                  weight_wide, weight_vec, first_wide, first_vec, second_wide, second_vec,
                  update, small_update, small_weight, part_sums, new_first_attn, new_first_mlp, new_second_attn, new_second_mlp,
                  new_first_wide, new_first_vec, new_second_wide, new_second_vec,
                  first_out, second_out, small_first, small_second, out_sems):
    clip_coef = jnp.minimum(1.0, MAX_NORM / jnp.sqrt(total[0:1, :]))

    first_step = (1.0 - BETA_FIRST) * clip_coef
    second_step = (1.0 - BETA_SECOND) * clip_coef * clip_coef
    first_bias = 1.0 - BETA_FIRST ** STEP_NUMBER
    root_scale = first_bias ** 2 / (1.0 - BETA_SECOND ** STEP_NUMBER)

    def direction(mean_grad, weight, first, second):
        new_first = BETA_FIRST * first + first_step * mean_grad
        new_second = BETA_SECOND * second + second_step * (mean_grad * mean_grad)
        square = jnp.maximum(new_second * root_scale, ROOT_FLOOR)
        root = square * lax.rsqrt(square) + EPSILON * first_bias
        return new_first / root + WEIGHT_DECAY * weight, new_first, new_second

    def tile_sum(value):
        return jnp.sum((value * value).reshape(-1, 8, LANES), axis=0)

    def copies(third, chunk):
        slot = (third * CHUNKS + chunk) % OUT_SLOTS
        first_to, base = bank_part(third, new_first_attn, new_first_mlp)
        second_to, _ = bank_part(third, new_second_attn, new_second_mlp)
        rows = pl.ds(base + chunk * CHUNK, CHUNK)
        return (
            pltpu.make_async_copy(first_out.at[slot], first_to.at[rows], out_sems.at[slot, 0]),
            pltpu.make_async_copy(second_out.at[slot], second_to.at[rows], out_sems.at[slot, 1]),
        )

    totals = []
    for third in THIRDS:
        weight, base = bank_part(third, weight_attn, weight_mlp)
        first, _ = bank_part(third, first_attn, first_mlp)
        second, _ = bank_part(third, second_attn, second_mlp)

        def work(chunk, carry, third=third, weight=weight, first=first, second=second, base=base):
            slot = (third * CHUNKS + chunk) % OUT_SLOTS
            place = third * CHUNKS + chunk

            @pl.when(place >= OUT_SLOTS)
            def _():
                for copy in copies(third, chunk):
                    copy.wait()

            def block(step, carry):
                squares_weight, squares_update = carry
                inner = pl.multiple_of(step * BLOCK, BLOCK)
                rows = pl.ds(pl.multiple_of(base + chunk * CHUNK + inner, BLOCK), BLOCK)
                old = weight[rows]
                new_update, new_first, new_second = direction(
                    sums[pl.ds(pl.multiple_of(third * THIRD + chunk * CHUNK + inner, BLOCK), BLOCK)], old, first[rows], second[rows])
                first_out[slot, pl.ds(inner, BLOCK)] = new_first
                second_out[slot, pl.ds(inner, BLOCK)] = new_second
                update[pl.ds(pl.multiple_of(third * THIRD + chunk * CHUNK + inner, BLOCK), BLOCK)] = new_update
                return squares_weight + tile_sum(old), squares_update + tile_sum(new_update)

            carry = lax.fori_loop(0, CHUNK // BLOCK, block, carry)
            for copy in copies(third, chunk):
                copy.start()
            return carry

        zero = jnp.zeros(TILE, jnp.float32)
        totals.append(lax.fori_loop(0, CHUNKS, work, (zero, zero)))
    pack_rows(weight_wide, weight_vec, small_weight)
    pack_rows(first_wide, first_vec, small_first)
    pack_rows(second_wide, second_vec, small_second)
    small, small_m, small_v = direction(small_sums[...], small_weight[...], small_first[...], small_second[...])
    small_update[...] = small
    small_first[...] = small_m
    small_second[...] = small_v
    unpack_rows(small_first, new_first_wide, new_first_vec)
    unpack_rows(small_second, new_second_wide, new_second_vec)
    old = small_weight[...]
    columns = [
        totals[0][0], totals[0][1], totals[1][0] + totals[2][0], totals[1][1] + totals[2][1],
        (old * old)[0:8], (small * small)[0:8], (old * old)[8:16], (small * small)[8:16],
    ]
    lane = lax.broadcasted_iota(jnp.int32, TILE, 1)
    tile = jnp.zeros(TILE, jnp.float32)
    for place, column in enumerate(columns):
        tile = jnp.where(lane == place, jnp.sum(column, axis=1, keepdims=True), tile)
    part_sums[...] = tile
    for place in range(3 * CHUNKS - OUT_SLOTS, 3 * CHUNKS):
        for copy in copies(place // CHUNKS, place % CHUNKS):
            copy.wait()


def resident(value):
    return pltpu.with_memory_space_constraint(value, pltpu.VMEM)


def update_step(sums, small_sums, total, weights, firsts, seconds, smalls):
    anywhere = pl.BlockSpec(memory_space=pl.ANY)
    inside = pl.BlockSpec(memory_space=pltpu.VMEM)
    attn = pltpu.HBM((ATTN_ROWS, LANES), jnp.float32)
    mlp = pltpu.HBM((MLP_ROWS, LANES), jnp.float32)
    wide = jax.ShapeDtypeStruct((1, 320), jnp.float32)
    vec = jax.ShapeDtypeStruct((11, 80), jnp.float32)
    operands = [sums, small_sums, total, *weights, *firsts, *seconds]
    return pl.pallas_call(
        update_kernel,
        name="update",
        out_shape=(
            pltpu.VMEM((ROWS, LANES), jnp.float32),
            pltpu.VMEM((SMALL_ROWS, LANES), jnp.float32),
            pltpu.VMEM((SMALL_ROWS, LANES), jnp.float32),
            pltpu.VMEM(TILE, jnp.float32),
            attn, mlp, attn, mlp, wide, vec, wide, vec,
        ),
        in_specs=[inside] * 15,
        out_specs=(inside,) * 4 + (anywhere,) * 4 + (inside,) * 4,
        scratch_shapes=[
            pltpu.VMEM((OUT_SLOTS, CHUNK, LANES), jnp.float32),
            pltpu.VMEM((OUT_SLOTS, CHUNK, LANES), jnp.float32),
            pltpu.VMEM((SMALL_ROWS, LANES), jnp.float32),
            pltpu.VMEM((SMALL_ROWS, LANES), jnp.float32),
            pltpu.SemaphoreType.DMA((OUT_SLOTS, 2)),
        ],
        compiler_params=pltpu.CompilerParams(vmem_limit_bytes=UPDATE_VMEM),
    )(*[resident(value) for value in operands], *smalls)


def gather_kernel(part_sums, weight_attn, weight_mlp, update, small_weight, small_update,
                  everything, all_wide, all_vec, new_weight, new_wide, new_vec,
                  all_small, fresh_small, new_small, slots, wide_flat, pair,
                  tile_send, tile_recv, small_send, small_recv, link_send, link_recv, twin_send, twin_recv,
                  own_send, own_recv, last_send, last_recv, last_twin_send, last_twin_recv):
    me = lax.axis_index("data")
    twin = flip(me, CORE)
    greet_everyone(me)
    meet_everyone()
    slots[me] = part_sums[...]
    tile_to_everyone(me, lambda owner: part_sums, slots, tile_send, tile_recv, True)
    tile_to_everyone(me, lambda owner: part_sums, slots, tile_send, tile_recv, False)
    sums = jnp.sum(slots[...], axis=0)
    lane = lax.broadcasted_iota(jnp.int32, TILE, 1)

    def column(place):
        return jnp.sum(jnp.where(lane == place, sums, 0.0), axis=1, keepdims=True)

    def same_tensor(value, rows):
        total = value
        for shift in range(rows, 8, rows):
            total = total + pltpu.roll(value, shift, 0)
        return total

    def wide_rows(value):
        row = lax.broadcasted_iota(jnp.int32, (8, 1), 0)
        mine = jnp.logical_and(row >= 3, row < 6)
        return jnp.where(mine, jnp.sum(jnp.where(mine, value, 0.0), axis=0, keepdims=True), value)

    def spread(value):
        return jnp.broadcast_to(value, TILE)

    def ratio(weights, updates):
        safe = jnp.where(updates > 0.0, updates, 1.0)
        return jnp.sqrt(weights) / jnp.sqrt(safe)

    ratio_attn = ratio(same_tensor(spread(column(0)), 4), same_tensor(spread(column(1)), 4))
    ratio_mlp = ratio(same_tensor(spread(column(2)), 2), same_tensor(spread(column(3)), 2))
    ratio_low = ratio(spread(column(4)), spread(column(5)))
    ratio_high = ratio(spread(wide_rows(column(6))), spread(wide_rows(column(7))))

    def place_of(third, owner):
        return everything.at[owner, pl.ds(third * THIRD, THIRD)]

    def link(third, stage, hops):
        number = ARRIVALS.index((stage, hops))
        to = flip(me, ORDERS[third][stage])
        owner = flip_all(me, [ORDERS[third][hop] for hop in hops])
        place = place_of(third, owner)
        return pltpu.make_async_remote_copy(
            place, place, link_send.at[third, number], link_recv.at[third, number],
            device_id=(to,), device_id_type=MESH)

    def landed(third, stage, hops):
        number = ARRIVALS.index((stage, hops))
        owner = flip_all(flip(me, ORDERS[third][stage]), [ORDERS[third][hop] for hop in hops])
        place = place_of(third, owner)
        return pltpu.make_async_remote_copy(
            place, place, link_send.at[third, number], link_recv.at[third, number],
            device_id=(flip(me, ORDERS[third][stage]),), device_id_type=MESH)

    def to_twin(third, number, hops):
        owner = flip_all(me, [ORDERS[third][hop] for hop in hops])
        place = place_of(third, owner)
        return pltpu.make_async_remote_copy(
            place, place, twin_send.at[third, number], twin_recv.at[third, number],
            device_id=(twin,), device_id_type=MESH)

    def from_twin(third, number, hops):
        owner = flip_all(twin, [ORDERS[third][hop] for hop in hops])
        place = place_of(third, owner)
        return pltpu.make_async_remote_copy(
            place, place, twin_send.at[third, number], twin_recv.at[third, number],
            device_id=(twin,), device_id_type=MESH)

    def own_part(third, part, owner):
        start, rows = OWN_PARTS[part]
        place = everything.at[owner, pl.ds(third * THIRD + start, rows)]
        return pltpu.make_async_remote_copy(
            place, place, own_send.at[third, part], own_recv.at[third, part],
            device_id=(flip(me, ORDERS[third][0]),), device_id_type=MESH)

    for part, (first_row, rows_here) in enumerate(OWN_PARTS):
        for third in THIRDS:
            scale = LEARN_RATE * (ratio_attn if third == 0 else ratio_mlp)
            weight, base = bank_part(third, weight_attn, weight_mlp)

            def refresh(piece, carry, third=third, scale=scale, weight=weight, base=base, first_row=first_row):
                row = first_row + piece * BLOCK
                rows = pl.ds(pl.multiple_of(third * THIRD + row, BLOCK), BLOCK)
                old = weight[pl.ds(pl.multiple_of(base + row, BLOCK), BLOCK)].reshape((-1,) + TILE)
                new = (old - scale[None] * update[rows].reshape((-1,) + TILE)).reshape(BLOCK, LANES)
                new_weight[rows] = new
                everything[me, rows] = new.astype(jnp.bfloat16)
                return carry

            lax.fori_loop(0, rows_here // BLOCK, refresh, 0)
            own_part(third, part, me).start()
    for stage in (1, 2):
        for third in THIRDS:
            link(third, stage, ()).start()
    for third in THIRDS:
        to_twin(third, 0, ()).start()
    low = small_weight[0:8] - LEARN_RATE * ratio_low * small_update[0:8]
    high = small_weight[8:16] - LEARN_RATE * ratio_high * small_update[8:16]
    new_small[...] = jnp.concatenate([low, high], axis=0)
    unpack_rows(new_small, new_wide, new_vec)
    fresh_small[...] = new_small[...].astype(jnp.bfloat16)
    all_small[me] = fresh_small[...]
    tile_to_everyone(me, lambda owner: fresh_small, all_small, small_send, small_recv, True)

    def last_part(third, part, owner, to, send_sem, recv_sem):
        place = everything.at[owner, pl.ds(third * THIRD + part * LAST, LAST)]
        return pltpu.make_async_remote_copy(
            place, place, send_sem.at[third, part], recv_sem.at[third, part], device_id=(to,), device_id_type=MESH)

    def last_link(third, part):
        owner = flip_all(me, ORDERS[third][:2])
        return last_part(third, part, owner, flip(me, ORDERS[third][2]), last_send, last_recv)

    def last_landed(third, part):
        return last_part(third, part, flip_all(me, ORDERS[third]), flip(me, ORDERS[third][2]), last_send, last_recv)

    def last_to_twin(third, part):
        return last_part(third, part, flip_all(me, ORDERS[third]), twin, last_twin_send, last_twin_recv)

    def last_from_twin(third, part):
        return last_part(third, part, flip_all(twin, ORDERS[third]), twin, last_twin_send, last_twin_recv)

    sent = []
    for number, (stage, hops) in enumerate(ARRIVALS):
        for third in THIRDS:
            if number == 0:
                for part in range(len(OWN_PARTS)):
                    own_part(third, part, flip(me, ORDERS[third][0])).wait_recv()
            else:
                landed(third, stage, hops).wait_recv()
            for later in () if hops else range(stage + 1, len(THIRDS)):
                copy = link(third, later, (stage,))
                copy.start()
                sent.append(copy)
            if hops and stage == 1:
                for part in range(PARTS):
                    last_link(third, part).start()
            to_twin(third, number + 1, (stage,) + hops).start()
        if number == 2:
            tile_to_everyone(me, lambda owner: fresh_small, all_small, small_send, small_recv, False)
            shares_to(all_small, all_wide, all_vec, wide_flat, pair)
    for number, hops in enumerate(((),) + tuple((stage,) + hops for stage, hops in ARRIVALS)):
        for third in THIRDS:
            from_twin(third, number, hops).wait_recv()
            to_twin(third, number, hops).wait_send()
    for third in THIRDS:
        for part in range(len(OWN_PARTS)):
            own_part(third, part, me).wait_send()
        for stage in (1, 2):
            link(third, stage, ()).wait_send()
    for copy in sent:
        copy.wait_send()
    for part in range(PARTS):
        for third in THIRDS:
            last_landed(third, part).wait_recv()
            last_to_twin(third, part).start()
    for part in range(PARTS):
        for third in THIRDS:
            last_link(third, part).wait_send()
            last_to_twin(third, part).wait_send()
            last_from_twin(third, part).wait_recv()


def all_gather(part_sums, weights, update, small_weight, small_update):
    inside = pl.BlockSpec(memory_space=pltpu.VMEM)
    dma = pltpu.SemaphoreType.DMA
    return pl.pallas_call(
        gather_kernel,
        name="gather",
        out_shape=(
            pltpu.VMEM((GROUP, ROWS, LANES), jnp.bfloat16),
            pltpu.VMEM((1, WIDE), jnp.bfloat16),
            pltpu.VMEM((VECS, VEC), jnp.bfloat16),
            pltpu.VMEM((ROWS, LANES), jnp.float32),
            pltpu.VMEM((1, WIDE_SHARE), jnp.float32),
            pltpu.VMEM((VECS, VEC_SHARE), jnp.float32),
        ),
        in_specs=[inside] * 6,
        out_specs=(inside,) * 6,
        scratch_shapes=[
            pltpu.VMEM((GROUP, SMALL_ROWS, LANES), jnp.bfloat16),
            pltpu.VMEM((SMALL_ROWS, LANES), jnp.bfloat16),
            pltpu.VMEM((SMALL_ROWS, LANES), jnp.float32),
            pltpu.VMEM((GROUP, 8, LANES), jnp.float32),
            pltpu.VMEM((8, 5120), jnp.float32),
            pltpu.VMEM((2, SMALL_ROWS, LANES), jnp.float32),
            *[dma((GROUP,))] * 4,
            *[dma((len(THIRDS), len(ARRIVALS)))] * 2, *[dma((len(THIRDS), len(ARRIVALS) + 1))] * 2, *[dma((len(THIRDS), len(OWN_PARTS)))] * 2, *[dma((len(THIRDS), PARTS))] * 4,
        ],
        compiler_params=pltpu.CompilerParams(collective_id=1, has_side_effects=True, vmem_limit_bytes=GATHER_VMEM),
    )(*[resident(value) for value in (part_sums, *weights, update, small_weight, small_update)])


def write_kernel(everything, replica_attn, replica_mlp, attn_sems, mlp_sems):
    writes = []
    for owner in range(GROUP):
        writes.append(pltpu.make_async_copy(
            everything.at[owner, pl.ds(0, ATTN_ROWS)], replica_attn.at[pl.ds(owner * ATTN_ROWS, ATTN_ROWS)], attn_sems.at[owner]))
        writes.append(pltpu.make_async_copy(
            everything.at[owner, pl.ds(ATTN_ROWS, MLP_ROWS)], replica_mlp.at[pl.ds(owner * MLP_ROWS, MLP_ROWS)], mlp_sems.at[owner]))
    for copy in writes:
        copy.start()
    for copy in writes:
        copy.wait()


def write_replica(everything):
    anywhere = pl.BlockSpec(memory_space=pl.ANY)
    dma = pltpu.SemaphoreType.DMA
    return pl.pallas_call(
        write_kernel,
        name="write",
        out_shape=(
            pltpu.HBM((GROUP * ATTN_ROWS, LANES), jnp.bfloat16),
            pltpu.HBM((GROUP * MLP_ROWS, LANES), jnp.bfloat16),
        ),
        in_specs=[pl.BlockSpec(memory_space=pltpu.VMEM)],
        out_specs=(anywhere,) * 2,
        scratch_shapes=[dma((GROUP,)), dma((GROUP,))],
        compiler_params=pltpu.CompilerParams(vmem_limit_bytes=FINISH_VMEM),
    )(resident(everything))


def finish_kernel(new_weight, wide_in, vec_in, all_wide, all_vec, new_attn, new_mlp, new_wide, new_vec, replica_wide, replica_vec, sems):
    copies = [
        pltpu.make_async_copy(new_weight.at[pl.ds(0, ATTN_ROWS)], new_attn, sems.at[0]),
        pltpu.make_async_copy(new_weight.at[pl.ds(ATTN_ROWS, MLP_ROWS)], new_mlp, sems.at[1]),
    ]
    for number, (source, to) in enumerate(((wide_in, new_wide), (vec_in, new_vec), (all_wide, replica_wide), (all_vec, replica_vec))):
        copies.append(pltpu.make_async_copy(source, to, sems.at[number + 2]))
    for copy in copies:
        copy.start()
    for copy in copies:
        copy.wait()


def finish(new_weight, new_wide, new_vec, all_wide, all_vec):
    anywhere = pl.BlockSpec(memory_space=pl.ANY)
    inside = pl.BlockSpec(memory_space=pltpu.VMEM)
    return pl.pallas_call(
        finish_kernel,
        name="finish",
        out_shape=(
            pltpu.HBM((ATTN_ROWS, LANES), jnp.float32),
            pltpu.HBM((MLP_ROWS, LANES), jnp.float32),
            pltpu.HBM(new_wide.shape, jnp.float32),
            pltpu.HBM(new_vec.shape, jnp.float32),
            pltpu.HBM(all_wide.shape, jnp.bfloat16),
            pltpu.HBM(all_vec.shape, jnp.bfloat16),
        ),
        in_specs=[inside] * 5,
        out_specs=(anywhere,) * 6,
        scratch_shapes=[pltpu.SemaphoreType.DMA((6,))],
        compiler_params=pltpu.CompilerParams(vmem_limit_bytes=FINISH_VMEM),
    )(*[resident(value) for value in (new_weight, new_wide, new_vec, all_wide, all_vec)])


def linear(bank):
    rows, length = bank.shape
    return bank.reshape(rows, length // LANES, LANES).transpose(1, 0, 2).reshape(rows * length // LANES, LANES)


def banked(flat, rows):
    blocks = flat.size // (rows * LANES)
    return flat.reshape(blocks, rows, LANES).transpose(1, 0, 2).reshape(rows, blocks * LANES)


def solution(mesh):
    grad_spec = P("data", None, None)
    shard_spec = P(None, "data")
    full_spec = P(None, None)

    def local_step(*banks):
        grads = banks[0:4]
        attn_grad = linear(grads[0][0]).reshape(GROUP, ATTN_ROWS, LANES)
        mlp_grad = linear(grads[1][0]).reshape(GROUP, MLP_ROWS, LANES)
        states = [(linear(banks[first]), linear(banks[first + 1])) for first in (4, 8, 12)]
        smalls = [bank for first in (4, 8, 12) for bank in banks[first + 2:first + 4]]
        sums, small_sums, total = reduce_scatter(attn_grad, mlp_grad, grads[2][0], grads[3][0])
        update, small_update, small_weight, part_sums, *moments = update_step(sums, small_sums, total, *states, smalls)
        everything, all_wide, all_vec, *new = all_gather(part_sums, states[0], update, small_weight, small_update)
        replica_attn, replica_mlp = write_replica(everything)
        replica_attn, all_wide = lax.optimization_barrier((replica_attn, all_wide))
        new_attn, new_mlp, new_wide, new_vec, replica_wide, replica_vec = finish(*new, all_wide, all_vec)
        return (
            banked(replica_attn, 4), banked(replica_mlp, 2), replica_wide, replica_vec,
            banked(new_attn, 4), banked(new_mlp, 2), new_wide, new_vec,
            banked(moments[0], 4), banked(moments[1], 2), moments[4], moments[5],
            banked(moments[2], 4), banked(moments[3], 2), moments[6], moments[7],
        )

    return jax.shard_map(local_step, mesh=mesh, in_specs=(grad_spec,) * 4 + (shard_spec,) * 12, out_specs=(full_spec,) * 4 + (shard_spec,) * 12, check_vma=False)
```

```python
import functools

import jax
import jax.numpy as jnp
from jax import lax
from jax.experimental import pallas as pl
from jax.experimental.pallas import tpu as pltpu
from jax.sharding import PartitionSpec as P

STEP_NUMBER = 10
LEARN_RATE = 0.04
BETA_FIRST = 0.9
BETA_SECOND = 0.999
EPSILON = 1e-6
WEIGHT_DECAY = 0.01
MAX_NORM = 1.0
ROOT_FLOOR = 1e-36

MESH = pl.DeviceIdType.MESH
GROUP = 16
LANES = 128
TILE = (8, LANES)
THIRDS = range(3)
VECS = 11
VEC_SHARE = 80
VEC = 1280
WIDE = 5120
WIDE_PARTS = ((0, LANES), (1, LANES), (2, 64))
WIDE_SHARE = 320
MIB = 2 ** 20
ATTN_ROWS = 3200
MLP_ROWS = 6400
ROWS = ATTN_ROWS + MLP_ROWS
THIRD = 3200
PIECE = 400
PIECES = THIRD // PIECE
LOAD_SLOTS = 3
SEND_SLOTS = 4
SMALL_ROWS = 16
BLOCK = 640
PARTS = 4
LAST = THIRD // PARTS
OWN_PARTS = ((0, 640), (640, 2560))
CHUNK = 640
CHUNKS = THIRD // CHUNK
OUT_SLOTS = 4
SCATTER_VMEM = 36 * MIB
UPDATE_VMEM = 8 * MIB
GATHER_VMEM = 2 * MIB
FINISH_VMEM = 3 * MIB
CORE = 1
ORDERS = ((2, 4, 8), (4, 8, 2), (8, 2, 4))
MASKS = sorted(range(1, GROUP), key=lambda mask: (-(mask // 2).bit_count(), mask))
UNITS = (
    (0, (0, 1, 2), ()),
    (0, (0, 1), ()),
    (0, (0, 2), ()),
    (1, (1, 2), (0,)),
    (0, (0,), ()),
    (1, (1,), (1,)),
    (2, (2,), (2, 3)),
    (None, (), (4, 5, 6)),
)


ARRIVALS = [(0, ()), (1, ()), (2, ()), (1, (0,)), (2, (0,)), (2, (1,))]


def flip(index, width):
    return index + width * (1 - 2 * ((index // width) % 2))


def flip_all(index, widths):
    for width in widths:
        index = flip(index, width)
    return index


def across(me, mask):
    return flip_all(me, [width for width in (CORE,) + ORDERS[0] if mask & width])


def greet_everyone(me):
    for mask in MASKS:
        pl.semaphore_signal(pltpu.get_barrier_semaphore(), inc=1, device_id=(across(me, mask),), device_id_type=MESH)


def meet_everyone():
    pl.semaphore_wait(pltpu.get_barrier_semaphore(), GROUP - 1)


def tile_to_everyone(me, source_of, slots, send_sems, recv_sems, begin):
    for mask in MASKS:
        other = across(me, mask)

        def copy(slot):
            return pltpu.make_async_remote_copy(
                source_of(other), slots.at[slot], send_sems.at[mask], recv_sems.at[mask], device_id=(other,), device_id_type=MESH)

        if begin:
            copy(me).start()
        else:
            copy(other).wait()


def small_places(packed, wide, vec):
    places = [(packed.at[pl.ds(0, VECS), pl.ds(0, VEC_SHARE)], vec)]
    for part, width in WIDE_PARTS:
        places.append((packed.at[pl.ds(VECS + part, 1), pl.ds(0, width)], wide.at[:, pl.ds(LANES * part, width)]))
    return places


def pack_rows(wide, vec, packed):
    packed[...] = jnp.zeros_like(packed)
    for inner, outer in small_places(packed, wide, vec):
        inner[...] = outer[...]


def unpack_rows(packed, wide, vec):
    for inner, outer in small_places(packed, wide, vec):
        outer[...] = inner[...]


def shares_from(wide, vec, wide_rows, vec_rows, packed):
    wide_rows[...] = jnp.zeros_like(wide_rows)
    wide_rows[:1] = wide[...].astype(jnp.float32)
    vec_rows[...] = jnp.zeros_like(vec_rows)
    vec_rows[:VECS] = vec[...].astype(jnp.float32)
    packed[...] = jnp.zeros_like(packed)

    def window(rows, start):
        block, shift = start // LANES * LANES, start % LANES
        value = rows[:, block:block + LANES]
        if shift == 0:
            return value
        lane = lax.broadcasted_iota(jnp.int32, value.shape, 1)
        value = pltpu.roll(value, LANES - shift, 1)
        if block + LANES == rows.shape[1]:
            return value
        after = pltpu.roll(rows[:, block + LANES:block + 2 * LANES], LANES - shift, 1)
        return jnp.where(lane < LANES - shift, value, after)

    lane = lax.broadcasted_iota(jnp.int32, (SMALL_ROWS, LANES), 1)
    for owner in range(GROUP):
        packed[owner] = jnp.where(lane < VEC_SHARE, window(vec_rows, VEC_SHARE * owner), 0.0)
        for part, width in WIDE_PARTS:
            value = window(wide_rows, WIDE_SHARE * owner + LANES * part)
            packed[owner, pl.ds(VECS + part, 1)] = jnp.where(lane[:1] < width, value[:1], 0.0)


def shares_to(shares, wide, vec, wide_rows, pair):
    lane = lax.broadcasted_iota(jnp.int32, (SMALL_ROWS, LANES), 1)
    low = lax.broadcasted_iota(jnp.int32, (1, LANES), 1) < 64
    for block in range(VEC // LANES):
        value = jnp.zeros((SMALL_ROWS, LANES), jnp.float32)
        for owner in range(GROUP):
            begin, end = max(VEC_SHARE * owner, LANES * block), min(VEC_SHARE * (owner + 1), LANES * (block + 1))
            if begin < end:
                shift = (VEC_SHARE * owner - LANES * block) % LANES
                moved = shares[owner].astype(jnp.float32)
                if shift:
                    moved = pltpu.roll(moved, shift, 1)
                inside = jnp.logical_and(lane >= begin - LANES * block, lane < end - LANES * block)
                value = jnp.where(inside, moved, value)
        vec[:, LANES * block:LANES * (block + 1)] = value[:VECS].astype(jnp.bfloat16)
    for place in range(GROUP // 2):
        pair[0] = shares[2 * place].astype(jnp.float32)
        pair[1] = pltpu.roll(shares[2 * place + 1].astype(jnp.float32), 64, 1)
        even, odd = [[pair[half, pl.ds(VECS + part, 1)] for part, _ in WIDE_PARTS] for half in range(2)]
        blocks = [
            even[0], even[1], jnp.where(low, even[2], odd[0]), jnp.where(low, odd[0], odd[1]), jnp.where(low, odd[1], odd[2]),
        ]
        for number, value in enumerate(blocks):
            wide_rows[:1, pl.ds(LANES * (len(blocks) * place + number), LANES)] = value
    wide[...] = wide_rows[:1].astype(jnp.bfloat16)


def scatter_kernel(grad_attn, grad_mlp, grad_wide, grad_vec, sums, small_sums, total, pair_raw, landed,
                   raw_own, raw_pair, partial, outgoing, square_sum, small_slots, square_slots,
                   pair_near, landed_near, wide_raw, vec_raw, wide_rows, vec_rows, packed, small_shares,
                   load_sems, send_sems, pair_send_first, pair_recv_first, pair_send, pair_recv, land_sems,
                   small_send, small_recv, square_send, square_recv, local_sems):
    me = lax.axis_index("data")
    twin = flip(me, CORE)
    greet_everyone(me)

    def grad_of(third, owner, row, count):
        if third == 0:
            return grad_attn.at[owner, pl.ds(row, count)]
        return grad_mlp.at[owner, pl.ds(row + (third - 1) * THIRD, count)]

    def owner_of(unit, third):
        return flip_all(me, [ORDERS[third][place] for place in UNITS[unit][1]])

    def pair_first(third, piece):
        rows = piece * PIECE
        return pltpu.make_async_remote_copy(
            grad_of(third, flip(owner_of(0, third), CORE), rows, PIECE), pair_near.at[third, pl.ds(rows, PIECE)],
            pair_send_first.at[third, piece], pair_recv_first.at[third, piece], device_id=(twin,), device_id_type=MESH)

    def pair_copy(unit, third):
        return pltpu.make_async_remote_copy(
            grad_of(third, flip(owner_of(unit, third), CORE), 0, THIRD), pair_raw.at[unit - 1, third],
            pair_send.at[unit, third], pair_recv.at[unit, third], device_id=(twin,), device_id_type=MESH)

    def start_first(piece, carry):
        for third in THIRDS:
            pair_first(third, piece).start()
        return carry

    own_small = (
        pltpu.make_async_copy(grad_wide, wide_raw, local_sems.at[0]), pltpu.make_async_copy(grad_vec, vec_raw, local_sems.at[1]))
    for copy in own_small:
        copy.start()

    def loads(unit, third, piece):
        rows = piece * PIECE
        slot = (unit * PIECES + piece) % LOAD_SLOTS
        copies = [
            pltpu.make_async_copy(grad_of(third, owner_of(unit, third), rows, PIECE), raw_own.at[slot, third], load_sems.at[slot, third, 0])]
        if unit > 0:
            copies.append(pltpu.make_async_copy(
                pair_raw.at[unit - 1, third, pl.ds(rows, PIECE)], raw_pair.at[slot, third], load_sems.at[slot, third, 1]))
        for place, source in enumerate(UNITS[unit][2]):
            if source < 6:
                copies.append(pltpu.make_async_copy(
                    landed.at[source, third, pl.ds(rows, PIECE)], partial.at[slot, third, place], load_sems.at[slot, third, 2 + place]))
        return copies

    def send(unit, third, piece):
        rows = piece * PIECE
        slot = (unit * PIECES + piece) % SEND_SLOTS
        to = flip(me, ORDERS[third][UNITS[unit][0]])
        return pltpu.make_async_remote_copy(
            outgoing.at[slot, third], (landed.at[unit, third] if unit < 6 else landed_near.at[third]).at[pl.ds(rows, PIECE)],
            send_sems.at[slot, third], land_sems.at[unit, third, piece], device_id=(to,), device_id_type=MESH)

    def begin(unit, piece):
        for third in THIRDS:
            if unit > 0:
                @pl.when(piece == 0)
                def _():
                    pair_copy(unit, third).wait_recv()
            for source in UNITS[unit][2]:
                if source < 6:
                    send(source, third, piece).wait_recv()
            for copy in loads(unit, third, piece):
                copy.start()

    ahead = LOAD_SLOTS - 1
    for piece in range(ahead):
        begin(0, piece)
    meet_everyone()
    lax.fori_loop(0, PIECES, start_first, 0)

    for unit in range(8):
        def work(piece, carry, unit=unit):
            @pl.when(piece + ahead < PIECES)
            def _():
                begin(unit, piece + ahead)
            if unit < 7:
                @pl.when(piece + ahead >= PIECES)
                def _():
                    begin(unit + 1, piece + ahead - PIECES)
            slot = (unit * PIECES + piece) % LOAD_SLOTS
            out_slot = (unit * PIECES + piece) % SEND_SLOTS
            for third in THIRDS:
                for copy in loads(unit, third, piece):
                    copy.wait()
                rows = pl.ds(pl.multiple_of(piece * PIECE, PIECE), PIECE)
                if unit == 0:
                    pair_first(third, piece).wait_recv()
                    value = raw_own[slot, third].astype(jnp.float32) + pair_near[third, rows].astype(jnp.float32)
                else:
                    value = raw_own[slot, third].astype(jnp.float32) + raw_pair[slot, third].astype(jnp.float32)
                for place, source in enumerate(UNITS[unit][2]):
                    if source < 6:
                        value = value + partial[slot, third, place]
                    else:
                        send(source, third, piece).wait_recv()
                        value = value + landed_near[third, rows]
                if unit < 7:
                    if unit == 0:
                        @pl.when(piece >= SEND_SLOTS)
                        def _():
                            send(unit, third, piece).wait_send()
                    else:
                        send(unit, third, piece).wait_send()
                    outgoing[out_slot, third] = value
                    send(unit, third, piece).start()
                else:
                    value = value * (1.0 / GROUP)
                    sums[pl.ds(pl.multiple_of(third * THIRD + piece * PIECE, PIECE), PIECE)] = value
                    square_sum[...] += jnp.sum((value * value).reshape(PIECE // 8, 8, LANES), axis=0)
            if unit == 0:
                @pl.when(piece == 0)
                def _():
                    for later in range(1, 8):
                        for third in THIRDS:
                            pair_copy(later, third).start()
            return carry

        lax.fori_loop(0, PIECES, work, 0)
        if unit == 0:
            for copy in own_small:
                copy.wait()
            shares_from(wide_raw, vec_raw, wide_rows, vec_rows, packed)
            small_shares[...] = packed[...].astype(jnp.bfloat16)
            small_slots[me] = small_shares[me]
        if unit == 1:
            tile_to_everyone(me, lambda owner: small_shares.at[owner], small_slots, small_send, small_recv, True)
        if unit == 5:
            tile_to_everyone(me, lambda owner: small_shares.at[owner], small_slots, small_send, small_recv, False)
            small = jnp.sum(small_slots[...].astype(jnp.float32), axis=0) * (1.0 / GROUP)
            small_sums[...] = small
            square_sum[...] = (small * small)[0:8] + (small * small)[8:16]

    square_slots[me] = square_sum[...]
    tile_to_everyone(me, lambda owner: square_sum, square_slots, square_send, square_recv, True)
    for slot in range(SEND_SLOTS):
        for third in THIRDS:
            send(6, third, slot).wait_send()

    def drain(piece, carry):
        for third in THIRDS:
            pair_first(third, piece).wait_send()
        return carry

    lax.fori_loop(0, PIECES, drain, 0)
    for unit in range(1, 8):
        for third in THIRDS:
            pair_copy(unit, third).wait_send()
    tile_to_everyone(me, lambda owner: square_sum, square_slots, square_send, square_recv, False)
    total[...] = jnp.full(TILE, jnp.sum(square_slots[...]), jnp.float32)


def reduce_scatter(grad_attn, grad_mlp, grad_wide, grad_vec):
    anywhere = pl.BlockSpec(memory_space=pl.ANY)
    inside = pl.BlockSpec(memory_space=pltpu.VMEM)
    dma = pltpu.SemaphoreType.DMA
    return pl.pallas_call(
        scatter_kernel,
        name="scatter",
        out_shape=(
            pltpu.VMEM((ROWS, LANES), jnp.float32),
            pltpu.VMEM((SMALL_ROWS, LANES), jnp.float32),
            pltpu.VMEM(TILE, jnp.float32),
            pltpu.HBM((7, 3, THIRD, LANES), jnp.bfloat16),
            pltpu.HBM((6, 3, THIRD, LANES), jnp.float32),
        ),
        in_specs=[anywhere] * 4,
        out_specs=(inside, inside, inside, anywhere, anywhere),
        scratch_shapes=[
            pltpu.VMEM((LOAD_SLOTS, 3, PIECE, LANES), jnp.bfloat16),
            pltpu.VMEM((LOAD_SLOTS, 3, PIECE, LANES), jnp.bfloat16),
            pltpu.VMEM((LOAD_SLOTS, 3, 3, PIECE, LANES), jnp.float32),
            pltpu.VMEM((SEND_SLOTS, 3, PIECE, LANES), jnp.float32),
            pltpu.VMEM(TILE, jnp.float32),
            pltpu.VMEM((GROUP, SMALL_ROWS, LANES), jnp.bfloat16),
            pltpu.VMEM((GROUP, 8, LANES), jnp.float32),
            pltpu.VMEM((3, THIRD, LANES), jnp.bfloat16),
            pltpu.VMEM((3, THIRD, LANES), jnp.float32),
            pltpu.VMEM((1, 5120), jnp.bfloat16),
            pltpu.VMEM((11, 1280), jnp.bfloat16),
            pltpu.VMEM((8, 5120), jnp.float32),
            pltpu.VMEM((SMALL_ROWS, 1280), jnp.float32),
            pltpu.VMEM((GROUP, SMALL_ROWS, LANES), jnp.float32),
            pltpu.VMEM((GROUP, SMALL_ROWS, LANES), jnp.bfloat16),
            dma((LOAD_SLOTS, 3, 5)),
            dma((SEND_SLOTS, 3)),
            dma((3, PIECES)),
            dma((3, PIECES)),
            dma((8, 3)),
            dma((8, 3)),
            dma((7, 3, PIECES)),
            dma((GROUP,)),
            dma((GROUP,)),
            dma((GROUP,)),
            dma((GROUP,)),
            dma((2,)),
        ],
        compiler_params=pltpu.CompilerParams(collective_id=0, has_side_effects=True, vmem_limit_bytes=SCATTER_VMEM),
    )(*[pltpu.with_memory_space_constraint(grad, pltpu.HBM) for grad in (grad_attn, grad_mlp, grad_wide, grad_vec)])[:3]


def bank_part(third, attn, mlp):
    return (attn, 0) if third == 0 else (mlp, (third - 1) * THIRD)


def update_kernel(sums, small_sums, total, weight_attn, weight_mlp, first_attn, first_mlp, second_attn, second_mlp,
                  weight_wide, weight_vec, first_wide, first_vec, second_wide, second_vec,
                  update, small_update, small_weight, part_sums, new_first_attn, new_first_mlp, new_second_attn, new_second_mlp,
                  new_first_wide, new_first_vec, new_second_wide, new_second_vec,
                  first_out, second_out, small_first, small_second, out_sems):
    clip_coef = jnp.minimum(1.0, MAX_NORM / jnp.sqrt(total[0:1, :]))

    first_step = (1.0 - BETA_FIRST) * clip_coef
    second_step = (1.0 - BETA_SECOND) * clip_coef * clip_coef
    first_bias = 1.0 - BETA_FIRST ** STEP_NUMBER
    root_scale = first_bias ** 2 / (1.0 - BETA_SECOND ** STEP_NUMBER)

    def direction(mean_grad, weight, first, second):
        new_first = BETA_FIRST * first + first_step * mean_grad
        new_second = BETA_SECOND * second + second_step * (mean_grad * mean_grad)
        square = jnp.maximum(new_second * root_scale, ROOT_FLOOR)
        root = square * lax.rsqrt(square) + EPSILON * first_bias
        return new_first / root + WEIGHT_DECAY * weight, new_first, new_second

    def tile_sum(value):
        return jnp.sum((value * value).reshape(-1, 8, LANES), axis=0)

    def copies(third, chunk):
        slot = (third * CHUNKS + chunk) % OUT_SLOTS
        first_to, base = bank_part(third, new_first_attn, new_first_mlp)
        second_to, _ = bank_part(third, new_second_attn, new_second_mlp)
        rows = pl.ds(base + chunk * CHUNK, CHUNK)
        return (
            pltpu.make_async_copy(first_out.at[slot], first_to.at[rows], out_sems.at[slot, 0]),
            pltpu.make_async_copy(second_out.at[slot], second_to.at[rows], out_sems.at[slot, 1]),
        )

    totals = []
    for third in THIRDS:
        weight, base = bank_part(third, weight_attn, weight_mlp)
        first, _ = bank_part(third, first_attn, first_mlp)
        second, _ = bank_part(third, second_attn, second_mlp)

        def work(chunk, carry, third=third, weight=weight, first=first, second=second, base=base):
            slot = (third * CHUNKS + chunk) % OUT_SLOTS
            place = third * CHUNKS + chunk

            @pl.when(place >= OUT_SLOTS)
            def _():
                for copy in copies(third, chunk):
                    copy.wait()

            def block(step, carry):
                squares_weight, squares_update = carry
                inner = pl.multiple_of(step * BLOCK, BLOCK)
                rows = pl.ds(pl.multiple_of(base + chunk * CHUNK + inner, BLOCK), BLOCK)
                old = weight[rows]
                new_update, new_first, new_second = direction(
                    sums[pl.ds(pl.multiple_of(third * THIRD + chunk * CHUNK + inner, BLOCK), BLOCK)], old, first[rows], second[rows])
                first_out[slot, pl.ds(inner, BLOCK)] = new_first
                second_out[slot, pl.ds(inner, BLOCK)] = new_second
                update[pl.ds(pl.multiple_of(third * THIRD + chunk * CHUNK + inner, BLOCK), BLOCK)] = new_update
                return squares_weight + tile_sum(old), squares_update + tile_sum(new_update)

            carry = lax.fori_loop(0, CHUNK // BLOCK, block, carry)
            for copy in copies(third, chunk):
                copy.start()
            return carry

        zero = jnp.zeros(TILE, jnp.float32)
        totals.append(lax.fori_loop(0, CHUNKS, work, (zero, zero)))
    pack_rows(weight_wide, weight_vec, small_weight)
    pack_rows(first_wide, first_vec, small_first)
    pack_rows(second_wide, second_vec, small_second)
    small, small_m, small_v = direction(small_sums[...], small_weight[...], small_first[...], small_second[...])
    small_update[...] = small
    small_first[...] = small_m
    small_second[...] = small_v
    unpack_rows(small_first, new_first_wide, new_first_vec)
    unpack_rows(small_second, new_second_wide, new_second_vec)
    old = small_weight[...]
    columns = [
        totals[0][0], totals[0][1], totals[1][0] + totals[2][0], totals[1][1] + totals[2][1],
        (old * old)[0:8], (small * small)[0:8], (old * old)[8:16], (small * small)[8:16],
    ]
    lane = lax.broadcasted_iota(jnp.int32, TILE, 1)
    tile = jnp.zeros(TILE, jnp.float32)
    for place, column in enumerate(columns):
        tile = jnp.where(lane == place, jnp.sum(column, axis=1, keepdims=True), tile)
    part_sums[...] = tile
    for place in range(3 * CHUNKS - OUT_SLOTS, 3 * CHUNKS):
        for copy in copies(place // CHUNKS, place % CHUNKS):
            copy.wait()


def resident(value):
    return pltpu.with_memory_space_constraint(value, pltpu.VMEM)


def update_step(sums, small_sums, total, weights, firsts, seconds, smalls):
    anywhere = pl.BlockSpec(memory_space=pl.ANY)
    inside = pl.BlockSpec(memory_space=pltpu.VMEM)
    attn = pltpu.HBM((ATTN_ROWS, LANES), jnp.float32)
    mlp = pltpu.HBM((MLP_ROWS, LANES), jnp.float32)
    wide = jax.ShapeDtypeStruct((1, 320), jnp.float32)
    vec = jax.ShapeDtypeStruct((11, 80), jnp.float32)
    operands = [sums, small_sums, total, *weights, *firsts, *seconds]
    return pl.pallas_call(
        update_kernel,
        name="update",
        out_shape=(
            pltpu.VMEM((ROWS, LANES), jnp.float32),
            pltpu.VMEM((SMALL_ROWS, LANES), jnp.float32),
            pltpu.VMEM((SMALL_ROWS, LANES), jnp.float32),
            pltpu.VMEM(TILE, jnp.float32),
            attn, mlp, attn, mlp, wide, vec, wide, vec,
        ),
        in_specs=[inside] * 15,
        out_specs=(inside,) * 4 + (anywhere,) * 4 + (inside,) * 4,
        scratch_shapes=[
            pltpu.VMEM((OUT_SLOTS, CHUNK, LANES), jnp.float32),
            pltpu.VMEM((OUT_SLOTS, CHUNK, LANES), jnp.float32),
            pltpu.VMEM((SMALL_ROWS, LANES), jnp.float32),
            pltpu.VMEM((SMALL_ROWS, LANES), jnp.float32),
            pltpu.SemaphoreType.DMA((OUT_SLOTS, 2)),
        ],
        compiler_params=pltpu.CompilerParams(vmem_limit_bytes=UPDATE_VMEM),
    )(*[resident(value) for value in operands], *smalls)


def gather_kernel(part_sums, weight_attn, weight_mlp, update, small_weight, small_update,
                  everything, all_wide, all_vec, new_weight, new_wide, new_vec,
                  all_small, fresh_small, new_small, slots, wide_flat, pair,
                  tile_send, tile_recv, small_send, small_recv, link_send, link_recv, twin_send, twin_recv,
                  own_send, own_recv, last_send, last_recv, last_twin_send, last_twin_recv):
    me = lax.axis_index("data")
    twin = flip(me, CORE)
    greet_everyone(me)
    meet_everyone()
    slots[me] = part_sums[...]
    tile_to_everyone(me, lambda owner: part_sums, slots, tile_send, tile_recv, True)
    tile_to_everyone(me, lambda owner: part_sums, slots, tile_send, tile_recv, False)
    sums = jnp.sum(slots[...], axis=0)
    lane = lax.broadcasted_iota(jnp.int32, TILE, 1)

    def column(place):
        return jnp.sum(jnp.where(lane == place, sums, 0.0), axis=1, keepdims=True)

    def same_tensor(value, rows):
        total = value
        for shift in range(rows, 8, rows):
            total = total + pltpu.roll(value, shift, 0)
        return total

    def wide_rows(value):
        row = lax.broadcasted_iota(jnp.int32, (8, 1), 0)
        mine = jnp.logical_and(row >= 3, row < 6)
        return jnp.where(mine, jnp.sum(jnp.where(mine, value, 0.0), axis=0, keepdims=True), value)

    def spread(value):
        return jnp.broadcast_to(value, TILE)

    def ratio(weights, updates):
        safe = jnp.where(updates > 0.0, updates, 1.0)
        return jnp.sqrt(weights) / jnp.sqrt(safe)

    ratio_attn = ratio(same_tensor(spread(column(0)), 4), same_tensor(spread(column(1)), 4))
    ratio_mlp = ratio(same_tensor(spread(column(2)), 2), same_tensor(spread(column(3)), 2))
    ratio_low = ratio(spread(column(4)), spread(column(5)))
    ratio_high = ratio(spread(wide_rows(column(6))), spread(wide_rows(column(7))))

    def place_of(third, owner):
        return everything.at[owner, pl.ds(third * THIRD, THIRD)]

    def link(third, stage, hops):
        number = ARRIVALS.index((stage, hops))
        to = flip(me, ORDERS[third][stage])
        owner = flip_all(me, [ORDERS[third][hop] for hop in hops])
        place = place_of(third, owner)
        return pltpu.make_async_remote_copy(
            place, place, link_send.at[third, number], link_recv.at[third, number],
            device_id=(to,), device_id_type=MESH)

    def landed(third, stage, hops):
        number = ARRIVALS.index((stage, hops))
        owner = flip_all(flip(me, ORDERS[third][stage]), [ORDERS[third][hop] for hop in hops])
        place = place_of(third, owner)
        return pltpu.make_async_remote_copy(
            place, place, link_send.at[third, number], link_recv.at[third, number],
            device_id=(flip(me, ORDERS[third][stage]),), device_id_type=MESH)

    def to_twin(third, number, hops):
        owner = flip_all(me, [ORDERS[third][hop] for hop in hops])
        place = place_of(third, owner)
        return pltpu.make_async_remote_copy(
            place, place, twin_send.at[third, number], twin_recv.at[third, number],
            device_id=(twin,), device_id_type=MESH)

    def from_twin(third, number, hops):
        owner = flip_all(twin, [ORDERS[third][hop] for hop in hops])
        place = place_of(third, owner)
        return pltpu.make_async_remote_copy(
            place, place, twin_send.at[third, number], twin_recv.at[third, number],
            device_id=(twin,), device_id_type=MESH)

    def own_part(third, part, owner):
        start, rows = OWN_PARTS[part]
        place = everything.at[owner, pl.ds(third * THIRD + start, rows)]
        return pltpu.make_async_remote_copy(
            place, place, own_send.at[third, part], own_recv.at[third, part],
            device_id=(flip(me, ORDERS[third][0]),), device_id_type=MESH)

    for part, (first_row, rows_here) in enumerate(OWN_PARTS):
        for third in THIRDS:
            scale = LEARN_RATE * (ratio_attn if third == 0 else ratio_mlp)
            weight, base = bank_part(third, weight_attn, weight_mlp)

            def refresh(piece, carry, third=third, scale=scale, weight=weight, base=base, first_row=first_row):
                row = first_row + piece * BLOCK
                rows = pl.ds(pl.multiple_of(third * THIRD + row, BLOCK), BLOCK)
                old = weight[pl.ds(pl.multiple_of(base + row, BLOCK), BLOCK)].reshape((-1,) + TILE)
                new = (old - scale[None] * update[rows].reshape((-1,) + TILE)).reshape(BLOCK, LANES)
                new_weight[rows] = new
                everything[me, rows] = new.astype(jnp.bfloat16)
                return carry

            lax.fori_loop(0, rows_here // BLOCK, refresh, 0)
            own_part(third, part, me).start()
    for stage in (1, 2):
        for third in THIRDS:
            link(third, stage, ()).start()
    for third in THIRDS:
        to_twin(third, 0, ()).start()
    low = small_weight[0:8] - LEARN_RATE * ratio_low * small_update[0:8]
    high = small_weight[8:16] - LEARN_RATE * ratio_high * small_update[8:16]
    new_small[...] = jnp.concatenate([low, high], axis=0)
    unpack_rows(new_small, new_wide, new_vec)
    fresh_small[...] = new_small[...].astype(jnp.bfloat16)
    all_small[me] = fresh_small[...]
    tile_to_everyone(me, lambda owner: fresh_small, all_small, small_send, small_recv, True)

    def last_part(third, part, owner, to, send_sem, recv_sem):
        place = everything.at[owner, pl.ds(third * THIRD + part * LAST, LAST)]
        return pltpu.make_async_remote_copy(
            place, place, send_sem.at[third, part], recv_sem.at[third, part], device_id=(to,), device_id_type=MESH)

    def last_link(third, part):
        owner = flip_all(me, ORDERS[third][:2])
        return last_part(third, part, owner, flip(me, ORDERS[third][2]), last_send, last_recv)

    def last_landed(third, part):
        return last_part(third, part, flip_all(me, ORDERS[third]), flip(me, ORDERS[third][2]), last_send, last_recv)

    def last_to_twin(third, part):
        return last_part(third, part, flip_all(me, ORDERS[third]), twin, last_twin_send, last_twin_recv)

    def last_from_twin(third, part):
        return last_part(third, part, flip_all(twin, ORDERS[third]), twin, last_twin_send, last_twin_recv)

    sent = []
    for number, (stage, hops) in enumerate(ARRIVALS):
        for third in THIRDS:
            if number == 0:
                for part in range(len(OWN_PARTS)):
                    own_part(third, part, flip(me, ORDERS[third][0])).wait_recv()
            else:
                landed(third, stage, hops).wait_recv()
            for later in () if hops else range(stage + 1, len(THIRDS)):
                copy = link(third, later, (stage,))
                copy.start()
                sent.append(copy)
            if hops and stage == 1:
                for part in range(PARTS):
                    last_link(third, part).start()
            to_twin(third, number + 1, (stage,) + hops).start()
        if number == 2:
            tile_to_everyone(me, lambda owner: fresh_small, all_small, small_send, small_recv, False)
            shares_to(all_small, all_wide, all_vec, wide_flat, pair)
    for number, hops in enumerate(((),) + tuple((stage,) + hops for stage, hops in ARRIVALS)):
        for third in THIRDS:
            from_twin(third, number, hops).wait_recv()
            to_twin(third, number, hops).wait_send()
    for third in THIRDS:
        for part in range(len(OWN_PARTS)):
            own_part(third, part, me).wait_send()
        for stage in (1, 2):
            link(third, stage, ()).wait_send()
    for copy in sent:
        copy.wait_send()
    for part in range(PARTS):
        for third in THIRDS:
            last_landed(third, part).wait_recv()
            last_to_twin(third, part).start()
    for part in range(PARTS):
        for third in THIRDS:
            last_link(third, part).wait_send()
            last_to_twin(third, part).wait_send()
            last_from_twin(third, part).wait_recv()


def all_gather(part_sums, weights, update, small_weight, small_update):
    inside = pl.BlockSpec(memory_space=pltpu.VMEM)
    dma = pltpu.SemaphoreType.DMA
    return pl.pallas_call(
        gather_kernel,
        name="gather",
        out_shape=(
            pltpu.VMEM((GROUP, ROWS, LANES), jnp.bfloat16),
            pltpu.VMEM((1, WIDE), jnp.bfloat16),
            pltpu.VMEM((VECS, VEC), jnp.bfloat16),
            pltpu.VMEM((ROWS, LANES), jnp.float32),
            pltpu.VMEM((1, WIDE_SHARE), jnp.float32),
            pltpu.VMEM((VECS, VEC_SHARE), jnp.float32),
        ),
        in_specs=[inside] * 6,
        out_specs=(inside,) * 6,
        scratch_shapes=[
            pltpu.VMEM((GROUP, SMALL_ROWS, LANES), jnp.bfloat16),
            pltpu.VMEM((SMALL_ROWS, LANES), jnp.bfloat16),
            pltpu.VMEM((SMALL_ROWS, LANES), jnp.float32),
            pltpu.VMEM((GROUP, 8, LANES), jnp.float32),
            pltpu.VMEM((8, 5120), jnp.float32),
            pltpu.VMEM((2, SMALL_ROWS, LANES), jnp.float32),
            *[dma((GROUP,))] * 4,
            *[dma((len(THIRDS), len(ARRIVALS)))] * 2, *[dma((len(THIRDS), len(ARRIVALS) + 1))] * 2, *[dma((len(THIRDS), len(OWN_PARTS)))] * 2, *[dma((len(THIRDS), PARTS))] * 4,
        ],
        compiler_params=pltpu.CompilerParams(collective_id=1, has_side_effects=True, vmem_limit_bytes=GATHER_VMEM),
    )(*[resident(value) for value in (part_sums, *weights, update, small_weight, small_update)])


def write_kernel(everything, replica_attn, replica_mlp, attn_sems, mlp_sems):
    writes = []
    for owner in range(GROUP):
        writes.append(pltpu.make_async_copy(
            everything.at[owner, pl.ds(0, ATTN_ROWS)], replica_attn.at[pl.ds(owner * ATTN_ROWS, ATTN_ROWS)], attn_sems.at[owner]))
        writes.append(pltpu.make_async_copy(
            everything.at[owner, pl.ds(ATTN_ROWS, MLP_ROWS)], replica_mlp.at[pl.ds(owner * MLP_ROWS, MLP_ROWS)], mlp_sems.at[owner]))
    for copy in writes:
        copy.start()
    for copy in writes:
        copy.wait()


def write_replica(everything):
    anywhere = pl.BlockSpec(memory_space=pl.ANY)
    dma = pltpu.SemaphoreType.DMA
    return pl.pallas_call(
        write_kernel,
        name="write",
        out_shape=(
            pltpu.HBM((GROUP * ATTN_ROWS, LANES), jnp.bfloat16),
            pltpu.HBM((GROUP * MLP_ROWS, LANES), jnp.bfloat16),
        ),
        in_specs=[pl.BlockSpec(memory_space=pltpu.VMEM)],
        out_specs=(anywhere,) * 2,
        scratch_shapes=[dma((GROUP,)), dma((GROUP,))],
        compiler_params=pltpu.CompilerParams(vmem_limit_bytes=FINISH_VMEM),
    )(resident(everything))


def finish_kernel(new_weight, wide_in, vec_in, all_wide, all_vec, new_attn, new_mlp, new_wide, new_vec, replica_wide, replica_vec, sems):
    copies = [
        pltpu.make_async_copy(new_weight.at[pl.ds(0, ATTN_ROWS)], new_attn, sems.at[0]),
        pltpu.make_async_copy(new_weight.at[pl.ds(ATTN_ROWS, MLP_ROWS)], new_mlp, sems.at[1]),
    ]
    for number, (source, to) in enumerate(((wide_in, new_wide), (vec_in, new_vec), (all_wide, replica_wide), (all_vec, replica_vec))):
        copies.append(pltpu.make_async_copy(source, to, sems.at[number + 2]))
    for copy in copies:
        copy.start()
    for copy in copies:
        copy.wait()


def finish(new_weight, new_wide, new_vec, all_wide, all_vec):
    anywhere = pl.BlockSpec(memory_space=pl.ANY)
    inside = pl.BlockSpec(memory_space=pltpu.VMEM)
    return pl.pallas_call(
        finish_kernel,
        name="finish",
        out_shape=(
            pltpu.HBM((ATTN_ROWS, LANES), jnp.float32),
            pltpu.HBM((MLP_ROWS, LANES), jnp.float32),
            pltpu.HBM(new_wide.shape, jnp.float32),
            pltpu.HBM(new_vec.shape, jnp.float32),
            pltpu.HBM(all_wide.shape, jnp.bfloat16),
            pltpu.HBM(all_vec.shape, jnp.bfloat16),
        ),
        in_specs=[inside] * 5,
        out_specs=(anywhere,) * 6,
        scratch_shapes=[pltpu.SemaphoreType.DMA((6,))],
        compiler_params=pltpu.CompilerParams(vmem_limit_bytes=FINISH_VMEM),
    )(*[resident(value) for value in (new_weight, new_wide, new_vec, all_wide, all_vec)])


def linear(bank):
    rows, length = bank.shape
    return bank.reshape(rows, length // LANES, LANES).transpose(1, 0, 2).reshape(rows * length // LANES, LANES)


def banked(flat, rows):
    blocks = flat.size // (rows * LANES)
    return flat.reshape(blocks, rows, LANES).transpose(1, 0, 2).reshape(rows, blocks * LANES)


def solution(mesh):
    grad_spec = P("data", None, None)
    shard_spec = P(None, "data")
    full_spec = P(None, None)

    def local_step(*banks):
        grads = banks[0:4]
        attn_grad = linear(grads[0][0]).reshape(GROUP, ATTN_ROWS, LANES)
        mlp_grad = linear(grads[1][0]).reshape(GROUP, MLP_ROWS, LANES)
        states = [(linear(banks[first]), linear(banks[first + 1])) for first in (4, 8, 12)]
        smalls = [bank for first in (4, 8, 12) for bank in banks[first + 2:first + 4]]
        sums, small_sums, total = reduce_scatter(attn_grad, mlp_grad, grads[2][0], grads[3][0])
        update, small_update, small_weight, part_sums, *moments = update_step(sums, small_sums, total, *states, smalls)
        everything, all_wide, all_vec, *new = all_gather(part_sums, states[0], update, small_weight, small_update)
        replica_attn, replica_mlp = write_replica(everything)
        replica_attn, all_wide = lax.optimization_barrier((replica_attn, all_wide))
        new_attn, new_mlp, new_wide, new_vec, replica_wide, replica_vec = finish(*new, all_wide, all_vec)
        return (
            banked(replica_attn, 4), banked(replica_mlp, 2), replica_wide, replica_vec,
            banked(new_attn, 4), banked(new_mlp, 2), new_wide, new_vec,
            banked(moments[0], 4), banked(moments[1], 2), moments[4], moments[5],
            banked(moments[2], 4), banked(moments[3], 2), moments[6], moments[7],
        )

    return jax.shard_map(local_step, mesh=mesh, in_specs=(grad_spec,) * 4 + (shard_spec,) * 12, out_specs=(full_spec,) * 4 + (shard_spec,) * 12, check_vma=False)
```

```python
import functools

import jax
import jax.numpy as jnp
from jax import lax
from jax.experimental import pallas as pl
from jax.experimental.pallas import tpu as pltpu
from jax.sharding import PartitionSpec as P

STEP_NUMBER = 10
LEARN_RATE = 0.04
BETA_FIRST = 0.9
BETA_SECOND = 0.999
EPSILON = 1e-6
WEIGHT_DECAY = 0.01
MAX_NORM = 1.0
ROOT_FLOOR = 1e-36

MESH = pl.DeviceIdType.MESH
GROUP = 16
LANES = 128
TILE = (8, LANES)
THIRDS = range(3)
VECS = 11
VEC_SHARE = 80
VEC = 1280
WIDE = 5120
WIDE_PARTS = ((0, LANES), (1, LANES), (2, 64))
WIDE_SHARE = 320
MIB = 2 ** 20
ATTN_ROWS = 3200
MLP_ROWS = 6400
ROWS = ATTN_ROWS + MLP_ROWS
THIRD = 3200
PIECE = 400
PIECES = THIRD // PIECE
LOAD_SLOTS = 3
SEND_SLOTS = 4
SMALL_ROWS = 16
BLOCK = 640
PARTS = 4
LAST = THIRD // PARTS
OWN_PARTS = ((0, 640), (640, 2560))
CHUNK = 640
CHUNKS = THIRD // CHUNK
OUT_SLOTS = 4
SCATTER_VMEM = 36 * MIB
UPDATE_VMEM = 8 * MIB
GATHER_VMEM = 2 * MIB
FINISH_VMEM = 3 * MIB
CORE = 1
ORDERS = ((2, 4, 8), (4, 8, 2), (8, 2, 4))
MASKS = sorted(range(1, GROUP), key=lambda mask: (-(mask // 2).bit_count(), mask))
NEIGHBOURS = (8, 4, 2, 1)
UNITS = (
    (0, (0, 1, 2), ()),
    (0, (0, 1), ()),
    (0, (0, 2), ()),
    (1, (1, 2), (0,)),
    (0, (0,), ()),
    (1, (1,), (1,)),
    (2, (2,), (2, 3)),
    (None, (), (4, 5, 6)),
)


ARRIVALS = [(0, ()), (1, ()), (2, ()), (1, (0,)), (2, (0,)), (2, (1,))]


def flip(index, width):
    return index + width * (1 - 2 * ((index // width) % 2))


def flip_all(index, widths):
    for width in widths:
        index = flip(index, width)
    return index


def across(me, mask):
    return flip_all(me, [width for width in (CORE,) + ORDERS[0] if mask & width])


def greet(me, masks):
    for mask in masks:
        pl.semaphore_signal(pltpu.get_barrier_semaphore(), inc=1, device_id=(across(me, mask),), device_id_type=MESH)


def meet(masks):
    pl.semaphore_wait(pltpu.get_barrier_semaphore(), len(masks))


def tile_to_everyone(me, source_of, slots, send_sems, recv_sems, begin):
    for mask in MASKS:
        other = across(me, mask)

        def copy(slot):
            return pltpu.make_async_remote_copy(
                source_of(other), slots.at[slot], send_sems.at[mask], recv_sems.at[mask], device_id=(other,), device_id_type=MESH)

        if begin:
            copy(me).start()
        else:
            copy(other).wait()


def small_places(packed, wide, vec):
    places = [(packed.at[pl.ds(0, VECS), pl.ds(0, VEC_SHARE)], vec)]
    for part, width in WIDE_PARTS:
        places.append((packed.at[pl.ds(VECS + part, 1), pl.ds(0, width)], wide.at[:, pl.ds(LANES * part, width)]))
    return places


def pack_rows(wide, vec, packed):
    packed[...] = jnp.zeros_like(packed)
    for inner, outer in small_places(packed, wide, vec):
        inner[...] = outer[...]


def unpack_rows(packed, wide, vec):
    for inner, outer in small_places(packed, wide, vec):
        outer[...] = inner[...]


def shares_from(wide, vec, wide_rows, vec_rows, packed):
    wide_rows[...] = jnp.zeros_like(wide_rows)
    wide_rows[:1] = wide[...].astype(jnp.float32)
    vec_rows[...] = jnp.zeros_like(vec_rows)
    vec_rows[:VECS] = vec[...].astype(jnp.float32)
    packed[...] = jnp.zeros_like(packed)

    def window(rows, start):
        block, shift = start // LANES * LANES, start % LANES
        value = rows[:, block:block + LANES]
        if shift == 0:
            return value
        lane = lax.broadcasted_iota(jnp.int32, value.shape, 1)
        value = pltpu.roll(value, LANES - shift, 1)
        if block + LANES == rows.shape[1]:
            return value
        after = pltpu.roll(rows[:, block + LANES:block + 2 * LANES], LANES - shift, 1)
        return jnp.where(lane < LANES - shift, value, after)

    lane = lax.broadcasted_iota(jnp.int32, (SMALL_ROWS, LANES), 1)
    for owner in range(GROUP):
        packed[owner] = jnp.where(lane < VEC_SHARE, window(vec_rows, VEC_SHARE * owner), 0.0)
        for part, width in WIDE_PARTS:
            value = window(wide_rows, WIDE_SHARE * owner + LANES * part)
            packed[owner, pl.ds(VECS + part, 1)] = jnp.where(lane[:1] < width, value[:1], 0.0)


def shares_to(shares, wide, vec, wide_rows, pair):
    lane = lax.broadcasted_iota(jnp.int32, (SMALL_ROWS, LANES), 1)
    low = lax.broadcasted_iota(jnp.int32, (1, LANES), 1) < 64
    for block in range(VEC // LANES):
        value = jnp.zeros((SMALL_ROWS, LANES), jnp.float32)
        for owner in range(GROUP):
            begin, end = max(VEC_SHARE * owner, LANES * block), min(VEC_SHARE * (owner + 1), LANES * (block + 1))
            if begin < end:
                shift = (VEC_SHARE * owner - LANES * block) % LANES
                moved = shares[owner].astype(jnp.float32)
                if shift:
                    moved = pltpu.roll(moved, shift, 1)
                inside = jnp.logical_and(lane >= begin - LANES * block, lane < end - LANES * block)
                value = jnp.where(inside, moved, value)
        vec[:, LANES * block:LANES * (block + 1)] = value[:VECS].astype(jnp.bfloat16)
    for place in range(GROUP // 2):
        pair[0] = shares[2 * place].astype(jnp.float32)
        pair[1] = pltpu.roll(shares[2 * place + 1].astype(jnp.float32), 64, 1)
        even, odd = [[pair[half, pl.ds(VECS + part, 1)] for part, _ in WIDE_PARTS] for half in range(2)]
        blocks = [
            even[0], even[1], jnp.where(low, even[2], odd[0]), jnp.where(low, odd[0], odd[1]), jnp.where(low, odd[1], odd[2]),
        ]
        for number, value in enumerate(blocks):
            wide_rows[:1, pl.ds(LANES * (len(blocks) * place + number), LANES)] = value
    wide[...] = wide_rows[:1].astype(jnp.bfloat16)


def scatter_kernel(grad_attn, grad_mlp, grad_wide, grad_vec, sums, small_sums, total, pair_raw, landed,
                   raw_own, raw_pair, partial, outgoing, square_sum, small_slots, square_slots,
                   pair_near, landed_near, wide_raw, vec_raw, wide_rows, vec_rows, packed, small_shares,
                   load_sems, send_sems, pair_send_first, pair_recv_first, pair_send, pair_recv, land_sems,
                   small_send, small_recv, square_send, square_recv, local_sems):
    me = lax.axis_index("data")
    twin = flip(me, CORE)
    greet(me, NEIGHBOURS)

    def grad_of(third, owner, row, count):
        if third == 0:
            return grad_attn.at[owner, pl.ds(row, count)]
        return grad_mlp.at[owner, pl.ds(row + (third - 1) * THIRD, count)]

    def owner_of(unit, third):
        return flip_all(me, [ORDERS[third][place] for place in UNITS[unit][1]])

    def pair_first(third, piece):
        rows = piece * PIECE
        return pltpu.make_async_remote_copy(
            grad_of(third, flip(owner_of(0, third), CORE), rows, PIECE), pair_near.at[third, pl.ds(rows, PIECE)],
            pair_send_first.at[third, piece], pair_recv_first.at[third, piece], device_id=(twin,), device_id_type=MESH)

    def pair_copy(unit, third):
        return pltpu.make_async_remote_copy(
            grad_of(third, flip(owner_of(unit, third), CORE), 0, THIRD), pair_raw.at[unit - 1, third],
            pair_send.at[unit, third], pair_recv.at[unit, third], device_id=(twin,), device_id_type=MESH)

    def start_first(piece, carry):
        for third in THIRDS:
            pair_first(third, piece).start()
        return carry

    own_small = (
        pltpu.make_async_copy(grad_wide, wide_raw, local_sems.at[0]), pltpu.make_async_copy(grad_vec, vec_raw, local_sems.at[1]))
    for copy in own_small:
        copy.start()

    def loads(unit, third, piece):
        rows = piece * PIECE
        slot = (unit * PIECES + piece) % LOAD_SLOTS
        copies = [
            pltpu.make_async_copy(grad_of(third, owner_of(unit, third), rows, PIECE), raw_own.at[slot, third], load_sems.at[slot, third, 0])]
        if unit > 0:
            copies.append(pltpu.make_async_copy(
                pair_raw.at[unit - 1, third, pl.ds(rows, PIECE)], raw_pair.at[slot, third], load_sems.at[slot, third, 1]))
        for place, source in enumerate(UNITS[unit][2]):
            if source < 6:
                copies.append(pltpu.make_async_copy(
                    landed.at[source, third, pl.ds(rows, PIECE)], partial.at[slot, third, place], load_sems.at[slot, third, 2 + place]))
        return copies

    def send(unit, third, piece):
        rows = piece * PIECE
        slot = (unit * PIECES + piece) % SEND_SLOTS
        to = flip(me, ORDERS[third][UNITS[unit][0]])
        return pltpu.make_async_remote_copy(
            outgoing.at[slot, third], (landed.at[unit, third] if unit < 6 else landed_near.at[third]).at[pl.ds(rows, PIECE)],
            send_sems.at[slot, third], land_sems.at[unit, third, piece], device_id=(to,), device_id_type=MESH)

    def begin(unit, piece):
        for third in THIRDS:
            if unit > 0:
                @pl.when(piece == 0)
                def _():
                    pair_copy(unit, third).wait_recv()
            for source in UNITS[unit][2]:
                if source < 6:
                    send(source, third, piece).wait_recv()
            for copy in loads(unit, third, piece):
                copy.start()

    ahead = LOAD_SLOTS - 1
    for piece in range(ahead):
        begin(0, piece)
    meet(NEIGHBOURS)
    lax.fori_loop(0, PIECES, start_first, 0)

    for unit in range(8):
        def work(piece, carry, unit=unit):
            @pl.when(piece + ahead < PIECES)
            def _():
                begin(unit, piece + ahead)
            if unit < 7:
                @pl.when(piece + ahead >= PIECES)
                def _():
                    begin(unit + 1, piece + ahead - PIECES)
            slot = (unit * PIECES + piece) % LOAD_SLOTS
            out_slot = (unit * PIECES + piece) % SEND_SLOTS
            for third in THIRDS:
                for copy in loads(unit, third, piece):
                    copy.wait()
                rows = pl.ds(pl.multiple_of(piece * PIECE, PIECE), PIECE)
                if unit == 0:
                    pair_first(third, piece).wait_recv()
                    value = raw_own[slot, third].astype(jnp.float32) + pair_near[third, rows].astype(jnp.float32)
                else:
                    value = raw_own[slot, third].astype(jnp.float32) + raw_pair[slot, third].astype(jnp.float32)
                for place, source in enumerate(UNITS[unit][2]):
                    if source < 6:
                        value = value + partial[slot, third, place]
                    else:
                        send(source, third, piece).wait_recv()
                        value = value + landed_near[third, rows]
                if unit < 7:
                    if unit == 0:
                        @pl.when(piece >= SEND_SLOTS)
                        def _():
                            send(unit, third, piece).wait_send()
                    else:
                        send(unit, third, piece).wait_send()
                    outgoing[out_slot, third] = value
                    send(unit, third, piece).start()
                else:
                    value = value * (1.0 / GROUP)
                    sums[pl.ds(pl.multiple_of(third * THIRD + piece * PIECE, PIECE), PIECE)] = value
                    square_sum[...] += jnp.sum((value * value).reshape(PIECE // 8, 8, LANES), axis=0)
            if unit == 7:
                @pl.when(piece == 0)
                def _():
                    tile_to_everyone(me, lambda owner: small_shares.at[owner], small_slots, small_send, small_recv, True)
            if unit == 0:
                @pl.when(piece == 0)
                def _():
                    for later in range(1, 8):
                        for third in THIRDS:
                            pair_copy(later, third).start()
            return carry

        lax.fori_loop(0, PIECES, work, 0)
        if unit == 0:
            for copy in own_small:
                copy.wait()
            shares_from(wide_raw, vec_raw, wide_rows, vec_rows, packed)
            small_shares[...] = packed[...].astype(jnp.bfloat16)
            small_slots[me] = small_shares[me]
            square_sum[...] = jnp.zeros_like(square_sum)

    tile_to_everyone(me, lambda owner: small_shares.at[owner], small_slots, small_send, small_recv, False)
    small = jnp.sum(small_slots[...].astype(jnp.float32), axis=0) * (1.0 / GROUP)
    small_sums[...] = small
    square_sum[...] += (small * small)[0:8] + (small * small)[8:16]
    square_slots[me] = square_sum[...]
    tile_to_everyone(me, lambda owner: square_sum, square_slots, square_send, square_recv, True)
    for slot in range(SEND_SLOTS):
        for third in THIRDS:
            send(6, third, slot).wait_send()

    def drain(piece, carry):
        for third in THIRDS:
            pair_first(third, piece).wait_send()
        return carry

    lax.fori_loop(0, PIECES, drain, 0)
    for unit in range(1, 8):
        for third in THIRDS:
            pair_copy(unit, third).wait_send()
    tile_to_everyone(me, lambda owner: square_sum, square_slots, square_send, square_recv, False)
    total[...] = jnp.full(TILE, jnp.sum(square_slots[...]), jnp.float32)


def reduce_scatter(grad_attn, grad_mlp, grad_wide, grad_vec):
    anywhere = pl.BlockSpec(memory_space=pl.ANY)
    inside = pl.BlockSpec(memory_space=pltpu.VMEM)
    dma = pltpu.SemaphoreType.DMA
    return pl.pallas_call(
        scatter_kernel,
        name="scatter",
        out_shape=(
            pltpu.VMEM((ROWS, LANES), jnp.float32),
            pltpu.VMEM((SMALL_ROWS, LANES), jnp.float32),
            pltpu.VMEM(TILE, jnp.float32),
            pltpu.HBM((7, 3, THIRD, LANES), jnp.bfloat16),
            pltpu.HBM((6, 3, THIRD, LANES), jnp.float32),
        ),
        in_specs=[anywhere] * 4,
        out_specs=(inside, inside, inside, anywhere, anywhere),
        scratch_shapes=[
            pltpu.VMEM((LOAD_SLOTS, 3, PIECE, LANES), jnp.bfloat16),
            pltpu.VMEM((LOAD_SLOTS, 3, PIECE, LANES), jnp.bfloat16),
            pltpu.VMEM((LOAD_SLOTS, 3, 3, PIECE, LANES), jnp.float32),
            pltpu.VMEM((SEND_SLOTS, 3, PIECE, LANES), jnp.float32),
            pltpu.VMEM(TILE, jnp.float32),
            pltpu.VMEM((GROUP, SMALL_ROWS, LANES), jnp.bfloat16),
            pltpu.VMEM((GROUP, 8, LANES), jnp.float32),
            pltpu.VMEM((3, THIRD, LANES), jnp.bfloat16),
            pltpu.VMEM((3, THIRD, LANES), jnp.float32),
            pltpu.VMEM((1, 5120), jnp.bfloat16),
            pltpu.VMEM((11, 1280), jnp.bfloat16),
            pltpu.VMEM((8, 5120), jnp.float32),
            pltpu.VMEM((SMALL_ROWS, 1280), jnp.float32),
            pltpu.VMEM((GROUP, SMALL_ROWS, LANES), jnp.float32),
            pltpu.VMEM((GROUP, SMALL_ROWS, LANES), jnp.bfloat16),
            dma((LOAD_SLOTS, 3, 5)),
            dma((SEND_SLOTS, 3)),
            dma((3, PIECES)),
            dma((3, PIECES)),
            dma((8, 3)),
            dma((8, 3)),
            dma((7, 3, PIECES)),
            dma((GROUP,)),
            dma((GROUP,)),
            dma((GROUP,)),
            dma((GROUP,)),
            dma((2,)),
        ],
        compiler_params=pltpu.CompilerParams(collective_id=0, has_side_effects=True, vmem_limit_bytes=SCATTER_VMEM),
    )(*[pltpu.with_memory_space_constraint(grad, pltpu.HBM) for grad in (grad_attn, grad_mlp, grad_wide, grad_vec)])[:3]


def bank_part(third, attn, mlp):
    return (attn, 0) if third == 0 else (mlp, (third - 1) * THIRD)


def update_kernel(sums, small_sums, total, weight_attn, weight_mlp, first_attn, first_mlp, second_attn, second_mlp,
                  weight_wide, weight_vec, first_wide, first_vec, second_wide, second_vec,
                  update, small_update, small_weight, part_sums, new_first_attn, new_first_mlp, new_second_attn, new_second_mlp,
                  new_first_wide, new_first_vec, new_second_wide, new_second_vec,
                  first_out, second_out, small_first, small_second, out_sems):
    clip_coef = jnp.minimum(1.0, MAX_NORM / jnp.sqrt(total[0:1, :]))

    first_step = (1.0 - BETA_FIRST) * clip_coef
    second_step = (1.0 - BETA_SECOND) * clip_coef * clip_coef
    first_bias = 1.0 - BETA_FIRST ** STEP_NUMBER
    root_scale = first_bias ** 2 / (1.0 - BETA_SECOND ** STEP_NUMBER)

    def direction(mean_grad, weight, first, second):
        new_first = BETA_FIRST * first + first_step * mean_grad
        new_second = BETA_SECOND * second + second_step * (mean_grad * mean_grad)
        square = jnp.maximum(new_second * root_scale, ROOT_FLOOR)
        root = square * lax.rsqrt(square) + EPSILON * first_bias
        return new_first / root + WEIGHT_DECAY * weight, new_first, new_second

    def tile_sum(value):
        return jnp.sum((value * value).reshape(-1, 8, LANES), axis=0)

    def copies(third, chunk):
        slot = (third * CHUNKS + chunk) % OUT_SLOTS
        first_to, base = bank_part(third, new_first_attn, new_first_mlp)
        second_to, _ = bank_part(third, new_second_attn, new_second_mlp)
        rows = pl.ds(base + chunk * CHUNK, CHUNK)
        return (
            pltpu.make_async_copy(first_out.at[slot], first_to.at[rows], out_sems.at[slot, 0]),
            pltpu.make_async_copy(second_out.at[slot], second_to.at[rows], out_sems.at[slot, 1]),
        )

    totals = []
    for third in THIRDS:
        weight, base = bank_part(third, weight_attn, weight_mlp)
        first, _ = bank_part(third, first_attn, first_mlp)
        second, _ = bank_part(third, second_attn, second_mlp)

        def work(chunk, carry, third=third, weight=weight, first=first, second=second, base=base):
            slot = (third * CHUNKS + chunk) % OUT_SLOTS
            place = third * CHUNKS + chunk

            @pl.when(place >= OUT_SLOTS)
            def _():
                for copy in copies(third, chunk):
                    copy.wait()

            def block(step, carry):
                squares_weight, squares_update = carry
                inner = pl.multiple_of(step * BLOCK, BLOCK)
                rows = pl.ds(pl.multiple_of(base + chunk * CHUNK + inner, BLOCK), BLOCK)
                old = weight[rows]
                new_update, new_first, new_second = direction(
                    sums[pl.ds(pl.multiple_of(third * THIRD + chunk * CHUNK + inner, BLOCK), BLOCK)], old, first[rows], second[rows])
                first_out[slot, pl.ds(inner, BLOCK)] = new_first
                second_out[slot, pl.ds(inner, BLOCK)] = new_second
                update[pl.ds(pl.multiple_of(third * THIRD + chunk * CHUNK + inner, BLOCK), BLOCK)] = new_update
                return squares_weight + tile_sum(old), squares_update + tile_sum(new_update)

            carry = lax.fori_loop(0, CHUNK // BLOCK, block, carry)
            for copy in copies(third, chunk):
                copy.start()
            return carry

        zero = jnp.zeros(TILE, jnp.float32)
        totals.append(lax.fori_loop(0, CHUNKS, work, (zero, zero)))
    pack_rows(weight_wide, weight_vec, small_weight)
    pack_rows(first_wide, first_vec, small_first)
    pack_rows(second_wide, second_vec, small_second)
    small, small_m, small_v = direction(small_sums[...], small_weight[...], small_first[...], small_second[...])
    small_update[...] = small
    small_first[...] = small_m
    small_second[...] = small_v
    unpack_rows(small_first, new_first_wide, new_first_vec)
    unpack_rows(small_second, new_second_wide, new_second_vec)
    old = small_weight[...]
    columns = [
        totals[0][0], totals[0][1], totals[1][0] + totals[2][0], totals[1][1] + totals[2][1],
        (old * old)[0:8], (small * small)[0:8], (old * old)[8:16], (small * small)[8:16],
    ]
    lane = lax.broadcasted_iota(jnp.int32, TILE, 1)
    tile = jnp.zeros(TILE, jnp.float32)
    for place, column in enumerate(columns):
        tile = jnp.where(lane == place, jnp.sum(column, axis=1, keepdims=True), tile)
    part_sums[...] = tile
    for place in range(3 * CHUNKS - OUT_SLOTS, 3 * CHUNKS):
        for copy in copies(place // CHUNKS, place % CHUNKS):
            copy.wait()


def resident(value):
    return pltpu.with_memory_space_constraint(value, pltpu.VMEM)


def update_step(sums, small_sums, total, weights, firsts, seconds, smalls):
    anywhere = pl.BlockSpec(memory_space=pl.ANY)
    inside = pl.BlockSpec(memory_space=pltpu.VMEM)
    attn = pltpu.HBM((ATTN_ROWS, LANES), jnp.float32)
    mlp = pltpu.HBM((MLP_ROWS, LANES), jnp.float32)
    wide = jax.ShapeDtypeStruct((1, 320), jnp.float32)
    vec = jax.ShapeDtypeStruct((11, 80), jnp.float32)
    operands = [sums, small_sums, total, *weights, *firsts, *seconds]
    return pl.pallas_call(
        update_kernel,
        name="update",
        out_shape=(
            pltpu.VMEM((ROWS, LANES), jnp.float32),
            pltpu.VMEM((SMALL_ROWS, LANES), jnp.float32),
            pltpu.VMEM((SMALL_ROWS, LANES), jnp.float32),
            pltpu.VMEM(TILE, jnp.float32),
            attn, mlp, attn, mlp, wide, vec, wide, vec,
        ),
        in_specs=[inside] * 15,
        out_specs=(inside,) * 4 + (anywhere,) * 4 + (inside,) * 4,
        scratch_shapes=[
            pltpu.VMEM((OUT_SLOTS, CHUNK, LANES), jnp.float32),
            pltpu.VMEM((OUT_SLOTS, CHUNK, LANES), jnp.float32),
            pltpu.VMEM((SMALL_ROWS, LANES), jnp.float32),
            pltpu.VMEM((SMALL_ROWS, LANES), jnp.float32),
            pltpu.SemaphoreType.DMA((OUT_SLOTS, 2)),
        ],
        compiler_params=pltpu.CompilerParams(vmem_limit_bytes=UPDATE_VMEM),
    )(*[resident(value) for value in operands], *smalls)


def gather_kernel(part_sums, weight_attn, weight_mlp, update, small_weight, small_update,
                  everything, all_wide, all_vec, new_weight, new_wide, new_vec,
                  all_small, fresh_small, new_small, slots, wide_flat, pair,
                  tile_send, tile_recv, small_send, small_recv, link_send, link_recv, twin_send, twin_recv,
                  own_send, own_recv, last_send, last_recv, last_twin_send, last_twin_recv):
    me = lax.axis_index("data")
    twin = flip(me, CORE)
    greet(me, MASKS)
    meet(MASKS)
    slots[me] = part_sums[...]
    tile_to_everyone(me, lambda owner: part_sums, slots, tile_send, tile_recv, True)
    tile_to_everyone(me, lambda owner: part_sums, slots, tile_send, tile_recv, False)
    sums = jnp.sum(slots[...], axis=0)
    lane = lax.broadcasted_iota(jnp.int32, TILE, 1)

    def column(place):
        return jnp.sum(jnp.where(lane == place, sums, 0.0), axis=1, keepdims=True)

    def same_tensor(value, rows):
        total = value
        for shift in range(rows, 8, rows):
            total = total + pltpu.roll(value, shift, 0)
        return total

    def wide_rows(value):
        row = lax.broadcasted_iota(jnp.int32, (8, 1), 0)
        mine = jnp.logical_and(row >= 3, row < 6)
        return jnp.where(mine, jnp.sum(jnp.where(mine, value, 0.0), axis=0, keepdims=True), value)

    def spread(value):
        return jnp.broadcast_to(value, TILE)

    def ratio(weights, updates):
        safe = jnp.where(updates > 0.0, updates, 1.0)
        return jnp.sqrt(weights) / jnp.sqrt(safe)

    ratio_attn = ratio(same_tensor(spread(column(0)), 4), same_tensor(spread(column(1)), 4))
    ratio_mlp = ratio(same_tensor(spread(column(2)), 2), same_tensor(spread(column(3)), 2))
    ratio_low = ratio(spread(column(4)), spread(column(5)))
    ratio_high = ratio(spread(wide_rows(column(6))), spread(wide_rows(column(7))))

    def place_of(third, owner):
        return everything.at[owner, pl.ds(third * THIRD, THIRD)]

    def link(third, stage, hops):
        number = ARRIVALS.index((stage, hops))
        to = flip(me, ORDERS[third][stage])
        owner = flip_all(me, [ORDERS[third][hop] for hop in hops])
        place = place_of(third, owner)
        return pltpu.make_async_remote_copy(
            place, place, link_send.at[third, number], link_recv.at[third, number],
            device_id=(to,), device_id_type=MESH)

    def landed(third, stage, hops):
        number = ARRIVALS.index((stage, hops))
        owner = flip_all(flip(me, ORDERS[third][stage]), [ORDERS[third][hop] for hop in hops])
        place = place_of(third, owner)
        return pltpu.make_async_remote_copy(
            place, place, link_send.at[third, number], link_recv.at[third, number],
            device_id=(flip(me, ORDERS[third][stage]),), device_id_type=MESH)

    def to_twin(third, number, hops):
        owner = flip_all(me, [ORDERS[third][hop] for hop in hops])
        place = place_of(third, owner)
        return pltpu.make_async_remote_copy(
            place, place, twin_send.at[third, number], twin_recv.at[third, number],
            device_id=(twin,), device_id_type=MESH)

    def from_twin(third, number, hops):
        owner = flip_all(twin, [ORDERS[third][hop] for hop in hops])
        place = place_of(third, owner)
        return pltpu.make_async_remote_copy(
            place, place, twin_send.at[third, number], twin_recv.at[third, number],
            device_id=(twin,), device_id_type=MESH)

    def own_part(third, part, owner):
        start, rows = OWN_PARTS[part]
        place = everything.at[owner, pl.ds(third * THIRD + start, rows)]
        return pltpu.make_async_remote_copy(
            place, place, own_send.at[third, part], own_recv.at[third, part],
            device_id=(flip(me, ORDERS[third][0]),), device_id_type=MESH)

    for part, (first_row, rows_here) in enumerate(OWN_PARTS):
        for third in THIRDS:
            scale = LEARN_RATE * (ratio_attn if third == 0 else ratio_mlp)
            weight, base = bank_part(third, weight_attn, weight_mlp)

            def refresh(piece, carry, third=third, scale=scale, weight=weight, base=base, first_row=first_row):
                row = first_row + piece * BLOCK
                rows = pl.ds(pl.multiple_of(third * THIRD + row, BLOCK), BLOCK)
                old = weight[pl.ds(pl.multiple_of(base + row, BLOCK), BLOCK)].reshape((-1,) + TILE)
                new = (old - scale[None] * update[rows].reshape((-1,) + TILE)).reshape(BLOCK, LANES)
                new_weight[rows] = new
                everything[me, rows] = new.astype(jnp.bfloat16)
                return carry

            lax.fori_loop(0, rows_here // BLOCK, refresh, 0)
            own_part(third, part, me).start()
    for stage in (1, 2):
        for third in THIRDS:
            link(third, stage, ()).start()
    for third in THIRDS:
        to_twin(third, 0, ()).start()
    low = small_weight[0:8] - LEARN_RATE * ratio_low * small_update[0:8]
    high = small_weight[8:16] - LEARN_RATE * ratio_high * small_update[8:16]
    new_small[...] = jnp.concatenate([low, high], axis=0)
    unpack_rows(new_small, new_wide, new_vec)
    fresh_small[...] = new_small[...].astype(jnp.bfloat16)
    all_small[me] = fresh_small[...]
    tile_to_everyone(me, lambda owner: fresh_small, all_small, small_send, small_recv, True)

    def last_part(third, part, owner, to, send_sem, recv_sem):
        place = everything.at[owner, pl.ds(third * THIRD + part * LAST, LAST)]
        return pltpu.make_async_remote_copy(
            place, place, send_sem.at[third, part], recv_sem.at[third, part], device_id=(to,), device_id_type=MESH)

    def last_link(third, part):
        owner = flip_all(me, ORDERS[third][:2])
        return last_part(third, part, owner, flip(me, ORDERS[third][2]), last_send, last_recv)

    def last_landed(third, part):
        return last_part(third, part, flip_all(me, ORDERS[third]), flip(me, ORDERS[third][2]), last_send, last_recv)

    def last_to_twin(third, part):
        return last_part(third, part, flip_all(me, ORDERS[third]), twin, last_twin_send, last_twin_recv)

    def last_from_twin(third, part):
        return last_part(third, part, flip_all(twin, ORDERS[third]), twin, last_twin_send, last_twin_recv)

    sent = []
    for number, (stage, hops) in enumerate(ARRIVALS):
        for third in THIRDS:
            if number == 0:
                for part in range(len(OWN_PARTS)):
                    own_part(third, part, flip(me, ORDERS[third][0])).wait_recv()
            else:
                landed(third, stage, hops).wait_recv()
            for later in () if hops else range(stage + 1, len(THIRDS)):
                copy = link(third, later, (stage,))
                copy.start()
                sent.append(copy)
            if hops and stage == 1:
                for part in range(PARTS):
                    last_link(third, part).start()
            to_twin(third, number + 1, (stage,) + hops).start()
        if number == 2:
            tile_to_everyone(me, lambda owner: fresh_small, all_small, small_send, small_recv, False)
            shares_to(all_small, all_wide, all_vec, wide_flat, pair)
    for number, hops in enumerate(((),) + tuple((stage,) + hops for stage, hops in ARRIVALS)):
        for third in THIRDS:
            from_twin(third, number, hops).wait_recv()
            to_twin(third, number, hops).wait_send()
    for third in THIRDS:
        for part in range(len(OWN_PARTS)):
            own_part(third, part, me).wait_send()
        for stage in (1, 2):
            link(third, stage, ()).wait_send()
    for copy in sent:
        copy.wait_send()
    for part in range(PARTS):
        for third in THIRDS:
            last_landed(third, part).wait_recv()
            last_to_twin(third, part).start()
    for part in range(PARTS):
        for third in THIRDS:
            last_link(third, part).wait_send()
            last_to_twin(third, part).wait_send()
            last_from_twin(third, part).wait_recv()


def all_gather(part_sums, weights, update, small_weight, small_update):
    inside = pl.BlockSpec(memory_space=pltpu.VMEM)
    dma = pltpu.SemaphoreType.DMA
    return pl.pallas_call(
        gather_kernel,
        name="gather",
        out_shape=(
            pltpu.VMEM((GROUP, ROWS, LANES), jnp.bfloat16),
            pltpu.VMEM((1, WIDE), jnp.bfloat16),
            pltpu.VMEM((VECS, VEC), jnp.bfloat16),
            pltpu.VMEM((ROWS, LANES), jnp.float32),
            pltpu.VMEM((1, WIDE_SHARE), jnp.float32),
            pltpu.VMEM((VECS, VEC_SHARE), jnp.float32),
        ),
        in_specs=[inside] * 6,
        out_specs=(inside,) * 6,
        scratch_shapes=[
            pltpu.VMEM((GROUP, SMALL_ROWS, LANES), jnp.bfloat16),
            pltpu.VMEM((SMALL_ROWS, LANES), jnp.bfloat16),
            pltpu.VMEM((SMALL_ROWS, LANES), jnp.float32),
            pltpu.VMEM((GROUP, 8, LANES), jnp.float32),
            pltpu.VMEM((8, 5120), jnp.float32),
            pltpu.VMEM((2, SMALL_ROWS, LANES), jnp.float32),
            *[dma((GROUP,))] * 4,
            *[dma((len(THIRDS), len(ARRIVALS)))] * 2, *[dma((len(THIRDS), len(ARRIVALS) + 1))] * 2, *[dma((len(THIRDS), len(OWN_PARTS)))] * 2, *[dma((len(THIRDS), PARTS))] * 4,
        ],
        compiler_params=pltpu.CompilerParams(collective_id=1, has_side_effects=True, vmem_limit_bytes=GATHER_VMEM),
    )(*[resident(value) for value in (part_sums, *weights, update, small_weight, small_update)])


def write_kernel(everything, replica_attn, replica_mlp, attn_sems, mlp_sems):
    writes = []
    for owner in range(GROUP):
        writes.append(pltpu.make_async_copy(
            everything.at[owner, pl.ds(0, ATTN_ROWS)], replica_attn.at[pl.ds(owner * ATTN_ROWS, ATTN_ROWS)], attn_sems.at[owner]))
        writes.append(pltpu.make_async_copy(
            everything.at[owner, pl.ds(ATTN_ROWS, MLP_ROWS)], replica_mlp.at[pl.ds(owner * MLP_ROWS, MLP_ROWS)], mlp_sems.at[owner]))
    for copy in writes:
        copy.start()
    for copy in writes:
        copy.wait()


def write_replica(everything):
    anywhere = pl.BlockSpec(memory_space=pl.ANY)
    dma = pltpu.SemaphoreType.DMA
    return pl.pallas_call(
        write_kernel,
        name="write",
        out_shape=(
            pltpu.HBM((GROUP * ATTN_ROWS, LANES), jnp.bfloat16),
            pltpu.HBM((GROUP * MLP_ROWS, LANES), jnp.bfloat16),
        ),
        in_specs=[pl.BlockSpec(memory_space=pltpu.VMEM)],
        out_specs=(anywhere,) * 2,
        scratch_shapes=[dma((GROUP,)), dma((GROUP,))],
        compiler_params=pltpu.CompilerParams(vmem_limit_bytes=FINISH_VMEM),
    )(resident(everything))


def finish_kernel(new_weight, wide_in, vec_in, all_wide, all_vec, new_attn, new_mlp, new_wide, new_vec, replica_wide, replica_vec, sems):
    copies = [
        pltpu.make_async_copy(new_weight.at[pl.ds(0, ATTN_ROWS)], new_attn, sems.at[0]),
        pltpu.make_async_copy(new_weight.at[pl.ds(ATTN_ROWS, MLP_ROWS)], new_mlp, sems.at[1]),
    ]
    for number, (source, to) in enumerate(((wide_in, new_wide), (vec_in, new_vec), (all_wide, replica_wide), (all_vec, replica_vec))):
        copies.append(pltpu.make_async_copy(source, to, sems.at[number + 2]))
    for copy in copies:
        copy.start()
    for copy in copies:
        copy.wait()


def finish(new_weight, new_wide, new_vec, all_wide, all_vec):
    anywhere = pl.BlockSpec(memory_space=pl.ANY)
    inside = pl.BlockSpec(memory_space=pltpu.VMEM)
    return pl.pallas_call(
        finish_kernel,
        name="finish",
        out_shape=(
            pltpu.HBM((ATTN_ROWS, LANES), jnp.float32),
            pltpu.HBM((MLP_ROWS, LANES), jnp.float32),
            pltpu.HBM(new_wide.shape, jnp.float32),
            pltpu.HBM(new_vec.shape, jnp.float32),
            pltpu.HBM(all_wide.shape, jnp.bfloat16),
            pltpu.HBM(all_vec.shape, jnp.bfloat16),
        ),
        in_specs=[inside] * 5,
        out_specs=(anywhere,) * 6,
        scratch_shapes=[pltpu.SemaphoreType.DMA((6,))],
        compiler_params=pltpu.CompilerParams(vmem_limit_bytes=FINISH_VMEM),
    )(*[resident(value) for value in (new_weight, new_wide, new_vec, all_wide, all_vec)])


def linear(bank):
    rows, length = bank.shape
    return bank.reshape(rows, length // LANES, LANES).transpose(1, 0, 2).reshape(rows * length // LANES, LANES)


def banked(flat, rows):
    blocks = flat.size // (rows * LANES)
    return flat.reshape(blocks, rows, LANES).transpose(1, 0, 2).reshape(rows, blocks * LANES)


def solution(mesh):
    grad_spec = P("data", None, None)
    shard_spec = P(None, "data")
    full_spec = P(None, None)

    def local_step(*banks):
        grads = banks[0:4]
        attn_grad = linear(grads[0][0]).reshape(GROUP, ATTN_ROWS, LANES)
        mlp_grad = linear(grads[1][0]).reshape(GROUP, MLP_ROWS, LANES)
        states = [(linear(banks[first]), linear(banks[first + 1])) for first in (4, 8, 12)]
        smalls = [bank for first in (4, 8, 12) for bank in banks[first + 2:first + 4]]
        sums, small_sums, total = reduce_scatter(attn_grad, mlp_grad, grads[2][0], grads[3][0])
        update, small_update, small_weight, part_sums, *moments = update_step(sums, small_sums, total, *states, smalls)
        everything, all_wide, all_vec, *new = all_gather(part_sums, states[0], update, small_weight, small_update)
        replica_attn, replica_mlp = write_replica(everything)
        replica_attn, all_wide = lax.optimization_barrier((replica_attn, all_wide))
        new_attn, new_mlp, new_wide, new_vec, replica_wide, replica_vec = finish(*new, all_wide, all_vec)
        return (
            banked(replica_attn, 4), banked(replica_mlp, 2), replica_wide, replica_vec,
            banked(new_attn, 4), banked(new_mlp, 2), new_wide, new_vec,
            banked(moments[0], 4), banked(moments[1], 2), moments[4], moments[5],
            banked(moments[2], 4), banked(moments[3], 2), moments[6], moments[7],
        )

    return jax.shard_map(local_step, mesh=mesh, in_specs=(grad_spec,) * 4 + (shard_spec,) * 12, out_specs=(full_spec,) * 4 + (shard_spec,) * 12, check_vma=False)
```

```python
import functools

import jax
import jax.numpy as jnp
from jax import lax
from jax.experimental import pallas as pl
from jax.experimental.pallas import tpu as pltpu
from jax.sharding import PartitionSpec as P

STEP_NUMBER = 10
LEARN_RATE = 0.04
BETA_FIRST = 0.9
BETA_SECOND = 0.999
EPSILON = 1e-6
WEIGHT_DECAY = 0.01
MAX_NORM = 1.0
ROOT_FLOOR = 1e-36

MESH = pl.DeviceIdType.MESH
GROUP = 16
LANES = 128
TILE = (8, LANES)
THIRDS = range(3)
VECS = 11
VEC_SHARE = 80
VEC = 1280
WIDE = 5120
WIDE_PARTS = ((0, LANES), (1, LANES), (2, 64))
WIDE_SHARE = 320
MIB = 2 ** 20
ATTN_ROWS = 3200
MLP_ROWS = 6400
ROWS = ATTN_ROWS + MLP_ROWS
THIRD = 3200
PIECE = 400
PIECES = THIRD // PIECE
LOAD_SLOTS = 3
SEND_SLOTS = 4
SMALL_ROWS = 16
BLOCK = 640
PARTS = 4
LAST = THIRD // PARTS
OWN_PARTS = ((0, 320), (320, 960), (1280, 1920))
REFRESH = 320
CHUNK = 640
CHUNKS = THIRD // CHUNK
OUT_SLOTS = 4
SCATTER_VMEM = 36 * MIB
UPDATE_VMEM = 8 * MIB
GATHER_VMEM = 2 * MIB
FINISH_VMEM = 3 * MIB
CORE = 1
ORDERS = ((2, 4, 8), (4, 8, 2), (8, 2, 4))
MASKS = sorted(range(1, GROUP), key=lambda mask: (-(mask // 2).bit_count(), mask))
NEIGHBOURS = (8, 4, 2, 1)
UNITS = (
    (0, (0, 1, 2), ()),
    (0, (0, 1), ()),
    (0, (0, 2), ()),
    (1, (1, 2), (0,)),
    (0, (0,), ()),
    (1, (1,), (1,)),
    (2, (2,), (2, 3)),
    (None, (), (4, 5, 6)),
)


ARRIVALS = [(0, ()), (1, ()), (2, ()), (1, (0,)), (2, (0,)), (2, (1,))]


def flip(index, width):
    return index + width * (1 - 2 * ((index // width) % 2))


def flip_all(index, widths):
    for width in widths:
        index = flip(index, width)
    return index


def across(me, mask):
    return flip_all(me, [width for width in (CORE,) + ORDERS[0] if mask & width])


def greet(me, masks):
    for mask in masks:
        pl.semaphore_signal(pltpu.get_barrier_semaphore(), inc=1, device_id=(across(me, mask),), device_id_type=MESH)


def meet(masks):
    pl.semaphore_wait(pltpu.get_barrier_semaphore(), len(masks))


def tile_to_everyone(me, source_of, slots, send_sems, recv_sems, begin):
    for mask in MASKS:
        other = across(me, mask)

        def copy(slot):
            return pltpu.make_async_remote_copy(
                source_of(other), slots.at[slot], send_sems.at[mask], recv_sems.at[mask], device_id=(other,), device_id_type=MESH)

        if begin:
            copy(me).start()
        else:
            copy(other).wait()


def small_places(packed, wide, vec):
    places = [(packed.at[pl.ds(0, VECS), pl.ds(0, VEC_SHARE)], vec)]
    for part, width in WIDE_PARTS:
        places.append((packed.at[pl.ds(VECS + part, 1), pl.ds(0, width)], wide.at[:, pl.ds(LANES * part, width)]))
    return places


def pack_rows(wide, vec, packed):
    packed[...] = jnp.zeros_like(packed)
    for inner, outer in small_places(packed, wide, vec):
        inner[...] = outer[...]


def unpack_rows(packed, wide, vec):
    for inner, outer in small_places(packed, wide, vec):
        outer[...] = inner[...]


def shares_from(wide, vec, wide_rows, vec_rows, packed):
    wide_rows[...] = jnp.zeros_like(wide_rows)
    wide_rows[:1] = wide[...].astype(jnp.float32)
    vec_rows[...] = jnp.zeros_like(vec_rows)
    vec_rows[:VECS] = vec[...].astype(jnp.float32)
    packed[...] = jnp.zeros_like(packed)

    def window(rows, start):
        block, shift = start // LANES * LANES, start % LANES
        value = rows[:, block:block + LANES]
        if shift == 0:
            return value
        lane = lax.broadcasted_iota(jnp.int32, value.shape, 1)
        value = pltpu.roll(value, LANES - shift, 1)
        if block + LANES == rows.shape[1]:
            return value
        after = pltpu.roll(rows[:, block + LANES:block + 2 * LANES], LANES - shift, 1)
        return jnp.where(lane < LANES - shift, value, after)

    lane = lax.broadcasted_iota(jnp.int32, (SMALL_ROWS, LANES), 1)
    for owner in range(GROUP):
        packed[owner] = jnp.where(lane < VEC_SHARE, window(vec_rows, VEC_SHARE * owner), 0.0)
        for part, width in WIDE_PARTS:
            value = window(wide_rows, WIDE_SHARE * owner + LANES * part)
            packed[owner, pl.ds(VECS + part, 1)] = jnp.where(lane[:1] < width, value[:1], 0.0)


def shares_to(shares, wide, vec, wide_rows, pair):
    lane = lax.broadcasted_iota(jnp.int32, (SMALL_ROWS, LANES), 1)
    low = lax.broadcasted_iota(jnp.int32, (1, LANES), 1) < 64
    for block in range(VEC // LANES):
        value = jnp.zeros((SMALL_ROWS, LANES), jnp.float32)
        for owner in range(GROUP):
            begin, end = max(VEC_SHARE * owner, LANES * block), min(VEC_SHARE * (owner + 1), LANES * (block + 1))
            if begin < end:
                shift = (VEC_SHARE * owner - LANES * block) % LANES
                moved = shares[owner].astype(jnp.float32)
                if shift:
                    moved = pltpu.roll(moved, shift, 1)
                inside = jnp.logical_and(lane >= begin - LANES * block, lane < end - LANES * block)
                value = jnp.where(inside, moved, value)
        vec[:, LANES * block:LANES * (block + 1)] = value[:VECS].astype(jnp.bfloat16)
    for place in range(GROUP // 2):
        pair[0] = shares[2 * place].astype(jnp.float32)
        pair[1] = pltpu.roll(shares[2 * place + 1].astype(jnp.float32), 64, 1)
        even, odd = [[pair[half, pl.ds(VECS + part, 1)] for part, _ in WIDE_PARTS] for half in range(2)]
        blocks = [
            even[0], even[1], jnp.where(low, even[2], odd[0]), jnp.where(low, odd[0], odd[1]), jnp.where(low, odd[1], odd[2]),
        ]
        for number, value in enumerate(blocks):
            wide_rows[:1, pl.ds(LANES * (len(blocks) * place + number), LANES)] = value
    wide[...] = wide_rows[:1].astype(jnp.bfloat16)


def scatter_kernel(grad_attn, grad_mlp, grad_wide, grad_vec, sums, small_sums, total, pair_raw, landed,
                   raw_own, raw_pair, partial, outgoing, square_sum, small_slots, square_slots,
                   pair_near, landed_near, wide_raw, vec_raw, wide_rows, vec_rows, packed, small_shares,
                   load_sems, send_sems, pair_send_first, pair_recv_first, pair_send, pair_recv, land_sems,
                   small_send, small_recv, square_send, square_recv, local_sems):
    me = lax.axis_index("data")
    twin = flip(me, CORE)
    greet(me, NEIGHBOURS)

    def grad_of(third, owner, row, count):
        if third == 0:
            return grad_attn.at[owner, pl.ds(row, count)]
        return grad_mlp.at[owner, pl.ds(row + (third - 1) * THIRD, count)]

    def owner_of(unit, third):
        return flip_all(me, [ORDERS[third][place] for place in UNITS[unit][1]])

    def pair_first(third, piece):
        rows = piece * PIECE
        return pltpu.make_async_remote_copy(
            grad_of(third, flip(owner_of(0, third), CORE), rows, PIECE), pair_near.at[third, pl.ds(rows, PIECE)],
            pair_send_first.at[third, piece], pair_recv_first.at[third, piece], device_id=(twin,), device_id_type=MESH)

    def pair_copy(unit, third):
        return pltpu.make_async_remote_copy(
            grad_of(third, flip(owner_of(unit, third), CORE), 0, THIRD), pair_raw.at[unit - 1, third],
            pair_send.at[unit, third], pair_recv.at[unit, third], device_id=(twin,), device_id_type=MESH)

    def start_first(piece, carry):
        for third in THIRDS:
            pair_first(third, piece).start()
        return carry

    own_small = (
        pltpu.make_async_copy(grad_wide, wide_raw, local_sems.at[0]), pltpu.make_async_copy(grad_vec, vec_raw, local_sems.at[1]))
    for copy in own_small:
        copy.start()

    def loads(unit, third, piece):
        rows = piece * PIECE
        slot = (unit * PIECES + piece) % LOAD_SLOTS
        copies = [
            pltpu.make_async_copy(grad_of(third, owner_of(unit, third), rows, PIECE), raw_own.at[slot, third], load_sems.at[slot, third, 0])]
        if unit > 0:
            copies.append(pltpu.make_async_copy(
                pair_raw.at[unit - 1, third, pl.ds(rows, PIECE)], raw_pair.at[slot, third], load_sems.at[slot, third, 1]))
        for place, source in enumerate(UNITS[unit][2]):
            if source < 6:
                copies.append(pltpu.make_async_copy(
                    landed.at[source, third, pl.ds(rows, PIECE)], partial.at[slot, third, place], load_sems.at[slot, third, 2 + place]))
        return copies

    def send(unit, third, piece):
        rows = piece * PIECE
        slot = (unit * PIECES + piece) % SEND_SLOTS
        to = flip(me, ORDERS[third][UNITS[unit][0]])
        return pltpu.make_async_remote_copy(
            outgoing.at[slot, third], (landed.at[unit, third] if unit < 6 else landed_near.at[third]).at[pl.ds(rows, PIECE)],
            send_sems.at[slot, third], land_sems.at[unit, third, piece], device_id=(to,), device_id_type=MESH)

    def begin(unit, piece):
        for third in THIRDS:
            if unit > 0:
                @pl.when(piece == 0)
                def _():
                    pair_copy(unit, third).wait_recv()
            for source in UNITS[unit][2]:
                if source < 6:
                    send(source, third, piece).wait_recv()
            for copy in loads(unit, third, piece):
                copy.start()

    ahead = LOAD_SLOTS - 1
    for piece in range(ahead):
        begin(0, piece)
    meet(NEIGHBOURS)
    lax.fori_loop(0, PIECES, start_first, 0)

    for unit in range(8):
        def work(piece, carry, unit=unit):
            @pl.when(piece + ahead < PIECES)
            def _():
                begin(unit, piece + ahead)
            if unit < 7:
                @pl.when(piece + ahead >= PIECES)
                def _():
                    begin(unit + 1, piece + ahead - PIECES)
            slot = (unit * PIECES + piece) % LOAD_SLOTS
            out_slot = (unit * PIECES + piece) % SEND_SLOTS
            for third in THIRDS:
                for copy in loads(unit, third, piece):
                    copy.wait()
                rows = pl.ds(pl.multiple_of(piece * PIECE, PIECE), PIECE)
                if unit == 0:
                    pair_first(third, piece).wait_recv()
                    value = raw_own[slot, third].astype(jnp.float32) + pair_near[third, rows].astype(jnp.float32)
                else:
                    value = raw_own[slot, third].astype(jnp.float32) + raw_pair[slot, third].astype(jnp.float32)
                for place, source in enumerate(UNITS[unit][2]):
                    if source < 6:
                        value = value + partial[slot, third, place]
                    else:
                        send(source, third, piece).wait_recv()
                        value = value + landed_near[third, rows]
                if unit < 7:
                    if unit == 0:
                        @pl.when(piece >= SEND_SLOTS)
                        def _():
                            send(unit, third, piece).wait_send()
                    else:
                        send(unit, third, piece).wait_send()
                    outgoing[out_slot, third] = value
                    send(unit, third, piece).start()
                else:
                    value = value * (1.0 / GROUP)
                    sums[pl.ds(pl.multiple_of(third * THIRD + piece * PIECE, PIECE), PIECE)] = value
                    square_sum[...] += jnp.sum((value * value).reshape(PIECE // 8, 8, LANES), axis=0)
            if unit == 7:
                @pl.when(piece == 0)
                def _():
                    tile_to_everyone(me, lambda owner: small_shares.at[owner], small_slots, small_send, small_recv, True)
            if unit == 0:
                @pl.when(piece == 0)
                def _():
                    for later in range(1, 8):
                        for third in THIRDS:
                            pair_copy(later, third).start()
            return carry

        lax.fori_loop(0, PIECES, work, 0)
        if unit == 0:
            for copy in own_small:
                copy.wait()
            shares_from(wide_raw, vec_raw, wide_rows, vec_rows, packed)
            small_shares[...] = packed[...].astype(jnp.bfloat16)
            small_slots[me] = small_shares[me]
            square_sum[...] = jnp.zeros_like(square_sum)

    tile_to_everyone(me, lambda owner: small_shares.at[owner], small_slots, small_send, small_recv, False)
    small = jnp.sum(small_slots[...].astype(jnp.float32), axis=0) * (1.0 / GROUP)
    small_sums[...] = small
    square_sum[...] += (small * small)[0:8] + (small * small)[8:16]
    square_slots[me] = square_sum[...]
    tile_to_everyone(me, lambda owner: square_sum, square_slots, square_send, square_recv, True)
    for slot in range(SEND_SLOTS):
        for third in THIRDS:
            send(6, third, slot).wait_send()

    def drain(piece, carry):
        for third in THIRDS:
            pair_first(third, piece).wait_send()
        return carry

    lax.fori_loop(0, PIECES, drain, 0)
    for unit in range(1, 8):
        for third in THIRDS:
            pair_copy(unit, third).wait_send()
    tile_to_everyone(me, lambda owner: square_sum, square_slots, square_send, square_recv, False)
    total[...] = jnp.full(TILE, jnp.sum(square_slots[...]), jnp.float32)


def reduce_scatter(grad_attn, grad_mlp, grad_wide, grad_vec):
    anywhere = pl.BlockSpec(memory_space=pl.ANY)
    inside = pl.BlockSpec(memory_space=pltpu.VMEM)
    dma = pltpu.SemaphoreType.DMA
    return pl.pallas_call(
        scatter_kernel,
        name="scatter",
        out_shape=(
            pltpu.VMEM((ROWS, LANES), jnp.float32),
            pltpu.VMEM((SMALL_ROWS, LANES), jnp.float32),
            pltpu.VMEM(TILE, jnp.float32),
            pltpu.HBM((7, 3, THIRD, LANES), jnp.bfloat16),
            pltpu.HBM((6, 3, THIRD, LANES), jnp.float32),
        ),
        in_specs=[anywhere] * 4,
        out_specs=(inside, inside, inside, anywhere, anywhere),
        scratch_shapes=[
            pltpu.VMEM((LOAD_SLOTS, 3, PIECE, LANES), jnp.bfloat16),
            pltpu.VMEM((LOAD_SLOTS, 3, PIECE, LANES), jnp.bfloat16),
            pltpu.VMEM((LOAD_SLOTS, 3, 3, PIECE, LANES), jnp.float32),
            pltpu.VMEM((SEND_SLOTS, 3, PIECE, LANES), jnp.float32),
            pltpu.VMEM(TILE, jnp.float32),
            pltpu.VMEM((GROUP, SMALL_ROWS, LANES), jnp.bfloat16),
            pltpu.VMEM((GROUP, 8, LANES), jnp.float32),
            pltpu.VMEM((3, THIRD, LANES), jnp.bfloat16),
            pltpu.VMEM((3, THIRD, LANES), jnp.float32),
            pltpu.VMEM((1, 5120), jnp.bfloat16),
            pltpu.VMEM((11, 1280), jnp.bfloat16),
            pltpu.VMEM((8, 5120), jnp.float32),
            pltpu.VMEM((SMALL_ROWS, 1280), jnp.float32),
            pltpu.VMEM((GROUP, SMALL_ROWS, LANES), jnp.float32),
            pltpu.VMEM((GROUP, SMALL_ROWS, LANES), jnp.bfloat16),
            dma((LOAD_SLOTS, 3, 5)),
            dma((SEND_SLOTS, 3)),
            dma((3, PIECES)),
            dma((3, PIECES)),
            dma((8, 3)),
            dma((8, 3)),
            dma((7, 3, PIECES)),
            dma((GROUP,)),
            dma((GROUP,)),
            dma((GROUP,)),
            dma((GROUP,)),
            dma((2,)),
        ],
        compiler_params=pltpu.CompilerParams(collective_id=0, has_side_effects=True, vmem_limit_bytes=SCATTER_VMEM),
    )(*[pltpu.with_memory_space_constraint(grad, pltpu.HBM) for grad in (grad_attn, grad_mlp, grad_wide, grad_vec)])[:3]


def bank_part(third, attn, mlp):
    return (attn, 0) if third == 0 else (mlp, (third - 1) * THIRD)


def update_kernel(sums, small_sums, total, weight_attn, weight_mlp, first_attn, first_mlp, second_attn, second_mlp,
                  weight_wide, weight_vec, first_wide, first_vec, second_wide, second_vec,
                  update, small_update, small_weight, part_sums, new_first_attn, new_first_mlp, new_second_attn, new_second_mlp,
                  new_first_wide, new_first_vec, new_second_wide, new_second_vec,
                  first_out, second_out, small_first, small_second, out_sems):
    clip_coef = jnp.minimum(1.0, MAX_NORM / jnp.sqrt(total[0:1, :]))

    first_step = (1.0 - BETA_FIRST) * clip_coef
    second_step = (1.0 - BETA_SECOND) * clip_coef * clip_coef
    first_bias = 1.0 - BETA_FIRST ** STEP_NUMBER
    root_scale = first_bias ** 2 / (1.0 - BETA_SECOND ** STEP_NUMBER)

    def direction(mean_grad, weight, first, second):
        new_first = BETA_FIRST * first + first_step * mean_grad
        new_second = BETA_SECOND * second + second_step * (mean_grad * mean_grad)
        square = jnp.maximum(new_second * root_scale, ROOT_FLOOR)
        root = square * lax.rsqrt(square) + EPSILON * first_bias
        return new_first / root + WEIGHT_DECAY * weight, new_first, new_second

    def tile_sum(value):
        return jnp.sum((value * value).reshape(-1, 8, LANES), axis=0)

    def copies(third, chunk):
        slot = (third * CHUNKS + chunk) % OUT_SLOTS
        first_to, base = bank_part(third, new_first_attn, new_first_mlp)
        second_to, _ = bank_part(third, new_second_attn, new_second_mlp)
        rows = pl.ds(base + chunk * CHUNK, CHUNK)
        return (
            pltpu.make_async_copy(first_out.at[slot], first_to.at[rows], out_sems.at[slot, 0]),
            pltpu.make_async_copy(second_out.at[slot], second_to.at[rows], out_sems.at[slot, 1]),
        )

    totals = []
    for third in THIRDS:
        weight, base = bank_part(third, weight_attn, weight_mlp)
        first, _ = bank_part(third, first_attn, first_mlp)
        second, _ = bank_part(third, second_attn, second_mlp)

        def work(chunk, carry, third=third, weight=weight, first=first, second=second, base=base):
            slot = (third * CHUNKS + chunk) % OUT_SLOTS
            place = third * CHUNKS + chunk

            @pl.when(place >= OUT_SLOTS)
            def _():
                for copy in copies(third, chunk):
                    copy.wait()

            def block(step, carry):
                squares_weight, squares_update = carry
                inner = pl.multiple_of(step * BLOCK, BLOCK)
                rows = pl.ds(pl.multiple_of(base + chunk * CHUNK + inner, BLOCK), BLOCK)
                old = weight[rows]
                new_update, new_first, new_second = direction(
                    sums[pl.ds(pl.multiple_of(third * THIRD + chunk * CHUNK + inner, BLOCK), BLOCK)], old, first[rows], second[rows])
                first_out[slot, pl.ds(inner, BLOCK)] = new_first
                second_out[slot, pl.ds(inner, BLOCK)] = new_second
                update[pl.ds(pl.multiple_of(third * THIRD + chunk * CHUNK + inner, BLOCK), BLOCK)] = new_update
                return squares_weight + tile_sum(old), squares_update + tile_sum(new_update)

            carry = lax.fori_loop(0, CHUNK // BLOCK, block, carry)
            for copy in copies(third, chunk):
                copy.start()
            return carry

        zero = jnp.zeros(TILE, jnp.float32)
        totals.append(lax.fori_loop(0, CHUNKS, work, (zero, zero)))
    pack_rows(weight_wide, weight_vec, small_weight)
    pack_rows(first_wide, first_vec, small_first)
    pack_rows(second_wide, second_vec, small_second)
    small, small_m, small_v = direction(small_sums[...], small_weight[...], small_first[...], small_second[...])
    small_update[...] = small
    small_first[...] = small_m
    small_second[...] = small_v
    unpack_rows(small_first, new_first_wide, new_first_vec)
    unpack_rows(small_second, new_second_wide, new_second_vec)
    old = small_weight[...]
    columns = [
        totals[0][0], totals[0][1], totals[1][0] + totals[2][0], totals[1][1] + totals[2][1],
        (old * old)[0:8], (small * small)[0:8], (old * old)[8:16], (small * small)[8:16],
    ]
    lane = lax.broadcasted_iota(jnp.int32, TILE, 1)
    tile = jnp.zeros(TILE, jnp.float32)
    for place, column in enumerate(columns):
        tile = jnp.where(lane == place, jnp.sum(column, axis=1, keepdims=True), tile)
    part_sums[...] = tile
    for place in range(3 * CHUNKS - OUT_SLOTS, 3 * CHUNKS):
        for copy in copies(place // CHUNKS, place % CHUNKS):
            copy.wait()


def resident(value):
    return pltpu.with_memory_space_constraint(value, pltpu.VMEM)


def update_step(sums, small_sums, total, weights, firsts, seconds, smalls):
    anywhere = pl.BlockSpec(memory_space=pl.ANY)
    inside = pl.BlockSpec(memory_space=pltpu.VMEM)
    attn = pltpu.HBM((ATTN_ROWS, LANES), jnp.float32)
    mlp = pltpu.HBM((MLP_ROWS, LANES), jnp.float32)
    wide = jax.ShapeDtypeStruct((1, 320), jnp.float32)
    vec = jax.ShapeDtypeStruct((11, 80), jnp.float32)
    operands = [sums, small_sums, total, *weights, *firsts, *seconds]
    return pl.pallas_call(
        update_kernel,
        name="update",
        out_shape=(
            pltpu.VMEM((ROWS, LANES), jnp.float32),
            pltpu.VMEM((SMALL_ROWS, LANES), jnp.float32),
            pltpu.VMEM((SMALL_ROWS, LANES), jnp.float32),
            pltpu.VMEM(TILE, jnp.float32),
            attn, mlp, attn, mlp, wide, vec, wide, vec,
        ),
        in_specs=[inside] * 15,
        out_specs=(inside,) * 4 + (anywhere,) * 4 + (inside,) * 4,
        scratch_shapes=[
            pltpu.VMEM((OUT_SLOTS, CHUNK, LANES), jnp.float32),
            pltpu.VMEM((OUT_SLOTS, CHUNK, LANES), jnp.float32),
            pltpu.VMEM((SMALL_ROWS, LANES), jnp.float32),
            pltpu.VMEM((SMALL_ROWS, LANES), jnp.float32),
            pltpu.SemaphoreType.DMA((OUT_SLOTS, 2)),
        ],
        compiler_params=pltpu.CompilerParams(vmem_limit_bytes=UPDATE_VMEM),
    )(*[resident(value) for value in operands], *smalls)


def gather_kernel(part_sums, weight_attn, weight_mlp, update, small_weight, small_update,
                  everything, all_wide, all_vec, new_weight, new_wide, new_vec,
                  all_small, fresh_small, new_small, slots, wide_flat, pair,
                  tile_send, tile_recv, small_send, small_recv, link_send, link_recv, twin_send, twin_recv,
                  own_send, own_recv, last_send, last_recv, last_twin_send, last_twin_recv):
    me = lax.axis_index("data")
    twin = flip(me, CORE)
    greet(me, MASKS)
    meet(MASKS)
    slots[me] = part_sums[...]
    tile_to_everyone(me, lambda owner: part_sums, slots, tile_send, tile_recv, True)
    tile_to_everyone(me, lambda owner: part_sums, slots, tile_send, tile_recv, False)
    sums = jnp.sum(slots[...], axis=0)
    lane = lax.broadcasted_iota(jnp.int32, TILE, 1)

    def column(place):
        return jnp.sum(jnp.where(lane == place, sums, 0.0), axis=1, keepdims=True)

    def same_tensor(value, rows):
        total = value
        for shift in range(rows, 8, rows):
            total = total + pltpu.roll(value, shift, 0)
        return total

    def wide_rows(value):
        row = lax.broadcasted_iota(jnp.int32, (8, 1), 0)
        mine = jnp.logical_and(row >= 3, row < 6)
        return jnp.where(mine, jnp.sum(jnp.where(mine, value, 0.0), axis=0, keepdims=True), value)

    def spread(value):
        return jnp.broadcast_to(value, TILE)

    def ratio(weights, updates):
        safe = jnp.where(updates > 0.0, updates, 1.0)
        return jnp.sqrt(weights) / jnp.sqrt(safe)

    ratio_attn = ratio(same_tensor(spread(column(0)), 4), same_tensor(spread(column(1)), 4))
    ratio_mlp = ratio(same_tensor(spread(column(2)), 2), same_tensor(spread(column(3)), 2))
    ratio_low = ratio(spread(column(4)), spread(column(5)))
    ratio_high = ratio(spread(wide_rows(column(6))), spread(wide_rows(column(7))))

    def place_of(third, owner):
        return everything.at[owner, pl.ds(third * THIRD, THIRD)]

    def link(third, stage, hops):
        number = ARRIVALS.index((stage, hops))
        to = flip(me, ORDERS[third][stage])
        owner = flip_all(me, [ORDERS[third][hop] for hop in hops])
        place = place_of(third, owner)
        return pltpu.make_async_remote_copy(
            place, place, link_send.at[third, number], link_recv.at[third, number],
            device_id=(to,), device_id_type=MESH)

    def landed(third, stage, hops):
        number = ARRIVALS.index((stage, hops))
        owner = flip_all(flip(me, ORDERS[third][stage]), [ORDERS[third][hop] for hop in hops])
        place = place_of(third, owner)
        return pltpu.make_async_remote_copy(
            place, place, link_send.at[third, number], link_recv.at[third, number],
            device_id=(flip(me, ORDERS[third][stage]),), device_id_type=MESH)

    def to_twin(third, number, hops):
        owner = flip_all(me, [ORDERS[third][hop] for hop in hops])
        place = place_of(third, owner)
        return pltpu.make_async_remote_copy(
            place, place, twin_send.at[third, number], twin_recv.at[third, number],
            device_id=(twin,), device_id_type=MESH)

    def from_twin(third, number, hops):
        owner = flip_all(twin, [ORDERS[third][hop] for hop in hops])
        place = place_of(third, owner)
        return pltpu.make_async_remote_copy(
            place, place, twin_send.at[third, number], twin_recv.at[third, number],
            device_id=(twin,), device_id_type=MESH)

    def own_part(third, part, owner):
        start, rows = OWN_PARTS[part]
        place = everything.at[owner, pl.ds(third * THIRD + start, rows)]
        return pltpu.make_async_remote_copy(
            place, place, own_send.at[third, part], own_recv.at[third, part],
            device_id=(flip(me, ORDERS[third][0]),), device_id_type=MESH)

    for part, (first_row, rows_here) in enumerate(OWN_PARTS):
        for third in THIRDS:
            scale = LEARN_RATE * (ratio_attn if third == 0 else ratio_mlp)
            weight, base = bank_part(third, weight_attn, weight_mlp)

            def refresh(piece, carry, third=third, scale=scale, weight=weight, base=base, first_row=first_row):
                row = first_row + piece * REFRESH
                rows = pl.ds(pl.multiple_of(third * THIRD + row, REFRESH), REFRESH)
                old = weight[pl.ds(pl.multiple_of(base + row, REFRESH), REFRESH)].reshape((-1,) + TILE)
                new = (old - scale[None] * update[rows].reshape((-1,) + TILE)).reshape(REFRESH, LANES)
                new_weight[rows] = new
                everything[me, rows] = new.astype(jnp.bfloat16)
                return carry

            lax.fori_loop(0, rows_here // REFRESH, refresh, 0)
            own_part(third, part, me).start()
    for stage in (1, 2):
        for third in THIRDS:
            link(third, stage, ()).start()
    for third in THIRDS:
        to_twin(third, 0, ()).start()
    low = small_weight[0:8] - LEARN_RATE * ratio_low * small_update[0:8]
    high = small_weight[8:16] - LEARN_RATE * ratio_high * small_update[8:16]
    new_small[...] = jnp.concatenate([low, high], axis=0)
    unpack_rows(new_small, new_wide, new_vec)
    fresh_small[...] = new_small[...].astype(jnp.bfloat16)
    all_small[me] = fresh_small[...]
    tile_to_everyone(me, lambda owner: fresh_small, all_small, small_send, small_recv, True)

    def last_part(third, part, owner, to, send_sem, recv_sem):
        place = everything.at[owner, pl.ds(third * THIRD + part * LAST, LAST)]
        return pltpu.make_async_remote_copy(
            place, place, send_sem.at[third, part], recv_sem.at[third, part], device_id=(to,), device_id_type=MESH)

    def last_link(third, part):
        owner = flip_all(me, ORDERS[third][:2])
        return last_part(third, part, owner, flip(me, ORDERS[third][2]), last_send, last_recv)

    def last_landed(third, part):
        return last_part(third, part, flip_all(me, ORDERS[third]), flip(me, ORDERS[third][2]), last_send, last_recv)

    def last_to_twin(third, part):
        return last_part(third, part, flip_all(me, ORDERS[third]), twin, last_twin_send, last_twin_recv)

    def last_from_twin(third, part):
        return last_part(third, part, flip_all(twin, ORDERS[third]), twin, last_twin_send, last_twin_recv)

    sent = []
    for number, (stage, hops) in enumerate(ARRIVALS):
        for third in THIRDS:
            if number == 0:
                for part in range(len(OWN_PARTS)):
                    own_part(third, part, flip(me, ORDERS[third][0])).wait_recv()
            else:
                landed(third, stage, hops).wait_recv()
            for later in () if hops else range(stage + 1, len(THIRDS)):
                copy = link(third, later, (stage,))
                copy.start()
                sent.append(copy)
            if hops and stage == 1:
                for part in range(PARTS):
                    last_link(third, part).start()
            to_twin(third, number + 1, (stage,) + hops).start()
        if number == 2:
            tile_to_everyone(me, lambda owner: fresh_small, all_small, small_send, small_recv, False)
            shares_to(all_small, all_wide, all_vec, wide_flat, pair)
    for number, hops in enumerate(((),) + tuple((stage,) + hops for stage, hops in ARRIVALS)):
        for third in THIRDS:
            from_twin(third, number, hops).wait_recv()
            to_twin(third, number, hops).wait_send()
    for third in THIRDS:
        for part in range(len(OWN_PARTS)):
            own_part(third, part, me).wait_send()
        for stage in (1, 2):
            link(third, stage, ()).wait_send()
    for copy in sent:
        copy.wait_send()
    for part in range(PARTS):
        for third in THIRDS:
            last_landed(third, part).wait_recv()
            last_to_twin(third, part).start()
    for part in range(PARTS):
        for third in THIRDS:
            last_link(third, part).wait_send()
            last_to_twin(third, part).wait_send()
            last_from_twin(third, part).wait_recv()


def all_gather(part_sums, weights, update, small_weight, small_update):
    inside = pl.BlockSpec(memory_space=pltpu.VMEM)
    dma = pltpu.SemaphoreType.DMA
    return pl.pallas_call(
        gather_kernel,
        name="gather",
        out_shape=(
            pltpu.VMEM((GROUP, ROWS, LANES), jnp.bfloat16),
            pltpu.VMEM((1, WIDE), jnp.bfloat16),
            pltpu.VMEM((VECS, VEC), jnp.bfloat16),
            pltpu.VMEM((ROWS, LANES), jnp.float32),
            pltpu.VMEM((1, WIDE_SHARE), jnp.float32),
            pltpu.VMEM((VECS, VEC_SHARE), jnp.float32),
        ),
        in_specs=[inside] * 6,
        out_specs=(inside,) * 6,
        scratch_shapes=[
            pltpu.VMEM((GROUP, SMALL_ROWS, LANES), jnp.bfloat16),
            pltpu.VMEM((SMALL_ROWS, LANES), jnp.bfloat16),
            pltpu.VMEM((SMALL_ROWS, LANES), jnp.float32),
            pltpu.VMEM((GROUP, 8, LANES), jnp.float32),
            pltpu.VMEM((8, 5120), jnp.float32),
            pltpu.VMEM((2, SMALL_ROWS, LANES), jnp.float32),
            *[dma((GROUP,))] * 4,
            *[dma((len(THIRDS), len(ARRIVALS)))] * 2, *[dma((len(THIRDS), len(ARRIVALS) + 1))] * 2, *[dma((len(THIRDS), len(OWN_PARTS)))] * 2, *[dma((len(THIRDS), PARTS))] * 4,
        ],
        compiler_params=pltpu.CompilerParams(collective_id=1, has_side_effects=True, vmem_limit_bytes=GATHER_VMEM),
    )(*[resident(value) for value in (part_sums, *weights, update, small_weight, small_update)])


def write_kernel(everything, replica_attn, replica_mlp, attn_sems, mlp_sems):
    writes = []
    for owner in range(GROUP):
        writes.append(pltpu.make_async_copy(
            everything.at[owner, pl.ds(0, ATTN_ROWS)], replica_attn.at[pl.ds(owner * ATTN_ROWS, ATTN_ROWS)], attn_sems.at[owner]))
        writes.append(pltpu.make_async_copy(
            everything.at[owner, pl.ds(ATTN_ROWS, MLP_ROWS)], replica_mlp.at[pl.ds(owner * MLP_ROWS, MLP_ROWS)], mlp_sems.at[owner]))
    for copy in writes:
        copy.start()
    for copy in writes:
        copy.wait()


def write_replica(everything):
    anywhere = pl.BlockSpec(memory_space=pl.ANY)
    dma = pltpu.SemaphoreType.DMA
    return pl.pallas_call(
        write_kernel,
        name="write",
        out_shape=(
            pltpu.HBM((GROUP * ATTN_ROWS, LANES), jnp.bfloat16),
            pltpu.HBM((GROUP * MLP_ROWS, LANES), jnp.bfloat16),
        ),
        in_specs=[pl.BlockSpec(memory_space=pltpu.VMEM)],
        out_specs=(anywhere,) * 2,
        scratch_shapes=[dma((GROUP,)), dma((GROUP,))],
        compiler_params=pltpu.CompilerParams(vmem_limit_bytes=FINISH_VMEM),
    )(resident(everything))


def finish_kernel(new_weight, wide_in, vec_in, all_wide, all_vec, new_attn, new_mlp, new_wide, new_vec, replica_wide, replica_vec, sems):
    copies = [
        pltpu.make_async_copy(new_weight.at[pl.ds(0, ATTN_ROWS)], new_attn, sems.at[0]),
        pltpu.make_async_copy(new_weight.at[pl.ds(ATTN_ROWS, MLP_ROWS)], new_mlp, sems.at[1]),
    ]
    for number, (source, to) in enumerate(((wide_in, new_wide), (vec_in, new_vec), (all_wide, replica_wide), (all_vec, replica_vec))):
        copies.append(pltpu.make_async_copy(source, to, sems.at[number + 2]))
    for copy in copies:
        copy.start()
    for copy in copies:
        copy.wait()


def finish(new_weight, new_wide, new_vec, all_wide, all_vec):
    anywhere = pl.BlockSpec(memory_space=pl.ANY)
    inside = pl.BlockSpec(memory_space=pltpu.VMEM)
    return pl.pallas_call(
        finish_kernel,
        name="finish",
        out_shape=(
            pltpu.HBM((ATTN_ROWS, LANES), jnp.float32),
            pltpu.HBM((MLP_ROWS, LANES), jnp.float32),
            pltpu.HBM(new_wide.shape, jnp.float32),
            pltpu.HBM(new_vec.shape, jnp.float32),
            pltpu.HBM(all_wide.shape, jnp.bfloat16),
            pltpu.HBM(all_vec.shape, jnp.bfloat16),
        ),
        in_specs=[inside] * 5,
        out_specs=(anywhere,) * 6,
        scratch_shapes=[pltpu.SemaphoreType.DMA((6,))],
        compiler_params=pltpu.CompilerParams(vmem_limit_bytes=FINISH_VMEM),
    )(*[resident(value) for value in (new_weight, new_wide, new_vec, all_wide, all_vec)])


def linear(bank):
    rows, length = bank.shape
    return bank.reshape(rows, length // LANES, LANES).transpose(1, 0, 2).reshape(rows * length // LANES, LANES)


def banked(flat, rows):
    blocks = flat.size // (rows * LANES)
    return flat.reshape(blocks, rows, LANES).transpose(1, 0, 2).reshape(rows, blocks * LANES)


def solution(mesh):
    grad_spec = P("data", None, None)
    shard_spec = P(None, "data")
    full_spec = P(None, None)

    def local_step(*banks):
        grads = banks[0:4]
        attn_grad = linear(grads[0][0]).reshape(GROUP, ATTN_ROWS, LANES)
        mlp_grad = linear(grads[1][0]).reshape(GROUP, MLP_ROWS, LANES)
        states = [(linear(banks[first]), linear(banks[first + 1])) for first in (4, 8, 12)]
        smalls = [bank for first in (4, 8, 12) for bank in banks[first + 2:first + 4]]
        sums, small_sums, total = reduce_scatter(attn_grad, mlp_grad, grads[2][0], grads[3][0])
        update, small_update, small_weight, part_sums, *moments = update_step(sums, small_sums, total, *states, smalls)
        everything, all_wide, all_vec, *new = all_gather(part_sums, states[0], update, small_weight, small_update)
        replica_attn, replica_mlp = write_replica(everything)
        replica_attn, all_wide = lax.optimization_barrier((replica_attn, all_wide))
        new_attn, new_mlp, new_wide, new_vec, replica_wide, replica_vec = finish(*new, all_wide, all_vec)
        return (
            banked(replica_attn, 4), banked(replica_mlp, 2), replica_wide, replica_vec,
            banked(new_attn, 4), banked(new_mlp, 2), new_wide, new_vec,
            banked(moments[0], 4), banked(moments[1], 2), moments[4], moments[5],
            banked(moments[2], 4), banked(moments[3], 2), moments[6], moments[7],
        )

    return jax.shard_map(local_step, mesh=mesh, in_specs=(grad_spec,) * 4 + (shard_spec,) * 12, out_specs=(full_spec,) * 4 + (shard_spec,) * 12, check_vma=False)
```
